32 devices in a mesh: hel: 8 (over z, x), rad: 4 (over y, core).
Axes of the slice: x: 2, y: 2, z: 4, core: 2. Of those that a mesh axis runs over, the one named last changes fastest.
Arguments:
- psi_start: float32 [8, 64, 16, 768], P('hel', 'rad'), may hold values from -6 to 6
- potential: float32 [64, 16, 1536], P('rad'), may hold values from -0.5 to 0.5
- basis: bfloat16 [768, 1536], replicated, may hold values from -0.21875 to 0.21875
- kinetic: bfloat16 [64, 64], replicated, may hold values from -0.75 to 0.75
- radial_factor: float32 [64], P('rad'), may hold values from 0.002 to 0.02
- damping: float32 [64], P('rad'), may hold values from 0.7 to 1
- coupling: bfloat16 [8, 768], P('hel'), may hold values from -2 to 2
- helicity: int32 [8], P('hel'), may hold values from 0 to 7
- chan_rad: int32 [1024], replicated, may hold values from 0 to 63
- chan_vib: int32 [1024], replicated, may hold values from 0 to 15
- projector: bfloat16 [1024, 768], replicated, may hold values from -0.21875 to 0.21875
Outputs:
- psi_final: float32 [8, 64, 16, 768], P('hel', 'rad')
- amplitude: float32 [8, 1024], P('hel', 'rad')
The draws below stay inside these ranges and needn't reach their ends.
All inputs are finite; a program needn't handle non-finite values.
Results may differ from the reference program's by a relative error of at most 0.0046.
Values may be sent and summed in bfloat16 or wider, within the bound.
No kernel may reach another device: no remote copies, remote signals or barrier semaphores. Data moves between devices by JAX's collectives and lax.ppermute only.
A program may use at most 64 MiB of HBM per device.

```python
import math
import jax
import jax.numpy as jnp
from jax import lax

NV = 16
J = 768
Q = 1536
CH = 1024
ITERS = 3
HEL = 8
NR = 64


def touch_ends(result, key, smallest, largest):
    extent = result.shape
    place = [jax.random.randint(jax.random.fold_in(key, axis), (), 0, extent[axis]) for axis in range(len(extent))]
    result = result.at[tuple(place)].set(smallest)
    longest = extent.index(max(extent))
    place[longest] = (place[longest] + 1) % extent[longest]
    return result.at[tuple(place)].set(largest)


def shard_levels(own_key, shape, shards, low, largest):
    def one(dim, parts):
        draws = jax.random.uniform(jax.random.fold_in(jax.random.fold_in(own_key, 6), dim), (parts,), jnp.float32, low / len(shards), largest / len(shards))
        return jnp.repeat(jnp.exp(draws), shape[dim] // parts).reshape((-1,) + (1,) * (len(shape) - dim - 1))

    level = one(*shards[0])
    for cut in shards[1:]:
        level = level * one(*cut)
    return level


def scatter_about(rng, extent, scale, reach, split=(), held_as=jnp.bfloat16):
    drawn = jax.random.normal(rng, extent, jnp.float32) * scale
    if len(split) > 0:
        drawn = shard_levels(rng, extent, split, -0.22, 0.18) * drawn
    return jnp.clip(drawn, min=-reach, max=reach).astype(held_as)


def setup_inputs(seed: int = 0) -> dict:
    arg_keys = jax.random.split(jax.random.key(seed), 12)
    psi_start = scatter_about(arg_keys[0], (HEL, NR, NV, J), 1.0, 6.0, ((0, 8), (1, 4)), jnp.float32)
    potential = jnp.clip(jax.random.uniform(arg_keys[1], (NR, NV, Q), jnp.float32, -0.5, 0.5) * shard_levels(arg_keys[1], (NR, NV, Q), ((0, 4),), -0.4, 0.0), -0.5, 0.5)
    basis = scatter_about(arg_keys[2], (J, Q), J ** -0.5, 0.21875)
    kinetic = scatter_about(arg_keys[3], (NR, NR), NR ** -0.5, 0.75)
    radial_factor = jnp.clip(jnp.exp(math.log(0.02) - 2.30258502 * jax.random.uniform(arg_keys[4], (NR,), jnp.float32) ** shard_levels(arg_keys[4], (NR,), ((0, 4),), -0.2, 0.2)), 0.002, 0.02)
    damping = jnp.clip(0.7 + 0.3 * jax.random.uniform(arg_keys[5], (NR,), jnp.float32) ** shard_levels(arg_keys[5], (NR,), ((0, 4),), -0.2, 0.2), 0.7, 1.0)
    coupling = scatter_about(arg_keys[6], (HEL, J), 0.3, 2.0, ((0, 8),))
    helicity = touch_ends(jax.random.randint(arg_keys[7], (HEL,), 0, 8), jax.random.fold_in(arg_keys[7], 1), 0, 7).astype(jnp.int32)
    chan_rad = touch_ends(jax.random.randint(arg_keys[8], (CH,), 0, NR), jax.random.fold_in(arg_keys[8], 1), 0, NR - 1).astype(jnp.int32)
    chan_vib = touch_ends(jax.random.randint(arg_keys[9], (CH,), 0, NV), jax.random.fold_in(arg_keys[9], 1), 0, NV - 1).astype(jnp.int32)
    projector = scatter_about(arg_keys[10], (CH, J), J ** -0.5, 0.21875)
    return {"psi_start": psi_start, "potential": potential, "basis": basis, "kinetic": kinetic, "radial_factor": radial_factor, "damping": damping, "coupling": coupling, "helicity": helicity, "chan_rad": chan_rad, "chan_vib": chan_vib, "projector": projector}


def apply_ham(psi, potential, basis, kinetic, radial_factor, coupling_eff, coupling_prev, kvalue):
    packed = psi.astype(jnp.bfloat16)
    packed_f = packed.astype(jnp.float32)
    kin = jnp.einsum('rs,ksvj->krvj', kinetic.astype(jnp.float32), packed_f)

    def angular(block):
        grid = jnp.dot(block.reshape(NR * NV, J), basis, preferred_element_type=jnp.float32)
        scaled = (grid * potential.reshape(NR * NV, Q)).astype(jnp.bfloat16)
        back = lax.dot_general(scaled, basis, (((1,), (1,)), ((), ())), preferred_element_type=jnp.float32)
        return back.reshape(NR, NV, J)

    ang = lax.map(angular, packed)
    zero = jnp.zeros((1, NR, NV, J), jnp.float32)
    upper = jnp.concatenate([packed_f[1:], zero], axis=0)
    lower = jnp.concatenate([zero, packed_f[:-1]], axis=0)
    cor = coupling_eff[:, None, None, :] * upper + coupling_prev[:, None, None, :] * lower
    cen = -2.0 * (kvalue * kvalue)[:, None, None, None] * radial_factor[None, :, None, None] * psi
    return kin + ang + cen + cor


def reference(psi_start, potential, basis, kinetic, radial_factor, damping, coupling, helicity, chan_rad, chan_vib, projector):
    keep = (jnp.arange(HEL) < HEL - 1).astype(jnp.float32)
    coupling_eff = coupling.astype(jnp.float32) * keep[:, None]
    coupling_prev = jnp.concatenate([jnp.zeros((1, J), jnp.float32), coupling_eff[:-1]], axis=0)
    kvalue = helicity.astype(jnp.float32)
    damp = damping[None, :, None, None]

    def ham(p):
        return apply_ham(p, potential, basis, kinetic, radial_factor, coupling_eff, coupling_prev, kvalue)

    previous = psi_start
    current = damp * ham(psi_start)
    for step in range(ITERS - 1):
        following = damp * (2.0 * ham(current) - damp * previous)
        previous, current = current, following
    final_b = current.astype(jnp.bfloat16).astype(jnp.float32)
    rows = final_b[:, chan_rad, chan_vib, :]
    amplitude = jnp.sum(rows * projector.astype(jnp.float32)[None], axis=-1)
    return current, amplitude
```

```python
import functools

import jax
import jax.numpy as jnp
from jax import lax
from jax.experimental import pallas as pl
from jax.experimental.pallas import tpu as pltpu
from jax.sharding import Mesh
from jax.sharding import PartitionSpec as P

ITERS = 3
LANES = 128
NT = (((1,), (1,)), ((), ()))
F32 = jnp.float32
BF16 = jnp.bfloat16


def windows(blocks, groups):
    own = blocks // groups
    spans = []
    for n in range(1, ITERS + 1):
        reach = ITERS - n
        size = max(
            min(blocks, (g + 1) * own + reach) - max(0, g * own - reach) for g in range(groups)
        )
        spans.append((size, reach))
    return own, spans


def propagate(shape, rotated, n_parts, *refs):
    blocks, ygroups, groups, slab, nang, nquad, nchan, qstep, jstep = shape
    where_ref = refs[0]
    psi_parts = refs[1 : 1 + n_parts]
    pot_parts = refs[1 + n_parts : 1 + 2 * n_parts]
    basis_ref, kin_ref, rad_ref, vib_ref, proj_ref, out_ref = refs[
        1 + 2 * n_parts : 7 + 2 * n_parts
    ]
    pb0, pb1, pb2, p1, p2, scaled, pot, damp, radial, centri, coup = refs[7 + 2 * n_parts :]
    core = where_ref[0]
    vib = where_ref[1]
    nrad = ygroups * groups * slab
    own, spans = windows(blocks, groups)
    chan_rows = nang // LANES

    zero_block = jnp.zeros((1, nrad, nang), BF16)
    for buf in (pb0, pb1, pb2):
        buf[pl.ds(0, 1)] = zero_block
        buf[pl.ds(blocks + 1, 1)] = zero_block
    coup[0] = jnp.zeros((1, nang), F32)

    part_index = 0
    for psi_ref, pot_ref in zip(psi_parts, pot_parts):
        for i in range(psi_ref.shape[0]):
            slot = lax.rem(core + part_index, groups) if rotated else part_index
            for y in range(ygroups):
                row = pl.multiple_of((y * groups + slot) * slab, slab)
                for k in range(blocks):
                    pb0[k + 1, pl.ds(row, slab), :] = psi_ref[i, k, y, :, :nang]
                pot[pl.ds(row, slab), :] = pot_ref[i, y, :, :nquad].astype(F32)
                extra = pot_ref[i, y, :, nquad:].astype(F32)
                radial[pl.ds(row, slab), :] = jnp.broadcast_to(
                    extra[:, 0:1] + extra[:, 1:2], (slab, jstep)
                )
                damp[pl.ds(row, slab), :] = jnp.broadcast_to(
                    extra[:, 2:3] + extra[:, 3:4], (slab, jstep)
                )
            part_index += 1
    for k in range(blocks):
        page = psi_parts[0][0, k, 0, :, nang:].astype(F32)
        coup[k + 1] = jnp.concatenate([page[i : i + 1, :] for i in range(chan_rows)], axis=1)
        kvalue = page[chan_rows : chan_rows + 1, 0:1]
        centri[k] = jnp.broadcast_to(-2.0 * kvalue * kvalue, (1, jstep))

    def begin(n):
        size, reach = spans[max(n, 1) - 1]
        return jnp.clip(core * own - reach, 0, blocks - size)

    def step(n, source, prev, cur, target_b, target_f):
        size, reach = spans[n - 1]
        start = begin(n)
        rows = size * nrad
        shifts = [start - begin(m) for m in (n - 1, n - 2)]

        @pl.loop(0, nquad // qstep)
        def _(qi):
            q0 = pl.multiple_of(qi * qstep, qstep)
            grid = jnp.dot(
                source[pl.ds(start + 1, size)].reshape(rows, nang),
                basis_ref[:, pl.ds(q0, qstep)],
                preferred_element_type=F32,
            )
            prod = grid.reshape(size, nrad, qstep) * pot[:, pl.ds(q0, qstep)][None]
            scaled[pl.ds(0, rows), pl.ds(q0, qstep)] = prod.astype(BF16).reshape(rows, qstep)

        @pl.loop(0, nang // jstep)
        def _(ji):
            j0 = pl.multiple_of(ji * jstep, jstep)
            cols = pl.ds(j0, jstep)
            ang = lax.dot_general(
                scaled[pl.ds(0, rows), :], basis_ref[cols, :], NT, preferred_element_type=F32
            ).reshape(size, nrad, jstep)
            for i in range(size):
                k = start + i
                kin = jnp.dot(kin_ref[...], source[k + 1, :, cols], preferred_element_type=F32)
                upper = source[k + 2, :, cols].astype(F32)
                lower = source[k, :, cols].astype(F32)
                cor = coup[k + 1, :, cols] * upper + coup[k, :, cols] * lower
                if cur is None:
                    here = source[k + 1, :, cols].astype(F32)
                else:
                    here = cur[shifts[0] + i, :, cols]
                total = kin + ang[i] + centri[k] * radial[...] * here + cor
                if n == 1:
                    new = damp[...] * total
                else:
                    if n == 2:
                        before = prev[k + 1, :, cols].astype(F32)
                    else:
                        before = prev[shifts[1] + i, :, cols]
                    new = damp[...] * (2.0 * total - damp[...] * before)
                target_b[k + 1, :, cols] = new.astype(BF16)
                if target_f is not None:
                    target_f[i, :, cols] = new

    step(1, pb0, None, None, pb1, p1)
    step(2, pb1, pb0, p1, pb2, p2)
    step(3, pb2, p1, p2, pb0, None)

    first = core * own
    chan_block = nchan // (ygroups * groups)
    pieces = -(-chan_block // LANES)
    final = pb0[pl.ds(first + 1, own)].reshape(own * nrad, nang)
    rows_at = lax.broadcasted_iota(jnp.int32, (nrad, chan_block), 0)
    for y in range(ygroups):
        for slot in range(groups):
            dest = lax.rem(slot - core + groups, groups) if rotated else slot
            c0 = (y * groups + slot) * chan_block
            table = lax.dot_general(
                final, proj_ref[pl.ds(c0, chan_block), :], NT, preferred_element_type=F32
            ).reshape(own, nrad, chan_block)
            hit = (rows_at == rad_ref[:, c0 : c0 + chan_block]) & (
                vib_ref[:, c0 : c0 + chan_block] == vib
            )
            row = (y * groups + slot) * slab
            for i in range(own):
                amp = jnp.sum(jnp.where(hit, table[i], 0.0), axis=0, keepdims=True)
                if pieces * LANES > chan_block:
                    amp = jnp.concatenate(
                        [amp, jnp.zeros((1, pieces * LANES - chan_block), F32)], axis=1
                    )
                high = amp.astype(BF16).astype(F32)
                low = amp - high
                lines = [high[:, s * LANES : (s + 1) * LANES] for s in range(pieces)]
                lines += [low[:, s * LANES : (s + 1) * LANES] for s in range(pieces)]
                lines.append(jnp.zeros((slab - 2 * pieces, LANES), F32))
                out_ref[dest, i, y, :, nang:] = jnp.concatenate(lines, axis=0).astype(BF16)
                out_ref[dest, i, y, :, :nang] = pb0[first + i + 1, row : row + slab, :]


def run_blocks(where, psi_parts, pot_parts, basis, kinetic, chan_rad, chan_vib, projector, dims):
    blocks, ygroups, groups, slab = dims
    nang, nquad = basis.shape
    nchan = projector.shape[0]
    nrad = ygroups * groups * slab
    own, spans = windows(blocks, groups)
    qstep, jstep = 256, 256
    shape = (blocks, ygroups, groups, slab, nang, nquad, nchan, qstep, jstep)
    rotated = len(psi_parts) > 1
    vmem = pl.BlockSpec(memory_space=pltpu.VMEM)
    smem = pl.BlockSpec(memory_space=pltpu.SMEM)
    body = functools.partial(propagate, shape, rotated, len(psi_parts))
    n_in = 2 * len(psi_parts) + 5
    most = spans[0][0]
    return pl.pallas_call(
        body,
        out_shape=jax.ShapeDtypeStruct((groups, own, ygroups, slab, nang + LANES), BF16),
        in_specs=[smem] + [vmem] * n_in,
        out_specs=vmem,
        scratch_shapes=[
            pltpu.VMEM((blocks + 2, nrad, nang), BF16),
            pltpu.VMEM((blocks + 2, nrad, nang), BF16),
            pltpu.VMEM((blocks + 2, nrad, nang), BF16),
            pltpu.VMEM((spans[0][0], nrad, nang), F32),
            pltpu.VMEM((spans[1][0], nrad, nang), F32),
            pltpu.VMEM((most * nrad, nquad), BF16),
            pltpu.VMEM((nrad, nquad), F32),
            pltpu.VMEM((nrad, jstep), F32),
            pltpu.VMEM((nrad, jstep), F32),
            pltpu.VMEM((blocks, 1, jstep), F32),
            pltpu.VMEM((blocks + 1, 1, nang), F32),
        ],
        compiler_params=pltpu.CompilerParams(vmem_limit_bytes=60 * 1024 * 1024),
        name="propagate",
    )(where, *psi_parts, *pot_parts, basis, kinetic, chan_rad, chan_vib, projector)


def two_halves(value):
    high = lax.reduce_precision(value, 8, 7)
    return high.astype(BF16), (value - high).astype(BF16)


def per_device(
    psi_start,
    potential,
    basis,
    kinetic,
    radial_factor,
    damping,
    coupling,
    helicity,
    chan_rad,
    chan_vib,
    projector,
):
    _, slab, nvib, nang = psi_start.shape
    nquad = basis.shape[1]
    nchan = projector.shape[0]
    blocks = lax.axis_size("hel")
    ygroups = lax.axis_size("y")
    groups = lax.axis_size("c")
    hel_index = lax.axis_index("hel")
    y_index = lax.axis_index("y")
    core = lax.axis_index("c")
    swap = [(0, 1), (1, 0)]

    rf_high, rf_low = two_halves(radial_factor)
    dp_high, dp_low = two_halves(damping)
    extra = jnp.stack([rf_high, rf_low, dp_high, dp_low], axis=1)
    extra = jnp.pad(extra, ((0, 0), (0, LANES - extra.shape[1])))
    mine = lax.dynamic_slice_in_dim(potential, hel_index * ygroups, ygroups, 1).astype(BF16)
    pages = jnp.concatenate(
        [
            jnp.swapaxes(mine, 0, 1),
            jnp.broadcast_to(extra[None], (ygroups,) + extra.shape),
        ],
        axis=2,
    )
    if ygroups == 2:
        kept = lax.dynamic_index_in_dim(pages, y_index, 0, False)
        got = lax.ppermute(lax.dynamic_index_in_dim(pages, 1 - y_index, 0, False), "y", swap)
        pages = jnp.stack(
            [jnp.where(y_index == 0, kept, got), jnp.where(y_index == 0, got, kept)]
        )
    elif ygroups > 2:
        pages = lax.all_to_all(pages, "y", 0, 0, tiled=True)

    ce = jnp.where(hel_index < blocks - 1, coupling, jnp.zeros_like(coupling))
    chan_rows = nang // LANES
    aux = jnp.concatenate(
        [
            ce.reshape(chan_rows, LANES),
            jnp.broadcast_to(helicity.astype(BF16)[:, None], (1, LANES)),
            jnp.zeros((slab - chan_rows - 1, LANES), BF16),
        ],
        axis=0,
    )
    send = jnp.concatenate(
        [
            jnp.swapaxes(psi_start[0].astype(BF16), 0, 1),
            jnp.broadcast_to(aux[None], (nvib, slab, LANES)),
        ],
        axis=2,
    )
    received = lax.all_to_all(send, ("hel", "y"), 0, 0, tiled=True)
    received = received.reshape(1, blocks, ygroups, slab, nang + LANES)
    pages = pages[None]
    if groups == 2:
        psi_parts = [received, lax.ppermute(received, "c", swap)]
        pot_parts = [pages, lax.ppermute(pages, "c", swap)]
    else:
        psi_parts = [lax.all_gather(received, "c", axis=0, tiled=True)]
        pot_parts = [lax.all_gather(pages, "c", axis=0, tiled=True)]

    where = jnp.stack([core, hel_index * ygroups + y_index]).astype(jnp.int32)
    result = run_blocks(
        where,
        psi_parts,
        pot_parts,
        basis,
        kinetic,
        chan_rad[None],
        chan_vib[None],
        projector,
        (blocks, ygroups, groups, slab),
    )
    if groups == 2:
        kept = result[0]
        got = lax.ppermute(result[1], "c", swap)
        back = jnp.concatenate(
            [jnp.where(core == 0, kept, got), jnp.where(core == 0, got, kept)], axis=0
        )
    else:
        back = lax.all_to_all(result, "c", 0, 0, tiled=True)
    back = back.reshape(blocks * ygroups, slab, nang + LANES)
    home = lax.all_to_all(back, ("hel", "y"), 0, 0, tiled=True)
    psi_final = jnp.swapaxes(home[:, :, :nang], 0, 1).astype(F32)[None]
    chan_block = nchan // (ygroups * groups)
    pieces = -(-chan_block // LANES)
    lines = jnp.sum(home[:, : 2 * pieces, nang:].astype(F32), axis=0)
    amplitude = (lines[:pieces] + lines[pieces:]).reshape(1, -1)[:, :chan_block]
    return (psi_final, amplitude)


def solution(mesh):
    nhel, nrad = mesh.shape["hel"], mesh.shape["rad"]

    def run(*args):
        nvib = args[0].shape[2]
        groups = nhel * nrad // nvib
        fine = Mesh(
            mesh.devices.reshape(nhel, nrad // groups, groups), ("hel", "y", "c")
        )
        rad = ("y", "c")
        placed = (
            P("hel", rad, None, None),
            P(rad, None, None),
            P(),
            P(),
            P(rad),
            P(rad),
            P("hel", None),
            P("hel"),
            P(),
            P(),
            P(),
        )
        return jax.shard_map(
            per_device,
            mesh=fine,
            in_specs=placed,
            out_specs=(P("hel", rad, None, None), P("hel", rad)),
            check_vma=False,
        )(*args)

    return run
```

```python
import functools

import jax
import jax.numpy as jnp
from jax import lax
from jax.experimental import pallas as pl
from jax.experimental.pallas import tpu as pltpu
from jax.sharding import Mesh
from jax.sharding import PartitionSpec as P

ITERS = 3
LANES = 128
STEP = 256
NT = (((1,), (1,)), ((), ()))
F32 = jnp.float32
BF16 = jnp.bfloat16
VMEM = pl.BlockSpec(memory_space=pltpu.VMEM)
SMEM = pl.BlockSpec(memory_space=pltpu.SMEM)
PARAMS = pltpu.CompilerParams(vmem_limit_bytes=24 * 1024 * 1024)


def rows_of(ref, k, nang):
    block = ref[k, :, :, :nang]
    return block.reshape(block.shape[0] * block.shape[1], nang)


def angular(dims, first_step, *refs):
    blocks, ygroups, slab, nang, nquad = dims
    if first_step:
        msg_ref, page_ref, basis_ref, out_ref = refs[:4]
        own_ref, here_ref = msg_ref, None
        scaled, pot, radial, coup = refs[4:]
    else:
        msg_ref, page_ref, basis_ref, own_ref, here_ref, out_ref = refs[:6]
        scaled, pot, radial, coup = refs[6:]
    nrad = ygroups * slab
    chan_rows = nang // LANES
    pot[...] = page_ref[:, :, :nquad].reshape(nrad, nquad).astype(F32)
    extra = page_ref[:, :, nquad:].reshape(nrad, LANES).astype(F32)
    factor = jnp.broadcast_to(extra[:, 0:1] + extra[:, 1:2], (nrad, STEP))
    for k in range(blocks):
        page = msg_ref[k, 0, :, nang:].astype(F32)
        coup[k] = jnp.concatenate([page[i : i + 1, :] for i in range(chan_rows)], axis=1)
        kvalue = page[chan_rows : chan_rows + 1, 0:1]
        radial[k] = (-2.0 * kvalue * kvalue) * factor

    @pl.loop(0, nquad // STEP)
    def _(qi):
        cols = pl.ds(pl.multiple_of(qi * STEP, STEP), STEP)
        grid = jnp.dot(
            own_ref[:, :, :, :nang].reshape(blocks * nrad, nang),
            basis_ref[:, cols],
            preferred_element_type=F32,
        )
        prod = grid.reshape(blocks, nrad, STEP) * pot[:, cols][None]
        scaled[:, cols] = prod.astype(BF16).reshape(blocks * nrad, STEP)

    @pl.loop(0, nang // STEP)
    def _(ji):
        cols = pl.ds(pl.multiple_of(ji * STEP, STEP), STEP)
        ang = lax.dot_general(
            scaled[...], basis_ref[cols, :], NT, preferred_element_type=F32
        ).reshape(blocks, nrad, STEP)

        def block(k):
            return own_ref[k, :, :, cols].reshape(nrad, STEP).astype(F32)

        for k in range(blocks):
            here = block(k) if here_ref is None else here_ref[k, :, cols]
            total = ang[k] + radial[k] * here
            if k + 1 < blocks:
                total += coup[k, :, cols] * block(k + 1)
            if k > 0:
                total += coup[k - 1, :, cols] * block(k - 1)
            out_ref[k, :, cols] = total


def finish(dims, rotated, n, *refs):
    blocks, ygroups, groups, slab, nang, nquad, nchan = dims
    last = n == ITERS
    where_ref, page_ref, kin_ref, part_ref, own_ref, got_ref = refs[:6]
    rest = list(refs[6:])
    prev_ref = rest.pop(0) if n > 1 else None
    if last:
        rad_ref, vib_ref, proj_ref, out_ref, final = rest
    else:
        next_ref, full_ref = rest
    core = where_ref[0]
    nrad = ygroups * slab
    every = nrad * groups

    spot = lax.broadcasted_iota(jnp.int32, (every, every), 1)
    slot = spot // nrad
    if rotated:
        slot = lax.rem(slot + core, groups)
    true_at = (lax.rem(spot // slab, ygroups) * groups + slot) * slab + lax.rem(spot, slab)
    pick = (lax.broadcasted_iota(jnp.int32, (every, every), 0) == true_at).astype(BF16)
    lines = [
        kin_ref[pl.ds(pl.multiple_of((y * groups + core) * slab, slab), slab), :]
        for y in range(ygroups)
    ]
    kin_rows = jnp.dot(
        jnp.concatenate(lines, axis=0), pick, preferred_element_type=F32
    ).astype(BF16)

    extra = page_ref[:, :, nquad:].reshape(nrad, LANES).astype(F32)
    damp = jnp.broadcast_to(extra[:, 2:3] + extra[:, 3:4], (nrad, nang))
    for k in range(blocks):
        if rotated:
            pieces = [rows_of(own_ref, k, nang), rows_of(got_ref, k, nang)]
        else:
            pieces = [rows_of(got_ref.at[g], k, nang) for g in range(groups)]
        near = jnp.concatenate(pieces, axis=0)
        total = part_ref[k] + jnp.dot(kin_rows, near, preferred_element_type=F32)
        if n == 1:
            new = damp * total
        else:
            if n == 2:
                before = rows_of(prev_ref, k, nang).astype(F32)
            else:
                before = prev_ref[k]
            new = damp * (2.0 * total - damp * before)
        if last:
            final[k] = new.astype(BF16)
        else:
            full_ref[k] = new
            next_ref[k] = new.astype(BF16).reshape(ygroups, slab, nang)
    if not last:
        return

    span = nchan // ygroups
    rows_at = lax.broadcasted_iota(jnp.int32, (nrad, span), 0)
    rows_at = (rows_at // slab * groups + core) * slab + lax.rem(rows_at, slab)
    for y in range(ygroups):
        chan = pl.ds(y * span, span)
        table = lax.dot_general(
            final[...].reshape(blocks * nrad, nang),
            proj_ref[chan, :],
            NT,
            preferred_element_type=F32,
        ).reshape(blocks, nrad, span)
        hit = (rows_at == rad_ref[:, chan]) & (vib_ref[:, chan] == where_ref[1])
        for k in range(blocks):
            amp = jnp.sum(jnp.where(hit, table[k], 0.0), axis=0, keepdims=True)
            high = amp.astype(BF16).astype(F32)
            low = amp - high
            tile = [part[:, s : s + LANES] for part in (high, low) for s in range(0, span, LANES)]
            if len(tile) < slab:
                tile.append(jnp.zeros((slab - len(tile), LANES), F32))
            out_ref[k, y, :, nang:] = jnp.concatenate(tile, axis=0).astype(BF16)
            out_ref[k, y, :, :nang] = final[k, y * slab : (y + 1) * slab, :]


def two_halves(value):
    high = lax.reduce_precision(value, 8, 7)
    return high.astype(BF16), (value - high).astype(BF16)


def per_device(
    psi_start,
    potential,
    basis,
    kinetic,
    radial_factor,
    damping,
    coupling,
    helicity,
    chan_rad,
    chan_vib,
    projector,
):
    _, slab, nvib, nang = psi_start.shape
    nquad = basis.shape[1]
    nchan = projector.shape[0]
    blocks = lax.axis_size("hel")
    ygroups = lax.axis_size("y")
    groups = lax.axis_size("c")
    hel_index = lax.axis_index("hel")
    y_index = lax.axis_index("y")
    core = lax.axis_index("c")
    swap = [(0, 1), (1, 0)]
    nrad = ygroups * slab
    rotated = groups == 2

    rf_high, rf_low = two_halves(radial_factor)
    dp_high, dp_low = two_halves(damping)
    extra = jnp.stack([rf_high, rf_low, dp_high, dp_low], axis=1)
    extra = jnp.pad(extra, ((0, 0), (0, LANES - extra.shape[1])))
    mine = lax.dynamic_slice_in_dim(potential, hel_index * ygroups, ygroups, 1).astype(BF16)
    pages = jnp.concatenate(
        [jnp.swapaxes(mine, 0, 1), jnp.broadcast_to(extra[None], (ygroups,) + extra.shape)],
        axis=2,
    )
    if ygroups == 2:
        kept = lax.dynamic_index_in_dim(pages, y_index, 0, False)
        got = lax.ppermute(lax.dynamic_index_in_dim(pages, 1 - y_index, 0, False), "y", swap)
        pages = jnp.stack(
            [jnp.where(y_index == 0, kept, got), jnp.where(y_index == 0, got, kept)]
        )
    elif ygroups > 2:
        pages = lax.all_to_all(pages, "y", 0, 0, tiled=True)

    ce = jnp.where(hel_index < blocks - 1, coupling, jnp.zeros_like(coupling))
    chan_rows = nang // LANES
    aux = jnp.concatenate(
        [
            ce.reshape(chan_rows, LANES),
            jnp.broadcast_to(helicity.astype(BF16)[:, None], (1, LANES)),
            jnp.zeros((slab - chan_rows - 1, LANES), BF16),
        ],
        axis=0,
    )
    send = jnp.concatenate(
        [
            jnp.swapaxes(psi_start[0].astype(BF16), 0, 1),
            jnp.broadcast_to(aux[None], (nvib, slab, LANES)),
        ],
        axis=2,
    )
    message = lax.all_to_all(send, ("hel", "y"), 0, 0, tiled=True)
    message = message.reshape(blocks, ygroups, slab, nang + LANES)

    where = jnp.stack([core, hel_index * ygroups + y_index]).astype(jnp.int32)
    flops = 4 * blocks * nrad * nang * nquad
    cost = pl.CostEstimate(flops=flops, bytes_accessed=8 * 1024 * 1024, transcendentals=0)
    own, full = message, None
    before = []
    for n in range(1, ITERS + 1):
        if rotated:
            got = lax.ppermute(own, "c", swap)
        else:
            got = lax.all_gather(own, "c", axis=0, tiled=False)
        extra_in = [] if n == 1 else [own, full]
        part = pl.pallas_call(
            functools.partial(angular, (blocks, ygroups, slab, nang, nquad), n == 1),
            out_shape=jax.ShapeDtypeStruct((blocks, nrad, nang), F32),
            in_specs=[VMEM] * (3 + len(extra_in)),
            out_specs=VMEM,
            scratch_shapes=[
                pltpu.VMEM((blocks * nrad, nquad), BF16),
                pltpu.VMEM((nrad, nquad), F32),
                pltpu.VMEM((blocks, nrad, STEP), F32),
                pltpu.VMEM((blocks, 1, nang), F32),
            ],
            compiler_params=PARAMS,
            cost_estimate=cost,
            name=f"angular{n}",
        )(message, pages, basis, *extra_in)
        operands = [where, pages, kinetic, part, own, got] + before[-1:]
        scratch = []
        if n == ITERS:
            operands += [chan_rad[None], chan_vib[None], projector]
            outs = jax.ShapeDtypeStruct((blocks, ygroups, slab, nang + LANES), BF16)
            scratch = [pltpu.VMEM((blocks, nrad, nang), BF16)]
        else:
            outs = [
                jax.ShapeDtypeStruct((blocks, ygroups, slab, nang), BF16),
                jax.ShapeDtypeStruct((blocks, nrad, nang), F32),
            ]
        before.append(own if n == 1 else full)
        done = pl.pallas_call(
            functools.partial(
                finish, (blocks, ygroups, groups, slab, nang, nquad, nchan), rotated, n
            ),
            out_shape=outs,
            in_specs=[SMEM] + [VMEM] * (len(operands) - 1),
            out_specs=VMEM if n == ITERS else [VMEM, VMEM],
            scratch_shapes=scratch,
            compiler_params=PARAMS,
            name=f"finish{n}",
        )(*operands)
        if n < ITERS:
            own, full = done

    back = done.reshape(blocks * ygroups, slab, nang + LANES)
    home = lax.all_to_all(back, ("hel", "y"), 0, 0, tiled=True)
    psi_final = jnp.swapaxes(home[:, :, :nang], 0, 1).astype(F32)[None]
    span = nchan // ygroups
    pieces = span // LANES
    lines = jnp.sum(home[:, : 2 * pieces, nang:].astype(F32), axis=0)
    shared = (lines[:pieces] + lines[pieces:]).reshape(groups, 1, span // groups)
    amplitude = lax.dynamic_index_in_dim(shared, core, 0, False)
    if rotated:
        amplitude += lax.ppermute(lax.dynamic_index_in_dim(shared, 1 - core, 0, False), "c", swap)
    else:
        amplitude = lax.dynamic_index_in_dim(lax.psum(shared, "c"), core, 0, False)
    return (psi_final, amplitude)


def solution(mesh):
    nhel, nrad = mesh.shape["hel"], mesh.shape["rad"]

    def run(*args):
        nvib = args[0].shape[2]
        groups = nhel * nrad // nvib
        fine = Mesh(mesh.devices.reshape(nhel, nrad // groups, groups), ("hel", "y", "c"))
        rad = ("y", "c")
        placed = (
            P("hel", rad, None, None),
            P(rad, None, None),
            P(),
            P(),
            P(rad),
            P(rad),
            P("hel", None),
            P("hel"),
            P(),
            P(),
            P(),
        )
        return jax.shard_map(
            per_device,
            mesh=fine,
            in_specs=placed,
            out_specs=(P("hel", rad, None, None), P("hel", rad)),
            check_vma=False,
        )(*args)

    return run
```

```python
import functools

import jax
import jax.numpy as jnp
from jax import lax
from jax.experimental import pallas as pl
from jax.experimental.pallas import tpu as pltpu
from jax.sharding import Mesh
from jax.sharding import PartitionSpec as P

ITERS = 3
LANES = 128
STEP = 256
NT = (((1,), (1,)), ((), ()))
F32 = jnp.float32
BF16 = jnp.bfloat16
VMEM = pl.BlockSpec(memory_space=pltpu.VMEM)
HBM = pl.BlockSpec(memory_space=pltpu.HBM)
SMEM = pl.BlockSpec(memory_space=pltpu.SMEM)
PARAMS = pltpu.CompilerParams(vmem_limit_bytes=24 * 1024 * 1024)


def pack(dims, where_ref, psi_ref, coup_ref, out_ref, wide, ready, in_sems, out_sems):
    slab, nvib, chan_rows, steps = dims
    rows = slab * nvib
    tall = STEP // LANES * slab

    def load(step):
        cols = pl.ds(step * STEP, STEP)
        return pltpu.make_async_copy(psi_ref.at[:, cols], wide.at[:, cols], in_sems.at[step])

    def save(step):
        size = tall if step < steps - 1 else ready.shape[1] - tall * step
        lines = pl.ds(step * tall, size)
        return pltpu.make_async_copy(
            ready.at[:, lines, :], out_ref.at[:, lines, :], out_sems.at[step]
        )

    for step in range(steps):
        load(step).start()
    at = lax.broadcasted_iota(jnp.int32, (rows, rows), 0)
    source = lax.rem(at, slab) * nvib + at // slab
    pick = (lax.broadcasted_iota(jnp.int32, (rows, rows), 1) == source).astype(BF16)

    keep = (where_ref[2] > 0).astype(F32)
    ce = coup_ref[...].astype(F32) * keep
    lines = [ce[:, i * LANES : (i + 1) * LANES] for i in range(chan_rows)]
    lines.append(jnp.zeros((1, LANES), F32) + where_ref[3].astype(F32))
    fill = -(chan_rows + 1) % 8
    if fill:
        lines.append(jnp.zeros((fill, LANES), F32))
    tile = jnp.concatenate(lines, axis=0).astype(BF16)
    for v in range(nvib):
        ready[v, chan_rows * slab :, :] = tile

    for step in range(steps):
        load(step).wait()
        here = wide[:, step * STEP : (step + 1) * STEP].astype(BF16)
        moved = jnp.dot(pick, here, preferred_element_type=F32)
        moved = moved.astype(BF16).reshape(nvib, slab, STEP)
        for i in range(STEP // LANES):
            row = step * tall + i * slab
            ready[:, row : row + slab, :] = moved[:, :, i * LANES : (i + 1) * LANES]
        save(step).start()
    for step in range(steps):
        save(step).wait()


def unpack(dims, msg_ref, out_ref, wide, sems):
    slab, nvib, steps = dims
    rows = slab * nvib
    tall = STEP // LANES * slab

    def save(step):
        cols = pl.ds(step * STEP, STEP)
        return pltpu.make_async_copy(wide.at[:, cols], out_ref.at[:, cols], sems.at[step])

    at = lax.broadcasted_iota(jnp.int32, (rows, rows), 0)
    source = lax.rem(at, nvib) * slab + at // nvib
    pick = (lax.broadcasted_iota(jnp.int32, (rows, rows), 1) == source).astype(BF16)
    for step in range(steps):
        parts = [
            msg_ref[:, row : row + slab, :].reshape(rows, LANES)
            for row in range(step * tall, (step + 1) * tall, slab)
        ]
        wide[:, step * STEP : (step + 1) * STEP] = jnp.dot(
            pick, jnp.concatenate(parts, axis=1), preferred_element_type=F32
        )
        save(step).start()
    for step in range(steps):
        save(step).wait()


def rows_of(ref, k):
    block = ref[k]
    return block.reshape(block.shape[0] * block.shape[1], block.shape[2])


def rows_in(ref, k, slab, nang):
    return jnp.concatenate(
        [
            jnp.concatenate(
                [ref[k, y, i * slab : (i + 1) * slab, :] for i in range(nang // LANES)], axis=1
            )
            for y in range(ref.shape[1])
        ],
        axis=0,
    )


def angular(dims, first_step, *refs):
    blocks, ygroups, slab, nang, nquad = dims
    msg_ref, page_ref, basis_ref = refs[:3]
    if first_step:
        out_ref, own_ref, held = refs[3:6]
        here_ref = None
        scaled, pot, radial, coup, sems = refs[6:]
        basis_hbm, basis_ref = basis_ref, held

        def load(qi):
            cols = pl.ds(qi * STEP, STEP)
            return pltpu.make_async_copy(basis_hbm.at[:, cols], held.at[:, cols], sems.at[qi])

        for qi in range(nquad // STEP):
            load(qi).start()
    else:
        own_ref, here_ref, out_ref = refs[3:6]
        scaled, pot, radial, coup = refs[6:]
    nrad = ygroups * slab
    chan_rows = nang // LANES
    base = chan_rows * slab
    pot[...] = page_ref[:, :, :nquad].reshape(nrad, nquad).astype(F32)
    extra = page_ref[:, :, nquad:].reshape(nrad, LANES).astype(F32)
    factor = jnp.broadcast_to(extra[:, 0:1] + extra[:, 1:2], (nrad, STEP))
    for k in range(blocks):
        page = msg_ref[k, 0, base : base + -(-(chan_rows + 1) // 8) * 8, :].astype(F32)
        coup[k] = jnp.concatenate([page[i : i + 1, :] for i in range(chan_rows)], axis=1)
        kvalue = page[chan_rows : chan_rows + 1, 0:1]
        radial[k] = (-2.0 * kvalue * kvalue) * factor
        if first_step:
            own_ref[k] = rows_in(msg_ref, k, slab, nang).reshape(ygroups, slab, nang)

    @pl.loop(0, nquad // STEP)
    def _(qi):
        cols = pl.ds(pl.multiple_of(qi * STEP, STEP), STEP)
        if first_step:
            pltpu.make_async_copy(basis_hbm.at[:, cols], held.at[:, cols], sems.at[qi]).wait()
        grid = jnp.dot(
            own_ref[...].reshape(blocks * nrad, nang),
            basis_ref[:, cols],
            preferred_element_type=F32,
        )
        prod = grid.reshape(blocks, nrad, STEP) * pot[:, cols][None]
        scaled[:, cols] = prod.astype(BF16).reshape(blocks * nrad, STEP)

    @pl.loop(0, nang // STEP)
    def _(ji):
        cols = pl.ds(pl.multiple_of(ji * STEP, STEP), STEP)
        ang = lax.dot_general(
            scaled[...], basis_ref[cols, :], NT, preferred_element_type=F32
        ).reshape(blocks, nrad, STEP)

        def block(k):
            return own_ref[k, :, :, cols].reshape(nrad, STEP).astype(F32)

        for k in range(blocks):
            here = block(k) if here_ref is None else here_ref[k, :, cols]
            total = ang[k] + radial[k] * here
            if k + 1 < blocks:
                total += coup[k, :, cols] * block(k + 1)
            if k > 0:
                total += coup[k - 1, :, cols] * block(k - 1)
            out_ref[k, :, cols] = total


def finish(dims, rotated, n, *refs):
    blocks, ygroups, groups, slab, nang, nquad, nchan = dims
    last = n == ITERS
    where_ref, page_ref, kin_ref, part_ref, own_ref, got_ref = refs[:6]
    rest = list(refs[6:])
    prev_ref = rest.pop(0) if n > 1 else None
    if last:
        rad_ref, vib_ref, proj_ref, out_ref, final = rest
    else:
        next_ref, full_ref = rest
    core = where_ref[0]
    nrad = ygroups * slab
    every = nrad * groups

    spot = lax.broadcasted_iota(jnp.int32, (every, every), 1)
    slot = spot // nrad
    if rotated:
        slot = lax.rem(slot + core, groups)
    true_at = (lax.rem(spot // slab, ygroups) * groups + slot) * slab + lax.rem(spot, slab)
    pick = (lax.broadcasted_iota(jnp.int32, (every, every), 0) == true_at).astype(BF16)
    lines = [
        kin_ref[pl.ds(pl.multiple_of((y * groups + core) * slab, slab), slab), :]
        for y in range(ygroups)
    ]
    kin_rows = jnp.dot(
        jnp.concatenate(lines, axis=0), pick, preferred_element_type=F32
    ).astype(BF16)

    def other(ref, k):
        return rows_in(ref, k, slab, nang) if n == 1 else rows_of(ref, k)

    extra = page_ref[:, :, nquad:].reshape(nrad, LANES).astype(F32)
    damp = jnp.broadcast_to(extra[:, 2:3] + extra[:, 3:4], (nrad, nang))
    for k in range(blocks):
        if rotated:
            pieces = [rows_of(own_ref, k), other(got_ref, k)]
        else:
            pieces = [other(got_ref.at[g], k) for g in range(groups)]
        near = jnp.concatenate(pieces, axis=0)
        total = part_ref[k] + jnp.dot(kin_rows, near, preferred_element_type=F32)
        if n == 1:
            new = damp * total
        else:
            if n == 2:
                before = rows_of(prev_ref, k).astype(F32)
            else:
                before = prev_ref[k]
            new = damp * (2.0 * total - damp * before)
        if last:
            final[k] = new.astype(BF16)
        else:
            full_ref[k] = new
            next_ref[k] = new.astype(BF16).reshape(ygroups, slab, nang)
    if not last:
        return

    span = nchan // ygroups
    height = 2 * (span // LANES)
    base = nang // LANES * slab
    rows_at = lax.broadcasted_iota(jnp.int32, (nrad, span), 0)
    rows_at = (rows_at // slab * groups + core) * slab + lax.rem(rows_at, slab)
    for y in range(ygroups):
        chan = pl.ds(y * span, span)
        table = lax.dot_general(
            final[...].reshape(blocks * nrad, nang),
            proj_ref[chan, :],
            NT,
            preferred_element_type=F32,
        ).reshape(blocks, nrad, span)
        hit = (rows_at == rad_ref[:, chan]) & (vib_ref[:, chan] == where_ref[1])
        for k in range(blocks):
            amp = jnp.sum(jnp.where(hit, table[k], 0.0), axis=0, keepdims=True)
            high = amp.astype(BF16).astype(F32)
            low = amp - high
            tile = [part[:, s : s + LANES] for part in (high, low) for s in range(0, span, LANES)]
            out_ref[k, y, base : base + height, :] = jnp.concatenate(tile, axis=0).astype(BF16)
            for i in range(nang // LANES):
                out_ref[k, y, i * slab : (i + 1) * slab, :] = final[
                    k, y * slab : (y + 1) * slab, i * LANES : (i + 1) * LANES
                ]


def in_hbm(array):
    return pltpu.with_memory_space_constraint(array, pltpu.HBM)


def two_halves(value):
    high = lax.reduce_precision(value, 8, 7)
    return high.astype(BF16), (value - high).astype(BF16)


def per_device(
    psi_start,
    potential,
    basis,
    kinetic,
    radial_factor,
    damping,
    coupling,
    helicity,
    chan_rad,
    chan_vib,
    projector,
):
    _, slab, nvib, nang = psi_start.shape
    nquad = basis.shape[1]
    nchan = projector.shape[0]
    blocks = lax.axis_size("hel")
    ygroups = lax.axis_size("y")
    groups = lax.axis_size("c")
    hel_index = lax.axis_index("hel")
    y_index = lax.axis_index("y")
    core = lax.axis_index("c")
    swap = [(0, 1), (1, 0)]
    nrad = ygroups * slab
    rotated = groups == 2

    rf_high, rf_low = two_halves(radial_factor)
    dp_high, dp_low = two_halves(damping)
    extra = jnp.stack([rf_high, rf_low, dp_high, dp_low], axis=1)
    extra = jnp.pad(extra, ((0, 0), (0, LANES - extra.shape[1])))
    mine = lax.dynamic_slice_in_dim(potential, hel_index * ygroups, ygroups, 1).astype(BF16)
    pages = jnp.concatenate(
        [jnp.swapaxes(mine, 0, 1), jnp.broadcast_to(extra[None], (ygroups,) + extra.shape)],
        axis=2,
    )
    if ygroups == 2:
        kept = lax.dynamic_index_in_dim(pages, y_index, 0, False)
        got = lax.ppermute(lax.dynamic_index_in_dim(pages, 1 - y_index, 0, False), "y", swap)
        pages = jnp.stack(
            [jnp.where(y_index == 0, kept, got), jnp.where(y_index == 0, got, kept)]
        )
    elif ygroups > 2:
        pages = lax.all_to_all(pages, "y", 0, 0, tiled=True)

    chan_rows = nang // LANES
    base = chan_rows * slab
    where = jnp.stack(
        [
            core,
            hel_index * ygroups + y_index,
            (hel_index < blocks - 1).astype(jnp.int32),
            helicity[0],
        ]
    ).astype(jnp.int32)
    steps = nang // STEP
    height = base + -(-(chan_rows + 1) // 8) * 8
    send = pl.pallas_call(
        functools.partial(pack, (slab, nvib, chan_rows, steps)),
        out_shape=jax.ShapeDtypeStruct((nvib, height, LANES), BF16),
        in_specs=[SMEM, HBM, VMEM],
        out_specs=HBM,
        scratch_shapes=[
            pltpu.VMEM((slab * nvib, nang), F32),
            pltpu.VMEM((nvib, height, LANES), BF16),
            pltpu.SemaphoreType.DMA((steps,)),
            pltpu.SemaphoreType.DMA((steps,)),
        ],
        compiler_params=PARAMS,
        name="pack",
    )(where, in_hbm(psi_start.reshape(slab * nvib, nang)), coupling)
    message = lax.all_to_all(send, ("hel", "y"), 0, 0, tiled=True)
    message = message.reshape(blocks, ygroups, height, LANES)
    basis = in_hbm(basis)
    flops = 4 * blocks * nrad * nang * nquad
    cost = pl.CostEstimate(flops=flops, bytes_accessed=8 * 1024 * 1024, transcendentals=0)
    sent, own, full = message, None, None
    out_height = base + 2 * (nchan // ygroups // LANES)
    block_type = jax.ShapeDtypeStruct((blocks, ygroups, slab, nang), BF16)
    full_type = jax.ShapeDtypeStruct((blocks, nrad, nang), F32)
    held = [pltpu.SemaphoreType.DMA((nquad // STEP,))]
    basis_type = jax.ShapeDtypeStruct(basis.shape, basis.dtype)
    before = []
    for n in range(1, ITERS + 1):
        if rotated:
            got = lax.ppermute(sent, "c", swap)
        else:
            got = lax.all_gather(sent, "c", axis=0, tiled=False)
        extra_in = [] if n == 1 else [own, full]
        part = pl.pallas_call(
            functools.partial(angular, (blocks, ygroups, slab, nang, nquad), n == 1),
            out_shape=[full_type, block_type, basis_type] if n == 1 else full_type,
            in_specs=[VMEM, VMEM, HBM if n == 1 else VMEM] + [VMEM] * len(extra_in),
            out_specs=[VMEM] * 3 if n == 1 else VMEM,
            scratch_shapes=[
                pltpu.VMEM((blocks * nrad, nquad), BF16),
                pltpu.VMEM((nrad, nquad), F32),
                pltpu.VMEM((blocks, nrad, STEP), F32),
                pltpu.VMEM((blocks, 1, nang), F32),
            ]
            + held * (n == 1),
            compiler_params=PARAMS,
            cost_estimate=cost,
            name=f"angular{n}",
        )(message, pages, basis, *extra_in)
        if n == 1:
            part, own, basis = part
        operands = [where, pages, kinetic, part, own, got] + before[-1:]
        scratch = []
        if n == ITERS:
            operands += [chan_rad[None], chan_vib[None], projector]
            outs = jax.ShapeDtypeStruct((blocks, ygroups, out_height, LANES), BF16)
            scratch = [pltpu.VMEM((blocks, nrad, nang), BF16)]
        else:
            outs = [block_type, full_type]
        before.append(own if n == 1 else full)
        done = pl.pallas_call(
            functools.partial(
                finish, (blocks, ygroups, groups, slab, nang, nquad, nchan), rotated, n
            ),
            out_shape=outs,
            in_specs=[SMEM] + [VMEM] * (len(operands) - 1),
            out_specs=VMEM if n == ITERS else [VMEM, VMEM],
            scratch_shapes=scratch,
            compiler_params=PARAMS,
            name=f"finish{n}",
        )(*operands)
        if n < ITERS:
            own, full = done
            sent = own

    back = done.reshape(blocks * ygroups, out_height, LANES)
    home = lax.all_to_all(back, ("hel", "y"), 0, 0, tiled=True)
    span = nchan // ygroups
    pieces = span // LANES
    lines = jnp.sum(home[:, base:, :].astype(F32), axis=0)
    shared = (lines[:pieces] + lines[pieces:]).reshape(groups, 1, span // groups)
    amplitude = lax.dynamic_index_in_dim(shared, core, 0, False)
    if rotated:
        amplitude += lax.ppermute(lax.dynamic_index_in_dim(shared, 1 - core, 0, False), "c", swap)
    else:
        amplitude = lax.dynamic_index_in_dim(lax.psum(shared, "c"), core, 0, False)
    psi_final = pl.pallas_call(
        functools.partial(unpack, (slab, nvib, steps)),
        out_shape=jax.ShapeDtypeStruct((slab * nvib, nang), F32),
        in_specs=[VMEM],
        out_specs=HBM,
        scratch_shapes=[
            pltpu.VMEM((slab * nvib, nang), F32),
            pltpu.SemaphoreType.DMA((steps,)),
        ],
        compiler_params=PARAMS,
        name="unpack",
    )(home)
    return (psi_final.reshape(1, slab, nvib, nang), amplitude)


def solution(mesh):
    nhel, nrad = mesh.shape["hel"], mesh.shape["rad"]

    def run(*args):
        nvib = args[0].shape[2]
        groups = nhel * nrad // nvib
        fine = Mesh(mesh.devices.reshape(nhel, nrad // groups, groups), ("hel", "y", "c"))
        rad = ("y", "c")
        placed = (
            P("hel", rad, None, None),
            P(rad, None, None),
            P(),
            P(),
            P(rad),
            P(rad),
            P("hel", None),
            P("hel"),
            P(),
            P(),
            P(),
        )
        return jax.shard_map(
            per_device,
            mesh=fine,
            in_specs=placed,
            out_specs=(P("hel", rad, None, None), P("hel", rad)),
            check_vma=False,
        )(*args)

    return run
```

```python
import functools

import jax
import jax.numpy as jnp
from jax import lax
from jax.experimental import pallas as pl
from jax.experimental.pallas import tpu as pltpu
from jax.sharding import Mesh
from jax.sharding import PartitionSpec as P

ITERS = 3
LANES = 128
STEP = 256
WIDE = 384
SMALL = 8
NT = (((1,), (1,)), ((), ()))
F32 = jnp.float32
BF16 = jnp.bfloat16
VMEM = pl.BlockSpec(memory_space=pltpu.VMEM)
HBM = pl.BlockSpec(memory_space=pltpu.HBM)
PARAMS = pltpu.CompilerParams(vmem_limit_bytes=24 * 1024 * 1024)


def in_hbm(array):
    return pltpu.with_memory_space_constraint(array, pltpu.HBM)


def moved_rows(rows, major):
    minor = rows // major
    at = lax.broadcasted_iota(jnp.int32, (1, rows), 1)
    dest = lax.rem(at, minor) * major + at // minor
    return (lax.broadcasted_iota(jnp.int32, (rows, rows), 0) == dest).astype(BF16)


def pack(
    dims, psi_ref, pot_ref, coup_ref, hel_ref, rf_ref, dp_ref, out_ref,
    wide, ready, coup, rf, dp, in_sems, out_sems, sems,
):
    slab, nvib, nang, share, blocks = dims
    near = lax.axis_size("hl")
    here = lax.axis_index("hl")
    is_last = lax.axis_index("g") * near + here == blocks - 1
    tall = WIDE // LANES * slab
    chunks = (nang + share) // WIDE
    height = (nang + share) // LANES * slab

    def load(i):
        if i * WIDE < share:
            first = pl.multiple_of(here * share + i * WIDE, LANES)
            source = pot_ref.at[:, pl.ds(first, WIDE)]
        else:
            source = psi_ref.at[:, pl.ds(i * WIDE - share, WIDE)]
        return pltpu.make_async_copy(source, wide.at[i], in_sems.at[i])

    def save(i):
        size = tall + (SMALL if i == chunks - 1 else 0)
        lines = pl.ds(i * tall, size)
        return pltpu.make_async_copy(
            ready.at[:, lines, :], out_ref.at[:, lines, :], out_sems.at[i]
        )

    small = [
        pltpu.make_async_copy(source, target, sems.at[i])
        for i, (source, target) in enumerate(
            [(coup_ref, coup), (rf_ref, rf), (dp_ref, dp)]
        )
    ]
    for i in range(chunks):
        load(i).start()
    for copy in small:
        copy.start()
    pick = moved_rows(slab * nvib, nvib)

    for copy in small:
        copy.wait()
    ce = jnp.where(is_last, 0.0, coup[...].astype(F32))
    lines = [ce[:, i * LANES : (i + 1) * LANES] for i in range(nang // LANES)]
    parts = []
    for value in (rf[...], dp[...]):
        high = value.astype(BF16).astype(F32)
        parts += [high, value - high]
    spread = (
        lax.rem(lax.broadcasted_iota(jnp.int32, (slab, LANES), 1), slab)
        == lax.broadcasted_iota(jnp.int32, (slab, LANES), 0)
    ).astype(BF16)
    filler = [jnp.zeros((SMALL - len(parts), slab), F32)]
    repeated = jnp.dot(
        jnp.concatenate(parts + filler, axis=0).astype(BF16), spread, preferred_element_type=F32
    )
    owner = lax.broadcasted_iota(jnp.int32, (SMALL, LANES), 1) // slab
    mine = owner == lax.broadcasted_iota(jnp.int32, (SMALL, LANES), 0)
    line = jnp.sum(jnp.where(mine, repeated, 0.0), axis=0, keepdims=True)
    lane = lax.broadcasted_iota(jnp.int32, (1, LANES), 1)
    lines.append(jnp.where(lane == LANES - 1, hel_ref[...].astype(F32), line))
    if len(lines) < SMALL:
        lines.append(jnp.zeros((SMALL - len(lines), LANES), F32))
    tile = jnp.concatenate(lines, axis=0).astype(BF16)
    for v in range(nvib):
        ready[v, height:, :] = tile

    for i in range(chunks):
        load(i).wait()
        moved = jnp.dot(pick, wide[i].astype(BF16), preferred_element_type=F32)
        moved = moved.astype(BF16).reshape(nvib, slab, WIDE)
        for t in range(WIDE // LANES):
            row = i * tall + t * slab
            ready[:, row : row + slab, :] = moved[:, :, t * LANES : (t + 1) * LANES]
        save(i).start()
    for i in range(chunks):
        save(i).wait()


def unpack(dims, msg_ref, out_ref, amp_ref, wide, sems):
    slab, nvib, nang, pieces = dims
    rows = slab * nvib
    tall = STEP // LANES * slab
    steps = nang // STEP

    def save(step):
        cols = pl.ds(step * STEP, STEP)
        return pltpu.make_async_copy(wide.at[:, cols], out_ref.at[:, cols], sems.at[step])

    pick = moved_rows(rows, slab)
    for step in range(steps):
        parts = [
            msg_ref[:, row : row + slab, :].reshape(rows, LANES)
            for row in range(step * tall, (step + 1) * tall, slab)
        ]
        wide[:, step * STEP : (step + 1) * STEP] = jnp.dot(
            pick, jnp.concatenate(parts, axis=1), preferred_element_type=F32
        )
        save(step).start()
    base = nang // LANES * slab
    lines = jnp.sum(msg_ref[:, base : base + SMALL, :].astype(F32), axis=0)
    lines = [lines[i : i + 1] + lines[pieces + i : pieces + i + 1] for i in range(pieces)]
    amp_ref[...] = jnp.concatenate(lines, axis=1)[:, : amp_ref.shape[1]]
    for step in range(steps):
        save(step).wait()


def rows_in(ref, first, count, slab, nang, base):
    return jnp.concatenate(
        [
            jnp.concatenate(
                [ref[m, base + i * slab : base + (i + 1) * slab, :] for i in range(nang // LANES)],
                axis=1,
            )
            for m in range(first, first + count)
        ],
        axis=0,
    )


def coupling_in(ref, m, base, nang):
    page = ref[m, base : base + SMALL, :].astype(F32)
    lines = [page[i : i + 1, :] for i in range(nang // LANES)]
    return jnp.concatenate(lines, axis=1), page[len(lines) : len(lines) + 1, :]


def unfold(dims, msg_ref, src, pot, radii, khat, coup):
    own, nslab, slab, nang, nquad = dims
    share = nquad // own
    top = share // LANES * slab
    base = top + nang // LANES * slab
    lane = lax.broadcasted_iota(jnp.int32, (slab, LANES), 1)
    row = lax.broadcasted_iota(jnp.int32, (slab, LANES), 0)
    for k in range(own):
        src[k] = rows_in(msg_ref, k * nslab, nslab, slab, nang, top)
        for m in range(nslab):
            for t in range(share // LANES):
                cols = pl.ds(k * share + t * LANES, LANES)
                tile = msg_ref[k * nslab + m, t * slab : (t + 1) * slab, :]
                pot[m * slab : (m + 1) * slab, cols] = tile.astype(F32)
        coup[k], line = coupling_in(msg_ref, k * nslab, base, nang)
        value = line[:, LANES - 1 :]
        khat[k] = jnp.broadcast_to(-2.0 * value * value, (1, LANES))
    for m in range(nslab):
        _, line = coupling_in(msg_ref, m, base, nang)
        for i in range(2):
            hit = (lane == row + 2 * i * slab) | (lane == row + (2 * i + 1) * slab)
            value = jnp.sum(jnp.where(hit, line, 0.0), axis=1, keepdims=True)
            radii[i, m * slab : (m + 1) * slab, :] = jnp.broadcast_to(value, (slab, LANES))


def advance(dims, n, *refs):
    own, nslab, slab, nang, nquad = dims
    nrad = nslab * slab
    full, before = None, None
    if n == 1:
        msg_ref, basis_hbm, kin_ref = refs[:3]
        new_ref, newb_ref, src, basis, pot, radii, khat, coup, scaled, sems = refs[3:]

        def load(qi):
            cols = pl.ds(qi * STEP, STEP)
            return pltpu.make_async_copy(basis_hbm.at[:, cols], basis.at[:, cols], sems.at[qi])

        for qi in range(nquad // STEP):
            load(qi).start()
        unfold(dims, msg_ref, src, pot, radii, khat, coup)
    else:
        src, full, before, basis, kin_ref, pot, radii, khat, coup = refs[:9]
        new_ref, newb_ref, scaled = refs[9:]

    @pl.loop(0, nquad // STEP)
    def _(qi):
        cols = pl.ds(pl.multiple_of(qi * STEP, STEP), STEP)
        if n == 1:
            pltpu.make_async_copy(basis_hbm.at[:, cols], basis.at[:, cols], sems.at[qi]).wait()
        grid = jnp.dot(
            src[...].reshape(own * nrad, nang), basis[:, cols], preferred_element_type=F32
        )
        prod = grid.reshape(own, nrad, STEP) * pot[:, cols][None]
        scaled[:, cols] = prod.astype(BF16).reshape(own * nrad, STEP)

    factor = jnp.concatenate([radii[0]] * (STEP // LANES), axis=1)
    damp = jnp.concatenate([radii[1]] * (STEP // LANES), axis=1)

    @pl.loop(0, nang // STEP)
    def _(ji):
        cols = pl.ds(pl.multiple_of(ji * STEP, STEP), STEP)
        ang = lax.dot_general(
            scaled[...], basis[cols, :], NT, preferred_element_type=F32
        ).reshape(own, nrad, STEP)
        for k in range(own):
            here = src[k, :, cols]
            total = ang[k] + jnp.dot(kin_ref[...], here, preferred_element_type=F32)
            value = here.astype(F32) if full is None else full[k, :, cols]
            total += jnp.concatenate([khat[k]] * (STEP // LANES), axis=1) * factor * value
            if k + 1 < own:
                total += coup[k, :, cols] * src[k + 1, :, cols].astype(F32)
            if k > 0:
                total += coup[k - 1, :, cols] * src[k - 1, :, cols].astype(F32)
            if n == 1:
                new = damp * total
            else:
                new = damp * (2.0 * total - damp * before[k, :, cols].astype(F32))
            new_ref[k, :, cols] = new
            newb_ref[k, :, cols] = new.astype(BF16)


def edges(dims, n, *refs):
    own, nslab, slab, nang, nquad, nchan, count = dims
    last = n == ITERS
    nrad = nslab * slab
    got_refs, rest = refs[:count], list(refs[count:])
    new_ref, newb_ref, radii, coup = rest[:4]
    rest = rest[4:]
    group = lax.axis_index("g")
    base = nang // LANES * slab
    if n == 1:
        newf_out, newb_out, *edge_outs, ce_out = rest
    elif last:
        ce_ref, rad_ref, vib_ref, proj_ref, out_ref, newb_out = rest
        newf_out = None
    else:
        ce_ref, newf_out, newb_out, *edge_outs = rest

    if count == 1:
        targets = [jnp.where(group == 0, own - 1, 0)]
    else:
        targets = [own - 1, 0]
    newb_out[...] = newb_ref[...]
    if not last:
        newf_out[...] = new_ref[...]
    scale = radii[1] if n == 1 else 2.0 * radii[1]
    scale = jnp.concatenate([scale] * (nang // LANES), axis=1)
    for i, (got, target) in enumerate(zip(got_refs, targets)):
        if n == 1:
            block = rows_in(got, 0, nslab, slab, nang, 0).astype(F32)
            theirs, _ = coupling_in(got, 0, base, nang)
            if count == 1:
                ce = jnp.where(group == 0, coup[own - 1], theirs)
            else:
                ce = coup[own - 1] if i == 0 else theirs
            ce_out[i] = ce
        else:
            block = got[...].astype(F32)
            ce = ce_ref[i]
        fixed = (new_ref[target] if i == 0 or own > 1 else fixed) + scale * (ce * block)
        if not last:
            newf_out[target] = fixed
        newb_out[target] = fixed.astype(BF16)
    if not last:
        for edge, target in zip(edge_outs, targets):
            edge[...] = newb_out[target]
        return

    chan = nchan // nslab
    pieces = -(-chan // LANES)
    high_at = nang // LANES * slab
    vib = lax.axis_index("hl") * nslab + lax.axis_index("rad")
    rows_at = lax.broadcasted_iota(jnp.int32, (nrad, chan), 0)
    final = newb_out[...].reshape(own * nrad, nang)
    for m in range(nslab):
        cols = slice(m * chan, (m + 1) * chan)
        table = lax.dot_general(
            final, proj_ref[cols, :], NT, preferred_element_type=F32
        ).reshape(own, nrad, chan)
        hit = (rows_at == rad_ref[:, cols]) & (vib_ref[:, cols] == vib)
        for k in range(own):
            amp = jnp.sum(jnp.where(hit, table[k], 0.0), axis=0, keepdims=True)
            if pieces * LANES > chan:
                amp = jnp.concatenate([amp, jnp.zeros((1, pieces * LANES - chan), F32)], axis=1)
            high = amp.astype(BF16).astype(F32)
            tile = [
                part[:, s * LANES : (s + 1) * LANES]
                for part in (high, amp - high)
                for s in range(pieces)
            ]
            if len(tile) < SMALL:
                tile.append(jnp.zeros((SMALL - len(tile), LANES), F32))
            to = k * nslab + m
            out_ref[to, high_at : high_at + SMALL, :] = jnp.concatenate(tile, axis=0).astype(BF16)
            for t in range(nang // LANES):
                out_ref[to, t * slab : (t + 1) * slab, :] = newb_out[
                    k, m * slab : (m + 1) * slab, t * LANES : (t + 1) * LANES
                ]


def per_device(
    psi_start,
    potential,
    basis,
    kinetic,
    radial_factor,
    damping,
    coupling,
    helicity,
    chan_rad,
    chan_vib,
    projector,
):
    _, slab, nvib, nang = psi_start.shape
    nquad = basis.shape[1]
    nchan = projector.shape[0]
    groups = lax.axis_size("g")
    own = lax.axis_size("hl")
    nslab = lax.axis_size("rad")
    blocks = groups * own
    group = lax.axis_index("g")
    nrad = nslab * slab
    share = nquad // own
    chunks = (nang + share) // WIDE
    height = (nang + share) // LANES * slab + SMALL
    shape = jax.ShapeDtypeStruct

    send = pl.pallas_call(
        functools.partial(pack, (slab, nvib, nang, share, blocks)),
        out_shape=shape((nvib, height, LANES), BF16),
        in_specs=[HBM] * 3 + [VMEM] + [HBM] * 2,
        out_specs=HBM,
        scratch_shapes=[
            pltpu.VMEM((chunks, slab * nvib, WIDE), F32),
            pltpu.VMEM((nvib, height, LANES), BF16),
            pltpu.VMEM((1, nang), BF16),
            pltpu.VMEM((1, slab), F32),
            pltpu.VMEM((1, slab), F32),
            pltpu.SemaphoreType.DMA((chunks,)),
            pltpu.SemaphoreType.DMA((chunks,)),
            pltpu.SemaphoreType.DMA((3,)),
        ],
        compiler_params=PARAMS,
        name="pack",
    )(
        in_hbm(psi_start.reshape(slab * nvib, nang)),
        in_hbm(potential.reshape(slab * nvib, nquad)),
        in_hbm(coupling),
        helicity[None],
        in_hbm(radial_factor[None]),
        in_hbm(damping[None]),
    )
    message = lax.all_to_all(send, ("hl", "rad"), 0, 0, tiled=True)

    count = 1 if groups == 2 else 2
    up = [(i, i + 1) for i in range(groups - 1)]
    down = [(i + 1, i) for i in range(groups - 1)]

    def swap(parts):
        if count == 1:
            return [lax.ppermute(parts[0], "g", [(0, 1), (1, 0)])]
        return [lax.ppermute(parts[1], "g", down), lax.ppermute(parts[0], "g", up)]

    rows = message[:, share // LANES * slab :]
    if count == 1:
        first = jnp.where(group == 0, own - 1, 0) * nslab
        edge = [lax.dynamic_slice_in_dim(rows, first, nslab, 0)]
    else:
        edge = [rows[(own - 1) * nslab :], rows[:nslab]]

    cost = pl.CostEstimate(
        flops=4 * own * nrad * nang * nquad, bytes_accessed=8 * 1024 * 1024, transcendentals=0
    )
    full_type = shape((own, nrad, nang), F32)
    block_type = shape((own, nrad, nang), BF16)
    edge_types = [shape((nrad, nang), BF16)] * count
    scaled = pltpu.VMEM((own * nrad, nquad), BF16)
    dims = (own, nslab, slab, nang, nquad)
    full = block = before = None
    for n in range(1, ITERS + 1):
        got = swap(edge)
        if n == 1:
            outs = [
                full_type,
                block_type,
                block_type,
                shape(basis.shape, BF16),
                shape((nrad, nquad), F32),
                shape((2, nrad, LANES), F32),
                shape((own, 1, LANES), F32),
                shape((own, 1, nang), F32),
            ]
            operands = [message, in_hbm(basis), kinetic]
            specs = [VMEM, HBM, VMEM]
            scratch = [scaled, pltpu.SemaphoreType.DMA((nquad // STEP,))]
        else:
            outs = [full_type, block_type]
            operands = [block, full, before, basis, kinetic, pot, radii, khat, coup]
            specs = [VMEM] * len(operands)
            scratch = [scaled]
        done = pl.pallas_call(
            functools.partial(advance, dims, n),
            out_shape=outs,
            in_specs=specs,
            out_specs=[VMEM] * len(outs),
            scratch_shapes=scratch,
            compiler_params=PARAMS,
            cost_estimate=cost,
            name=f"advance{n}",
        )(*operands)
        if n == 1:
            new, newb, before, basis, pot, radii, khat, coup = done
        else:
            before = full
            new, newb = done

        operands = got + [new, newb, radii, coup]
        outs = [full_type, block_type]
        scratch = []
        if n == 1:
            outs += edge_types + [shape((count, 1, nang), F32)]
        elif n == ITERS:
            operands += [ce, chan_rad[None], chan_vib[None], projector]
            outs = [shape((own * nslab, nang // LANES * slab + SMALL, LANES), BF16)]
            scratch = [pltpu.VMEM((own, nrad, nang), BF16)]
        else:
            operands += [ce]
            outs += edge_types
        done = pl.pallas_call(
            functools.partial(edges, dims + (nchan, count), n),
            out_shape=outs,
            in_specs=[VMEM] * len(operands),
            out_specs=[VMEM] * len(outs),
            scratch_shapes=scratch,
            compiler_params=PARAMS,
            name=f"edges{n}",
        )(*operands)
        if n == ITERS:
            break
        full, block = done[:2]
        edge = list(done[2 : 2 + count])
        if n == 1:
            ce = done[-1]

    home = lax.all_to_all(done[-1], ("hl", "rad"), 0, 0, tiled=True)
    chan = nchan // nslab
    psi_final, amplitude = pl.pallas_call(
        functools.partial(unpack, (slab, nvib, nang, -(-chan // LANES))),
        out_shape=[shape((slab * nvib, nang), F32), shape((1, chan), F32)],
        in_specs=[VMEM],
        out_specs=[HBM, VMEM],
        scratch_shapes=[
            pltpu.VMEM((slab * nvib, nang), F32),
            pltpu.SemaphoreType.DMA((nang // STEP,)),
        ],
        compiler_params=PARAMS,
        name="unpack",
    )(home)
    return (psi_final.reshape(1, slab, nvib, nang), amplitude)


def solution(mesh):
    nhel, nrad = mesh.shape["hel"], mesh.shape["rad"]

    def run(*args):
        nvib = args[0].shape[2]
        groups = nhel * nrad // nvib
        fine = Mesh(mesh.devices.reshape(groups, nhel // groups, nrad), ("g", "hl", "rad"))
        hel = ("g", "hl")
        placed = (
            P(hel, "rad", None, None),
            P("rad", None, None),
            P(),
            P(),
            P("rad"),
            P("rad"),
            P(hel, None),
            P(hel),
            P(),
            P(),
            P(),
        )
        return jax.shard_map(
            per_device,
            mesh=fine,
            in_specs=placed,
            out_specs=(P(hel, "rad", None, None), P(hel, "rad")),
            check_vma=False,
        )(*args)

    return run
```

```python
import functools

import jax
import jax.numpy as jnp
from jax import lax
from jax.experimental import pallas as pl
from jax.experimental.pallas import tpu as pltpu
from jax.sharding import Mesh
from jax.sharding import PartitionSpec as P

ITERS = 3
LANES = 128
STEP = 256
WIDE = 384
SMALL = 8
NT = (((1,), (1,)), ((), ()))
F32 = jnp.float32
BF16 = jnp.bfloat16
VMEM = pl.BlockSpec(memory_space=pltpu.VMEM)
HBM = pl.BlockSpec(memory_space=pltpu.HBM)
PARAMS = pltpu.CompilerParams(vmem_limit_bytes=24 * 1024 * 1024)


def in_hbm(array):
    return pltpu.with_memory_space_constraint(array, pltpu.HBM)


def moved_rows(rows, major):
    minor = rows // major
    at = lax.broadcasted_iota(jnp.int32, (1, rows), 1)
    dest = lax.rem(at, minor) * major + at // minor
    return (lax.broadcasted_iota(jnp.int32, (rows, rows), 0) == dest).astype(BF16)


def pack(
    dims, psi_ref, pot_ref, coup_ref, hel_ref, rf_ref, dp_ref, out_ref,
    wide, ready, coup, rf, dp, in_sems, out_sems, sems,
):
    slab, nvib, nang, share, blocks = dims
    near = lax.axis_size("hl")
    here = lax.axis_index("hl")
    is_last = lax.axis_index("g") * near + here == blocks - 1
    tall = WIDE // LANES * slab
    chunks = (nang + share) // WIDE
    height = (nang + share) // LANES * slab

    def load(i):
        if i * WIDE < share:
            first = pl.multiple_of(here * share + i * WIDE, LANES)
            source = pot_ref.at[:, pl.ds(first, WIDE)]
        else:
            source = psi_ref.at[:, pl.ds(i * WIDE - share, WIDE)]
        return pltpu.make_async_copy(source, wide.at[i], in_sems.at[i])

    def save(i):
        size = tall + (SMALL if i == chunks - 1 else 0)
        lines = pl.ds(i * tall, size)
        return pltpu.make_async_copy(
            ready.at[:, lines, :], out_ref.at[:, lines, :], out_sems.at[i]
        )

    small = [
        pltpu.make_async_copy(source, target, sems.at[i])
        for i, (source, target) in enumerate(
            [(coup_ref, coup), (rf_ref, rf), (dp_ref, dp)]
        )
    ]
    for i in range(chunks):
        load(i).start()
    for copy in small:
        copy.start()
    pick = moved_rows(slab * nvib, nvib)

    for copy in small:
        copy.wait()
    ce = jnp.where(is_last, 0.0, coup[...].astype(F32))
    lines = [ce[:, i * LANES : (i + 1) * LANES] for i in range(nang // LANES)]
    parts = []
    for value in (rf[...], dp[...]):
        high = value.astype(BF16).astype(F32)
        parts += [high, value - high]
    spread = (
        lax.rem(lax.broadcasted_iota(jnp.int32, (slab, LANES), 1), slab)
        == lax.broadcasted_iota(jnp.int32, (slab, LANES), 0)
    ).astype(BF16)
    filler = [jnp.zeros((SMALL - len(parts), slab), F32)]
    repeated = jnp.dot(
        jnp.concatenate(parts + filler, axis=0).astype(BF16), spread, preferred_element_type=F32
    )
    owner = lax.broadcasted_iota(jnp.int32, (SMALL, LANES), 1) // slab
    mine = owner == lax.broadcasted_iota(jnp.int32, (SMALL, LANES), 0)
    line = jnp.sum(jnp.where(mine, repeated, 0.0), axis=0, keepdims=True)
    lane = lax.broadcasted_iota(jnp.int32, (1, LANES), 1)
    lines.append(jnp.where(lane == LANES - 1, hel_ref[...].astype(F32), line))
    if len(lines) < SMALL:
        lines.append(jnp.zeros((SMALL - len(lines), LANES), F32))
    tile = jnp.concatenate(lines, axis=0).astype(BF16)
    for v in range(nvib):
        ready[v, height:, :] = tile

    for i in range(chunks):
        load(i).wait()
        moved = jnp.dot(pick, wide[i].astype(BF16), preferred_element_type=F32)
        moved = moved.astype(BF16).reshape(nvib, slab, WIDE)
        for t in range(WIDE // LANES):
            row = i * tall + t * slab
            ready[:, row : row + slab, :] = moved[:, :, t * LANES : (t + 1) * LANES]
        save(i).start()
    for i in range(chunks):
        save(i).wait()


def unpack(dims, msg_ref, out_ref, amp_ref, wide, sems):
    slab, nvib, nang, pieces = dims
    rows = slab * nvib
    tall = STEP // LANES * slab
    steps = nang // STEP

    def save(step):
        cols = pl.ds(step * STEP, STEP)
        return pltpu.make_async_copy(wide.at[:, cols], out_ref.at[:, cols], sems.at[step])

    pick = moved_rows(rows, slab)
    for step in range(steps):
        parts = [
            msg_ref[:, row : row + slab, :].reshape(rows, LANES)
            for row in range(step * tall, (step + 1) * tall, slab)
        ]
        wide[:, step * STEP : (step + 1) * STEP] = jnp.dot(
            pick, jnp.concatenate(parts, axis=1), preferred_element_type=F32
        )
        save(step).start()
    base = nang // LANES * slab
    lines = jnp.sum(msg_ref[:, base : base + SMALL, :].astype(F32), axis=0)
    lines = [lines[i : i + 1] + lines[pieces + i : pieces + i + 1] for i in range(pieces)]
    amp_ref[...] = jnp.concatenate(lines, axis=1)[:, : amp_ref.shape[1]]
    for step in range(steps):
        save(step).wait()


def rows_in(ref, first, count, slab, nang, base):
    return jnp.concatenate(
        [
            jnp.concatenate(
                [ref[m, base + i * slab : base + (i + 1) * slab, :] for i in range(nang // LANES)],
                axis=1,
            )
            for m in [first + i for i in range(count)]
        ],
        axis=0,
    )


def small_in(ref, m, base, nang):
    page = ref[m, base : base + SMALL, :].astype(F32)
    lines = [page[i : i + 1, :] for i in range(nang // LANES)]
    value = page[len(lines) : len(lines) + 1, LANES - 1 :]
    return jnp.concatenate(lines, axis=1), jnp.broadcast_to(-2.0 * value * value, (1, LANES))


def link(mirror, side, near, far):
    if mirror:
        return jnp.where(lax.axis_index("g") == 0, near, far)
    return far if side == 0 else near


def place(mirror, own, i):
    if mirror:
        return jnp.where(lax.axis_index("g") == 0, own - 1 - i, i)
    return i


def unfold(dims, msg_ref, src, pot, radii, khat, coup):
    own, nslab, slab, nang, nquad, mirror = dims
    share = nquad // own
    top = share // LANES * slab
    base = top + nang // LANES * slab
    lane = lax.broadcasted_iota(jnp.int32, (slab, LANES), 1)
    row = lax.broadcasted_iota(jnp.int32, (slab, LANES), 0)
    for k in range(own):
        for m in range(nslab):
            for t in range(share // LANES):
                cols = pl.ds(k * share + t * LANES, LANES)
                tile = msg_ref[k * nslab + m, t * slab : (t + 1) * slab, :]
                pot[m * slab : (m + 1) * slab, cols] = tile.astype(F32)
    for i in range(own):
        first = place(mirror, own, i) * nslab
        src[i] = rows_in(msg_ref, first, nslab, slab, nang, top)
        coup[i], khat[i] = small_in(msg_ref, first, base, nang)
    for m in range(nslab):
        page = msg_ref[m, base : base + SMALL, :].astype(F32)
        line = page[nang // LANES : nang // LANES + 1, :]
        for i in range(2):
            hit = (lane == row + 2 * i * slab) | (lane == row + (2 * i + 1) * slab)
            value = jnp.sum(jnp.where(hit, line, 0.0), axis=1, keepdims=True)
            radii[i, m * slab : (m + 1) * slab, :] = jnp.broadcast_to(value, (slab, LANES))


def wider(tile, size):
    return jnp.concatenate([tile] * (size // LANES), axis=1)


def advance(dims, sides, n, *refs):
    own, nslab, slab, nang, nquad, mirror = dims
    nrad = nslab * slab
    refs = list(refs)
    take = lambda count: [refs.pop(0) for _ in range(count)]
    edge_of = [0, own - 1]
    if n == 1:
        msg_ref, basis_hbm, kin_ref = take(3)
        new_ref, src, basis, pot, radii, khat, coup, chain = take(8)
        rows, scaled, sems = take(3)
        for qi in range(nquad // STEP):
            cols = pl.ds(qi * STEP, STEP)
            pltpu.make_async_copy(basis_hbm.at[:, cols], basis.at[:, cols], sems.at[qi]).start()
        unfold(dims, msg_ref, src, pot, radii, khat, coup)
        rows[...] = src[...]
        for i in range(own - 1):
            chain[i] = link(mirror, 0, coup[i + 1], coup[i])
    else:
        raw = take(sides)
        basis, kin_ref, pot, radii, khat, coup, chain = take(7)
        scale = wider(radii[1] if n == 2 else 2.0 * radii[1], nang)
        base = nang // LANES * slab
        if n == 2:
            part, first_b = take(2)
            full, block, new_ref, part_h, halo_b, halo_c, halo_k = take(7)
            rows, scaled, joint = take(3)
        else:
            part, first_b, first_f, halo_part, halo1_b, halo1_c, halo1_k, level1_b = take(8)
            new_ref, part_h, part_hh, halo_c = take(4)
            full, halo_b, halo_k, rows, scaled, joint = take(6)
        for i in range(own):
            value = part[i]
            full[i] = value
            rows[i] = value.astype(BF16)
        for s in range(sides):
            halo_b[s] = rows_in(raw[s], 0, nslab, slab, nang, 0)
            halo_c[s], halo_k[s] = small_in(raw[s], 0, base, nang)
            at = edge_of[s]
            if n == 2:
                joint[s, 0] = link(mirror, s, coup[at], halo_c[s])
                seen = halo_b[s]
                rows[own + s] = seen
            else:
                joint[s, 0] = link(mirror, s, coup[at], halo1_c[s])
                joint[s, 1] = link(mirror, s, halo1_c[s], halo_c[s])
                level = halo_part[s] + wider(radii[1], nang) * (
                    joint[s, 1] * halo_b[s].astype(F32)
                )
                seen = level.astype(BF16)
                rows[own + s] = seen
                rows[own + sides + s] = halo_b[s]
            value = full[at] + scale * (joint[s, 0] * seen.astype(F32))
            full[at] = value
            rows[at] = value.astype(BF16)
        if n == 2:
            block[...] = rows[:own]
    count = own + sides * (n - 1)

    @pl.loop(0, nquad // STEP)
    def _(qi):
        cols = pl.ds(pl.multiple_of(qi * STEP, STEP), STEP)
        if n == 1:
            pltpu.make_async_copy(basis_hbm.at[:, cols], basis.at[:, cols], sems.at[qi]).wait()
        grid = jnp.dot(
            rows[...].reshape(count * nrad, nang), basis[:, cols], preferred_element_type=F32
        )
        prod = grid.reshape(count, nrad, STEP) * pot[:, cols][None]
        scaled[:, cols] = prod.astype(BF16).reshape(count * nrad, STEP)

    factor = wider(radii[0], STEP)
    damp = wider(radii[1], STEP)

    @pl.loop(0, nang // STEP)
    def _(ji):
        cols = pl.ds(pl.multiple_of(ji * STEP, STEP), STEP)
        ang = lax.dot_general(
            scaled[...], basis[cols, :], NT, preferred_element_type=F32
        ).reshape(count, nrad, STEP)

        def local(i, hat, value):
            kin = jnp.dot(kin_ref[...], rows[i, :, cols], preferred_element_type=F32)
            return ang[i] + kin + wider(hat, STEP) * factor * value

        for i in range(own):
            value = rows[i, :, cols].astype(F32) if n == 1 else full[i, :, cols]
            total = local(i, khat[i], value)
            if i + 1 < own:
                total += chain[i, :, cols] * rows[i + 1, :, cols].astype(F32)
            if i > 0:
                total += chain[i - 1, :, cols] * rows[i - 1, :, cols].astype(F32)
            if n == 1:
                new_ref[i, :, cols] = damp * total
            else:
                before = first_b if n == 2 else first_f
                new_ref[i, :, cols] = damp * (
                    2.0 * total - damp * before[i, :, cols].astype(F32)
                )
        for s in range(sides if n > 1 else 0):
            at = edge_of[s]
            i = own + s
            hat = halo_k[s] if n == 2 else halo1_k[s]
            total = local(i, hat, rows[i, :, cols].astype(F32))
            edge_b = first_b if n == 2 else level1_b
            total += joint[s, 0, :, cols] * edge_b[at, :, cols].astype(F32)
            if n == 2:
                part_h[s, :, cols] = damp * total
                continue
            before = halo1_b[s, :, cols].astype(F32)
            part_h[s, :, cols] = damp * (2.0 * total - damp * before)
            i = own + sides + s
            total = local(i, halo_k[s], rows[i, :, cols].astype(F32))
            total += joint[s, 1, :, cols] * before
            part_hh[s, :, cols] = damp * total


def close(dims, sides, nchan, *refs):
    own, nslab, slab, nang, nquad, mirror = dims
    nrad = nslab * slab
    raw, refs = refs[:sides], refs[sides:]
    part, part_h, part_hh, halo1_c, halo2_c, coup, radii = refs[:7]
    rad_ref, vib_ref, proj_ref, out_ref, final = refs[7:]
    base = nang // LANES * slab
    damp = wider(radii[1], nang)
    for i in range(own):
        final[i] = part[i].astype(BF16)
    for s in range(sides):
        at = 0 if s == 0 else own - 1
        far = rows_in(raw[s], 0, nslab, slab, nang, 0).astype(F32)
        far_c, _ = small_in(raw[s], 0, base, nang)
        value = part_hh[s] + damp * (link(mirror, s, halo2_c[s], far_c) * far)
        value = value.astype(BF16).astype(F32)
        value = part_h[s] + 2.0 * damp * (link(mirror, s, halo1_c[s], halo2_c[s]) * value)
        value = value.astype(BF16).astype(F32)
        term = 2.0 * damp * (link(mirror, s, coup[at], halo1_c[s]) * value)
        fixed = (part[at] if s == 0 or own > 1 else fixed) + term
        final[at] = fixed.astype(BF16)

    chan = nchan // nslab
    pieces = -(-chan // LANES)
    vib = lax.axis_index("hl") * nslab + lax.axis_index("rad")
    rows_at = lax.broadcasted_iota(jnp.int32, (nrad, chan), 0)
    for m in range(nslab):
        cols = slice(m * chan, (m + 1) * chan)
        table = lax.dot_general(
            final[...].reshape(own * nrad, nang),
            proj_ref[cols, :],
            NT,
            preferred_element_type=F32,
        ).reshape(own, nrad, chan)
        hit = (rows_at == rad_ref[:, cols]) & (vib_ref[:, cols] == vib)
        for i in range(own):
            amp = jnp.sum(jnp.where(hit, table[i], 0.0), axis=0, keepdims=True)
            if pieces * LANES > chan:
                amp = jnp.concatenate([amp, jnp.zeros((1, pieces * LANES - chan), F32)], axis=1)
            high = amp.astype(BF16).astype(F32)
            tile = [
                half[:, p * LANES : (p + 1) * LANES]
                for half in (high, amp - high)
                for p in range(pieces)
            ]
            if len(tile) < SMALL:
                tile.append(jnp.zeros((SMALL - len(tile), LANES), F32))
            to = place(mirror, own, i) * nslab + m
            out_ref[to, base : base + SMALL, :] = jnp.concatenate(tile, axis=0).astype(BF16)
            for t in range(nang // LANES):
                out_ref[to, t * slab : (t + 1) * slab, :] = final[
                    i, m * slab : (m + 1) * slab, t * LANES : (t + 1) * LANES
                ]


def per_device(
    psi_start,
    potential,
    basis,
    kinetic,
    radial_factor,
    damping,
    coupling,
    helicity,
    chan_rad,
    chan_vib,
    projector,
):
    _, slab, nvib, nang = psi_start.shape
    nquad = basis.shape[1]
    nchan = projector.shape[0]
    groups = lax.axis_size("g")
    own = lax.axis_size("hl")
    nslab = lax.axis_size("rad")
    blocks = groups * own
    group = lax.axis_index("g")
    nrad = nslab * slab
    share = nquad // own
    chunks = (nang + share) // WIDE
    height = (nang + share) // LANES * slab + SMALL
    shape = jax.ShapeDtypeStruct

    send = pl.pallas_call(
        functools.partial(pack, (slab, nvib, nang, share, blocks)),
        out_shape=shape((nvib, height, LANES), BF16),
        in_specs=[HBM] * 3 + [VMEM] + [HBM] * 2,
        out_specs=HBM,
        scratch_shapes=[
            pltpu.VMEM((chunks, slab * nvib, WIDE), F32),
            pltpu.VMEM((nvib, height, LANES), BF16),
            pltpu.VMEM((1, nang), BF16),
            pltpu.VMEM((1, slab), F32),
            pltpu.VMEM((1, slab), F32),
            pltpu.SemaphoreType.DMA((chunks,)),
            pltpu.SemaphoreType.DMA((chunks,)),
            pltpu.SemaphoreType.DMA((3,)),
        ],
        compiler_params=PARAMS,
        name="pack",
    )(
        in_hbm(psi_start.reshape(slab * nvib, nang)),
        in_hbm(potential.reshape(slab * nvib, nquad)),
        in_hbm(coupling),
        helicity[None],
        in_hbm(radial_factor[None]),
        in_hbm(damping[None]),
    )
    message = lax.all_to_all(send, ("hl", "rad"), 0, 0, tiled=True)

    mirror = groups == 2 and own >= ITERS
    sides = 1 if mirror else 2
    rows = message[:, share // LANES * slab :]
    halos = []
    for j in range(ITERS):
        if mirror:
            first = jnp.where(group == 0, own - 1 - j, j) * nslab
            part = lax.dynamic_slice_in_dim(rows, first, nslab, 0)
            halos.append([lax.ppermute(part, "g", [(0, 1), (1, 0)])])
            continue
        away, at = j // own + 1, j % own
        upper = rows[at * nslab : (at + 1) * nslab]
        lower = rows[(own - 1 - at) * nslab : (own - at) * nslab]
        up = [(i, i + away) for i in range(groups - away)]
        halos.append(
            [
                lax.ppermute(lower, "g", up),
                lax.ppermute(upper, "g", [(i, j) for j, i in up]),
            ]
        )

    full_type = shape((own, nrad, nang), F32)
    block_type = shape((own, nrad, nang), BF16)
    side_type = shape((sides, nrad, nang), F32)
    halo_type = shape((sides, nrad, nang), BF16)
    coup_type = shape((sides, 1, nang), F32)
    hat_type = shape((sides, 1, LANES), F32)
    dims = (own, nslab, slab, nang, nquad, mirror)

    def run(n, operands, specs, outs, scratch):
        count = own + sides * (n - 1)
        return pl.pallas_call(
            functools.partial(advance, dims, sides, n),
            out_shape=outs,
            in_specs=specs,
            out_specs=[VMEM] * len(outs),
            scratch_shapes=scratch[:-1]
            + [
                pltpu.VMEM((count, nrad, nang), BF16),
                pltpu.VMEM((count * nrad, nquad), BF16),
                scratch[-1],
            ],
            compiler_params=PARAMS,
            cost_estimate=pl.CostEstimate(
                flops=4 * count * nrad * nang * nquad,
                bytes_accessed=8 * 1024 * 1024,
                transcendentals=0,
            ),
            name=f"advance{n}",
        )(*operands)

    new, first_b, basis, pot, radii, khat, coup, chain = run(
        1,
        [message, in_hbm(basis), kinetic],
        [VMEM, HBM, VMEM],
        [
            full_type,
            block_type,
            shape(basis.shape, BF16),
            shape((nrad, nquad), F32),
            shape((2, nrad, LANES), F32),
            shape((own, 1, LANES), F32),
            shape((own, 1, nang), F32),
            shape((max(own - 1, 1), 1, nang), F32),
        ],
        [pltpu.SemaphoreType.DMA((nquad // STEP,))],
    )
    common = [basis, kinetic, pot, radii, khat, coup, chain]
    joint = pltpu.VMEM((sides, 2, 1, nang), F32)
    operands = halos[0] + common + [new, first_b]
    first_f, level1_b, new, halo_part, halo1_b, halo1_c, halo1_k = run(
        2,
        operands,
        [VMEM] * len(operands),
        [full_type, block_type, full_type, side_type, halo_type, coup_type, hat_type],
        [joint],
    )
    operands = (
        halos[1]
        + common
        + [new, first_b, first_f, halo_part, halo1_b, halo1_c, halo1_k, level1_b]
    )
    new, halo_part, far_part, halo2_c = run(
        3,
        operands,
        [VMEM] * len(operands),
        [full_type, side_type, side_type, coup_type],
        [
            pltpu.VMEM((own, nrad, nang), F32),
            pltpu.VMEM((sides, nrad, nang), BF16),
            pltpu.VMEM((sides, 1, LANES), F32),
            joint,
        ],
    )
    operands = halos[2] + [new, halo_part, far_part, halo1_c, halo2_c, coup, radii]
    operands += [chan_rad[None], chan_vib[None], projector]
    back = pl.pallas_call(
        functools.partial(close, dims, sides, nchan),
        out_shape=shape((own * nslab, nang // LANES * slab + SMALL, LANES), BF16),
        in_specs=[VMEM] * len(operands),
        out_specs=VMEM,
        scratch_shapes=[pltpu.VMEM((own, nrad, nang), BF16)],
        compiler_params=PARAMS,
        name="close",
    )(*operands)

    home = lax.all_to_all(back, ("hl", "rad"), 0, 0, tiled=True)
    chan = nchan // nslab
    psi_final, amplitude = pl.pallas_call(
        functools.partial(unpack, (slab, nvib, nang, -(-chan // LANES))),
        out_shape=[shape((slab * nvib, nang), F32), shape((1, chan), F32)],
        in_specs=[VMEM],
        out_specs=[HBM, VMEM],
        scratch_shapes=[
            pltpu.VMEM((slab * nvib, nang), F32),
            pltpu.SemaphoreType.DMA((nang // STEP,)),
        ],
        compiler_params=PARAMS,
        name="unpack",
    )(home)
    return (psi_final.reshape(1, slab, nvib, nang), amplitude)


def solution(mesh):
    nhel, nrad = mesh.shape["hel"], mesh.shape["rad"]

    def run(*args):
        nvib = args[0].shape[2]
        groups = nhel * nrad // nvib
        fine = Mesh(mesh.devices.reshape(groups, nhel // groups, nrad), ("g", "hl", "rad"))
        hel = ("g", "hl")
        placed = (
            P(hel, "rad", None, None),
            P("rad", None, None),
            P(),
            P(),
            P("rad"),
            P("rad"),
            P(hel, None),
            P(hel),
            P(),
            P(),
            P(),
        )
        return jax.shard_map(
            per_device,
            mesh=fine,
            in_specs=placed,
            out_specs=(P(hel, "rad", None, None), P(hel, "rad")),
            check_vma=False,
        )(*args)

    return run
```

```python
import functools

import jax
import jax.numpy as jnp
from jax import lax
from jax.experimental import pallas as pl
from jax.experimental.pallas import tpu as pltpu
from jax.sharding import Mesh
from jax.sharding import PartitionSpec as P

ITERS = 3
LANES = 128
STEP = 256
WIDE = 384
SMALL = 8
NT = (((1,), (1,)), ((), ()))
F32 = jnp.float32
BF16 = jnp.bfloat16
VMEM = pl.BlockSpec(memory_space=pltpu.VMEM)
HBM = pl.BlockSpec(memory_space=pltpu.HBM)
PARAMS = pltpu.CompilerParams(vmem_limit_bytes=24 * 1024 * 1024)


def in_hbm(array):
    return pltpu.with_memory_space_constraint(array, pltpu.HBM)


def moved_rows(rows, major):
    minor = rows // major
    at = lax.broadcasted_iota(jnp.int32, (1, rows), 1)
    dest = lax.rem(at, minor) * major + at // minor
    return (lax.broadcasted_iota(jnp.int32, (rows, rows), 0) == dest).astype(BF16)


def pack(
    dims, psi_ref, pot_ref, coup_ref, hel_ref, rf_ref, dp_ref, out_ref,
    wide, ready, coup, rf, dp, in_sems, out_sems, sems,
):
    slab, nvib, nang, share, blocks = dims
    near = lax.axis_size("hl")
    here = lax.axis_index("hl")
    is_last = lax.axis_index("g") * near + here == blocks - 1
    tall = WIDE // LANES * slab
    chunks = (nang + share) // WIDE
    height = (nang + share) // LANES * slab

    def load(i):
        if i * WIDE < share:
            first = pl.multiple_of(here * share + i * WIDE, LANES)
            source = pot_ref.at[:, pl.ds(first, WIDE)]
        else:
            source = psi_ref.at[:, pl.ds(i * WIDE - share, WIDE)]
        return pltpu.make_async_copy(source, wide.at[i], in_sems.at[i])

    def save(i):
        size = tall + (SMALL if i == chunks - 1 else 0)
        lines = pl.ds(i * tall, size)
        return pltpu.make_async_copy(
            ready.at[:, lines, :], out_ref.at[:, lines, :], out_sems.at[i]
        )

    small = [
        pltpu.make_async_copy(source, target, sems.at[i])
        for i, (source, target) in enumerate(
            [(coup_ref, coup), (rf_ref, rf), (dp_ref, dp)]
        )
    ]
    for i in range(chunks):
        load(i).start()
    for copy in small:
        copy.start()
    pick = moved_rows(slab * nvib, nvib)

    for copy in small:
        copy.wait()
    ce = jnp.where(is_last, 0.0, coup[...].astype(F32))
    lines = [ce[:, i * LANES : (i + 1) * LANES] for i in range(nang // LANES)]
    parts = []
    for value in (rf[...], dp[...]):
        high = value.astype(BF16).astype(F32)
        parts += [high, value - high]
    spread = (
        lax.rem(lax.broadcasted_iota(jnp.int32, (slab, LANES), 1), slab)
        == lax.broadcasted_iota(jnp.int32, (slab, LANES), 0)
    ).astype(BF16)
    filler = [jnp.zeros((SMALL - len(parts), slab), F32)]
    repeated = jnp.dot(
        jnp.concatenate(parts + filler, axis=0).astype(BF16), spread, preferred_element_type=F32
    )
    owner = lax.broadcasted_iota(jnp.int32, (SMALL, LANES), 1) // slab
    mine = owner == lax.broadcasted_iota(jnp.int32, (SMALL, LANES), 0)
    line = jnp.sum(jnp.where(mine, repeated, 0.0), axis=0, keepdims=True)
    lane = lax.broadcasted_iota(jnp.int32, (1, LANES), 1)
    lines.append(jnp.where(lane == LANES - 1, hel_ref[...].astype(F32), line))
    if len(lines) < SMALL:
        lines.append(jnp.zeros((SMALL - len(lines), LANES), F32))
    tile = jnp.concatenate(lines, axis=0).astype(BF16)
    for v in range(nvib):
        ready[v, height:, :] = tile

    for i in range(chunks):
        load(i).wait()
        moved = jnp.dot(pick, wide[i].astype(BF16), preferred_element_type=F32)
        moved = moved.astype(BF16).reshape(nvib, slab, WIDE)
        for t in range(WIDE // LANES):
            row = i * tall + t * slab
            ready[:, row : row + slab, :] = moved[:, :, t * LANES : (t + 1) * LANES]
        save(i).start()
    for i in range(chunks):
        save(i).wait()


def unpack(dims, msg_ref, out_ref, amp_ref, wide, sems):
    slab, nvib, nang, pieces = dims
    rows = slab * nvib
    tall = STEP // LANES * slab
    steps = nang // STEP

    def save(step):
        cols = pl.ds(step * STEP, STEP)
        return pltpu.make_async_copy(wide.at[:, cols], out_ref.at[:, cols], sems.at[step])

    pick = moved_rows(rows, slab)
    for step in range(steps):
        parts = [
            msg_ref[:, row : row + slab, :].reshape(rows, LANES)
            for row in range(step * tall, (step + 1) * tall, slab)
        ]
        wide[:, step * STEP : (step + 1) * STEP] = jnp.dot(
            pick, jnp.concatenate(parts, axis=1), preferred_element_type=F32
        )
        save(step).start()
    base = nang // LANES * slab
    lines = jnp.sum(msg_ref[:, base : base + SMALL, :].astype(F32), axis=0)
    lines = [lines[i : i + 1] + lines[pieces + i : pieces + i + 1] for i in range(pieces)]
    amp_ref[...] = jnp.concatenate(lines, axis=1)[:, : amp_ref.shape[1]]
    for step in range(steps):
        save(step).wait()


def rows_in(ref, first, count, slab, nang, base):
    return jnp.concatenate(
        [
            jnp.concatenate(
                [ref[m, base + i * slab : base + (i + 1) * slab, :] for i in range(nang // LANES)],
                axis=1,
            )
            for m in [first + i for i in range(count)]
        ],
        axis=0,
    )


def small_in(ref, m, base, nang):
    page = ref[m, base : base + SMALL, :].astype(F32)
    lines = [page[i : i + 1, :] for i in range(nang // LANES)]
    value = page[len(lines) : len(lines) + 1, LANES - 1 :]
    return jnp.concatenate(lines, axis=1), jnp.broadcast_to(-2.0 * value * value, (1, LANES))


def link(mirror, side, near, far):
    if mirror:
        return jnp.where(lax.axis_index("g") == 0, near, far)
    return far if side == 0 else near


def place(mirror, own, i):
    if mirror:
        return jnp.where(lax.axis_index("g") == 0, own - 1 - i, i)
    return i


def edge_block(mirror, own, side, j):
    if mirror:
        return place(mirror, own, j)
    return own - 1 - j % own if side == 0 else j % own


def unfold(dims, msg_ref, src, pot, radii, khat, coup):
    own, nslab, slab, nang, nquad, mirror = dims
    share = nquad // own
    top = share // LANES * slab
    base = top + nang // LANES * slab
    lane = lax.broadcasted_iota(jnp.int32, (slab, LANES), 1)
    row = lax.broadcasted_iota(jnp.int32, (slab, LANES), 0)
    for k in range(own):
        for m in range(nslab):
            for t in range(share // LANES):
                cols = pl.ds(k * share + t * LANES, LANES)
                tile = msg_ref[k * nslab + m, t * slab : (t + 1) * slab, :]
                pot[m * slab : (m + 1) * slab, cols] = tile.astype(F32)
    for i in range(own):
        first = place(mirror, own, i) * nslab
        src[i] = rows_in(msg_ref, first, nslab, slab, nang, top)
        coup[i], khat[i] = small_in(msg_ref, first, base, nang)
    for m in range(nslab):
        page = msg_ref[m, base : base + SMALL, :].astype(F32)
        line = page[nang // LANES : nang // LANES + 1, :]
        for i in range(2):
            hit = (lane == row + 2 * i * slab) | (lane == row + (2 * i + 1) * slab)
            value = jnp.sum(jnp.where(hit, line, 0.0), axis=1, keepdims=True)
            radii[i, m * slab : (m + 1) * slab, :] = jnp.broadcast_to(value, (slab, LANES))


def wider(tile, size):
    return jnp.concatenate([tile] * (size // LANES), axis=1)


def advance(dims, sides, n, *refs):
    own, nslab, slab, nang, nquad, mirror = dims
    nrad = nslab * slab
    refs = list(refs)
    share = nquad // own
    top = share // LANES * slab
    take = lambda count: [refs.pop(0) for _ in range(count)]
    edge_of = [0, own - 1]
    if n == 1:
        msg_ref, basis_hbm, kin_ref = take(3)
        new_ref, src, basis, pot, radii, khat, coup, chain = take(8)
        sends = take(sides)
        rows, scaled, sems = take(3)
        for qi in range(nquad // STEP):
            cols = pl.ds(qi * STEP, STEP)
            pltpu.make_async_copy(basis_hbm.at[:, cols], basis.at[:, cols], sems.at[qi]).start()
        unfold(dims, msg_ref, src, pot, radii, khat, coup)
        rows[...] = src[...]
        for i in range(own - 1):
            chain[i] = link(mirror, 0, coup[i + 1], coup[i])
    else:
        raw = take(sides)
        basis, kin_ref, pot, radii, khat, coup, chain = take(7)
        scale = wider(radii[1] if n == 2 else 2.0 * radii[1], nang)
        base = nang // LANES * slab
        if n == 2:
            part, first_b, msg_ref = take(3)
            full, block, new_ref, part_h, halo_b, halo_c, halo_k = take(7)
            sends = take(sides)
            rows, scaled, joint = take(3)
        else:
            part, first_b, first_f, halo_part, halo1_b, halo1_c, halo1_k, level1_b = take(8)
            new_ref, part_h, part_hh, halo_c = take(4)
            full, halo_b, halo_k, rows, scaled, joint = take(6)
        for i in range(own):
            value = part[i]
            full[i] = value
            rows[i] = value.astype(BF16)
        for s in range(sides):
            halo_b[s] = rows_in(raw[s], 0, nslab, slab, nang, 0)
            halo_c[s], halo_k[s] = small_in(raw[s], 0, base, nang)
            at = edge_of[s]
            if n == 2:
                joint[s, 0] = link(mirror, s, coup[at], halo_c[s])
                seen = halo_b[s]
                rows[own + s] = seen
            else:
                joint[s, 0] = link(mirror, s, coup[at], halo1_c[s])
                joint[s, 1] = link(mirror, s, halo1_c[s], halo_c[s])
                level = halo_part[s] + wider(radii[1], nang) * (
                    joint[s, 1] * halo_b[s].astype(F32)
                )
                seen = level.astype(BF16)
                rows[own + s] = seen
                rows[own + sides + s] = halo_b[s]
            value = full[at] + scale * (joint[s, 0] * seen.astype(F32))
            full[at] = value
            rows[at] = value.astype(BF16)
        if n == 2:
            block[...] = rows[:own]
    count = own + sides * (n - 1)
    if n < ITERS:
        for s in range(sides):
            first = edge_block(mirror, own, s, n) * nslab
            for m in range(nslab):
                sends[s][m] = msg_ref[first + m, top:, :]

    @pl.loop(0, nquad // STEP)
    def _(qi):
        cols = pl.ds(pl.multiple_of(qi * STEP, STEP), STEP)
        if n == 1:
            pltpu.make_async_copy(basis_hbm.at[:, cols], basis.at[:, cols], sems.at[qi]).wait()
        grid = jnp.dot(
            rows[...].reshape(count * nrad, nang), basis[:, cols], preferred_element_type=F32
        )
        prod = grid.reshape(count, nrad, STEP) * pot[:, cols][None]
        scaled[:, cols] = prod.astype(BF16).reshape(count * nrad, STEP)

    factor = wider(radii[0], STEP)
    damp = wider(radii[1], STEP)

    @pl.loop(0, nang // STEP)
    def _(ji):
        cols = pl.ds(pl.multiple_of(ji * STEP, STEP), STEP)
        ang = lax.dot_general(
            scaled[...], basis[cols, :], NT, preferred_element_type=F32
        ).reshape(count, nrad, STEP)

        def local(i, hat, value):
            kin = jnp.dot(kin_ref[...], rows[i, :, cols], preferred_element_type=F32)
            return ang[i] + kin + wider(hat, STEP) * factor * value

        for i in range(own):
            value = rows[i, :, cols].astype(F32) if n == 1 else full[i, :, cols]
            total = local(i, khat[i], value)
            if i + 1 < own:
                total += chain[i, :, cols] * rows[i + 1, :, cols].astype(F32)
            if i > 0:
                total += chain[i - 1, :, cols] * rows[i - 1, :, cols].astype(F32)
            if n == 1:
                new_ref[i, :, cols] = damp * total
            else:
                before = first_b if n == 2 else first_f
                new_ref[i, :, cols] = damp * (
                    2.0 * total - damp * before[i, :, cols].astype(F32)
                )
        for s in range(sides if n > 1 else 0):
            at = edge_of[s]
            i = own + s
            hat = halo_k[s] if n == 2 else halo1_k[s]
            total = local(i, hat, rows[i, :, cols].astype(F32))
            edge_b = first_b if n == 2 else level1_b
            total += joint[s, 0, :, cols] * edge_b[at, :, cols].astype(F32)
            if n == 2:
                part_h[s, :, cols] = damp * total
                continue
            before = halo1_b[s, :, cols].astype(F32)
            part_h[s, :, cols] = damp * (2.0 * total - damp * before)
            i = own + sides + s
            total = local(i, halo_k[s], rows[i, :, cols].astype(F32))
            total += joint[s, 1, :, cols] * before
            part_hh[s, :, cols] = damp * total


def close(dims, sides, nchan, *refs):
    own, nslab, slab, nang, nquad, mirror = dims
    nrad = nslab * slab
    raw, refs = refs[:sides], refs[sides:]
    part, part_h, part_hh, halo1_c, halo2_c, coup, radii = refs[:7]
    rad_ref, vib_ref, proj_ref, out_ref, final = refs[7:]
    base = nang // LANES * slab
    damp = wider(radii[1], nang)
    for i in range(own):
        final[i] = part[i].astype(BF16)
    for s in range(sides):
        at = 0 if s == 0 else own - 1
        far = rows_in(raw[s], 0, nslab, slab, nang, 0).astype(F32)
        far_c, _ = small_in(raw[s], 0, base, nang)
        value = part_hh[s] + damp * (link(mirror, s, halo2_c[s], far_c) * far)
        value = value.astype(BF16).astype(F32)
        value = part_h[s] + 2.0 * damp * (link(mirror, s, halo1_c[s], halo2_c[s]) * value)
        value = value.astype(BF16).astype(F32)
        term = 2.0 * damp * (link(mirror, s, coup[at], halo1_c[s]) * value)
        fixed = (part[at] if s == 0 or own > 1 else fixed) + term
        final[at] = fixed.astype(BF16)

    chan = nchan // nslab
    pieces = -(-chan // LANES)
    vib = lax.axis_index("hl") * nslab + lax.axis_index("rad")
    rows_at = lax.broadcasted_iota(jnp.int32, (nrad, chan), 0)
    for m in range(nslab):
        cols = slice(m * chan, (m + 1) * chan)
        table = lax.dot_general(
            final[...].reshape(own * nrad, nang),
            proj_ref[cols, :],
            NT,
            preferred_element_type=F32,
        ).reshape(own, nrad, chan)
        hit = (rows_at == rad_ref[:, cols]) & (vib_ref[:, cols] == vib)
        for i in range(own):
            amp = jnp.sum(jnp.where(hit, table[i], 0.0), axis=0, keepdims=True)
            if pieces * LANES > chan:
                amp = jnp.concatenate([amp, jnp.zeros((1, pieces * LANES - chan), F32)], axis=1)
            high = amp.astype(BF16).astype(F32)
            tile = [
                half[:, p * LANES : (p + 1) * LANES]
                for half in (high, amp - high)
                for p in range(pieces)
            ]
            if len(tile) < SMALL:
                tile.append(jnp.zeros((SMALL - len(tile), LANES), F32))
            to = place(mirror, own, i) * nslab + m
            out_ref[to, base : base + SMALL, :] = jnp.concatenate(tile, axis=0).astype(BF16)
            for t in range(nang // LANES):
                out_ref[to, t * slab : (t + 1) * slab, :] = final[
                    i, m * slab : (m + 1) * slab, t * LANES : (t + 1) * LANES
                ]


def per_device(
    psi_start,
    potential,
    basis,
    kinetic,
    radial_factor,
    damping,
    coupling,
    helicity,
    chan_rad,
    chan_vib,
    projector,
):
    _, slab, nvib, nang = psi_start.shape
    nquad = basis.shape[1]
    nchan = projector.shape[0]
    groups = lax.axis_size("g")
    own = lax.axis_size("hl")
    nslab = lax.axis_size("rad")
    blocks = groups * own
    group = lax.axis_index("g")
    nrad = nslab * slab
    share = nquad // own
    chunks = (nang + share) // WIDE
    height = (nang + share) // LANES * slab + SMALL
    shape = jax.ShapeDtypeStruct

    send = pl.pallas_call(
        functools.partial(pack, (slab, nvib, nang, share, blocks)),
        out_shape=shape((nvib, height, LANES), BF16),
        in_specs=[HBM] * 3 + [VMEM] + [HBM] * 2,
        out_specs=HBM,
        scratch_shapes=[
            pltpu.VMEM((chunks, slab * nvib, WIDE), F32),
            pltpu.VMEM((nvib, height, LANES), BF16),
            pltpu.VMEM((1, nang), BF16),
            pltpu.VMEM((1, slab), F32),
            pltpu.VMEM((1, slab), F32),
            pltpu.SemaphoreType.DMA((chunks,)),
            pltpu.SemaphoreType.DMA((chunks,)),
            pltpu.SemaphoreType.DMA((3,)),
        ],
        compiler_params=PARAMS,
        name="pack",
    )(
        in_hbm(psi_start.reshape(slab * nvib, nang)),
        in_hbm(potential.reshape(slab * nvib, nquad)),
        in_hbm(coupling),
        helicity[None],
        in_hbm(radial_factor[None]),
        in_hbm(damping[None]),
    )
    message = lax.all_to_all(send, ("hl", "rad"), 0, 0, tiled=True)

    mirror = groups == 2 and own >= ITERS
    sides = 1 if mirror else 2
    send_type = shape((nslab, height - share // LANES * slab, LANES), BF16)

    def cross(parts, j):
        if mirror:
            return [lax.ppermute(parts[0], "g", [(0, 1), (1, 0)])]
        away = j // own + 1
        up = [(i, i + away) for i in range(groups - away)]
        return [
            lax.ppermute(parts[0], "g", up),
            lax.ppermute(parts[1], "g", [(i, j) for j, i in up]),
        ]

    rows = message[:, share // LANES * slab :]
    sent = [
        lax.dynamic_slice_in_dim(rows, edge_block(mirror, own, s, 0) * nslab, nslab, 0)
        for s in range(sides)
    ]
    halo = cross(sent, 0)

    full_type = shape((own, nrad, nang), F32)
    block_type = shape((own, nrad, nang), BF16)
    side_type = shape((sides, nrad, nang), F32)
    halo_type = shape((sides, nrad, nang), BF16)
    coup_type = shape((sides, 1, nang), F32)
    hat_type = shape((sides, 1, LANES), F32)
    dims = (own, nslab, slab, nang, nquad, mirror)

    def run(n, operands, specs, outs, scratch):
        count = own + sides * (n - 1)
        return pl.pallas_call(
            functools.partial(advance, dims, sides, n),
            out_shape=outs,
            in_specs=specs,
            out_specs=[VMEM] * len(outs),
            scratch_shapes=scratch[:-1]
            + [
                pltpu.VMEM((count, nrad, nang), BF16),
                pltpu.VMEM((count * nrad, nquad), BF16),
                scratch[-1],
            ],
            compiler_params=PARAMS,
            cost_estimate=pl.CostEstimate(
                flops=4 * count * nrad * nang * nquad,
                bytes_accessed=8 * 1024 * 1024,
                transcendentals=0,
            ),
            name=f"advance{n}",
        )(*operands)

    new, first_b, basis, pot, radii, khat, coup, chain, *sent = run(
        1,
        [message, in_hbm(basis), kinetic],
        [VMEM, HBM, VMEM],
        [
            full_type,
            block_type,
            shape(basis.shape, BF16),
            shape((nrad, nquad), F32),
            shape((2, nrad, LANES), F32),
            shape((own, 1, LANES), F32),
            shape((own, 1, nang), F32),
            shape((max(own - 1, 1), 1, nang), F32),
        ]
        + [send_type] * sides,
        [pltpu.SemaphoreType.DMA((nquad // STEP,))],
    )
    common = [basis, kinetic, pot, radii, khat, coup, chain]
    joint = pltpu.VMEM((sides, 2, 1, nang), F32)
    operands = halo + common + [new, first_b, message]
    halo = cross(sent, 1)
    first_f, level1_b, new, halo_part, halo1_b, halo1_c, halo1_k, *sent = run(
        2,
        operands,
        [VMEM] * len(operands),
        [full_type, block_type, full_type, side_type, halo_type, coup_type, hat_type]
        + [send_type] * sides,
        [joint],
    )
    operands = (
        halo
        + common
        + [new, first_b, first_f, halo_part, halo1_b, halo1_c, halo1_k, level1_b]
    )
    halo = cross(sent, 2)
    new, halo_part, far_part, halo2_c = run(
        3,
        operands,
        [VMEM] * len(operands),
        [full_type, side_type, side_type, coup_type],
        [
            pltpu.VMEM((own, nrad, nang), F32),
            pltpu.VMEM((sides, nrad, nang), BF16),
            pltpu.VMEM((sides, 1, LANES), F32),
            joint,
        ],
    )
    operands = halo + [new, halo_part, far_part, halo1_c, halo2_c, coup, radii]
    operands += [chan_rad[None], chan_vib[None], projector]
    back = pl.pallas_call(
        functools.partial(close, dims, sides, nchan),
        out_shape=shape((own * nslab, nang // LANES * slab + SMALL, LANES), BF16),
        in_specs=[VMEM] * len(operands),
        out_specs=VMEM,
        scratch_shapes=[pltpu.VMEM((own, nrad, nang), BF16)],
        compiler_params=PARAMS,
        name="close",
    )(*operands)

    home = lax.all_to_all(back, ("hl", "rad"), 0, 0, tiled=True)
    chan = nchan // nslab
    psi_final, amplitude = pl.pallas_call(
        functools.partial(unpack, (slab, nvib, nang, -(-chan // LANES))),
        out_shape=[shape((slab * nvib, nang), F32), shape((1, chan), F32)],
        in_specs=[VMEM],
        out_specs=[HBM, VMEM],
        scratch_shapes=[
            pltpu.VMEM((slab * nvib, nang), F32),
            pltpu.SemaphoreType.DMA((nang // STEP,)),
        ],
        compiler_params=PARAMS,
        name="unpack",
    )(home)
    return (psi_final.reshape(1, slab, nvib, nang), amplitude)


def solution(mesh):
    nhel, nrad = mesh.shape["hel"], mesh.shape["rad"]

    def run(*args):
        nvib = args[0].shape[2]
        groups = nhel * nrad // nvib
        fine = Mesh(mesh.devices.reshape(groups, nhel // groups, nrad), ("g", "hl", "rad"))
        hel = ("g", "hl")
        placed = (
            P(hel, "rad", None, None),
            P("rad", None, None),
            P(),
            P(),
            P("rad"),
            P("rad"),
            P(hel, None),
            P(hel),
            P(),
            P(),
            P(),
        )
        return jax.shard_map(
            per_device,
            mesh=fine,
            in_specs=placed,
            out_specs=(P(hel, "rad", None, None), P(hel, "rad")),
            check_vma=False,
        )(*args)

    return run
```

```python
import functools

import jax
import jax.numpy as jnp
from jax import lax
from jax.experimental import pallas as pl
from jax.experimental.pallas import tpu as pltpu
from jax.sharding import Mesh
from jax.sharding import PartitionSpec as P

ITERS = 3
LANES = 128
STEP = 256
WIDE = 128
AHEAD = 3
SMALL = 8
NT = (((1,), (1,)), ((), ()))
F32 = jnp.float32
BF16 = jnp.bfloat16
VMEM = pl.BlockSpec(memory_space=pltpu.VMEM)
HBM = pl.BlockSpec(memory_space=pltpu.HBM)
PARAMS = pltpu.CompilerParams(vmem_limit_bytes=24 * 1024 * 1024)


def in_hbm(array):
    return pltpu.with_memory_space_constraint(array, pltpu.HBM)


def moved_rows(rows, major):
    minor = rows // major
    at = lax.broadcasted_iota(jnp.int32, (1, rows), 1)
    dest = lax.rem(at, minor) * major + at // minor
    return (lax.broadcasted_iota(jnp.int32, (rows, rows), 0) == dest).astype(BF16)


def pack(
    dims, psi_ref, pot_ref, coup_ref, hel_ref, rf_ref, dp_ref, out_ref,
    wide, ready, coup, rf, dp, in_sems, out_sems, sems,
):
    slab, nvib, nang, share, blocks = dims
    near = lax.axis_size("hl")
    here = lax.axis_index("hl")
    is_last = lax.axis_index("g") * near + here == blocks - 1
    tall = WIDE // LANES * slab
    chunks = (nang + share) // WIDE
    height = (nang + share) // LANES * slab

    def load(i):
        if i * WIDE < share:
            first = pl.multiple_of(here * share + i * WIDE, LANES)
            source = pot_ref.at[:, pl.ds(first, WIDE)]
        else:
            source = psi_ref.at[:, pl.ds(i * WIDE - share, WIDE)]
        return pltpu.make_async_copy(source, wide.at[i], in_sems.at[i])

    def save(i):
        size = tall + (SMALL if i == chunks - 1 else 0)
        lines = pl.ds(i * tall, size)
        return pltpu.make_async_copy(
            ready.at[:, lines, :], out_ref.at[:, lines, :], out_sems.at[i]
        )

    small = [
        pltpu.make_async_copy(source, target, sems.at[i])
        for i, (source, target) in enumerate(
            [(coup_ref, coup), (rf_ref, rf), (dp_ref, dp)]
        )
    ]
    for i in range(min(AHEAD, chunks)):
        load(i).start()
    for copy in small:
        copy.start()
    pick = moved_rows(slab * nvib, nvib)

    for copy in small:
        copy.wait()
    ce = jnp.where(is_last, 0.0, coup[...].astype(F32))
    lines = [ce[:, i * LANES : (i + 1) * LANES] for i in range(nang // LANES)]
    parts = []
    for value in (rf[...], dp[...]):
        high = value.astype(BF16).astype(F32)
        parts += [high, value - high]
    spread = (
        lax.rem(lax.broadcasted_iota(jnp.int32, (slab, LANES), 1), slab)
        == lax.broadcasted_iota(jnp.int32, (slab, LANES), 0)
    ).astype(BF16)
    filler = [jnp.zeros((SMALL - len(parts), slab), F32)]
    repeated = jnp.dot(
        jnp.concatenate(parts + filler, axis=0).astype(BF16), spread, preferred_element_type=F32
    )
    owner = lax.broadcasted_iota(jnp.int32, (SMALL, LANES), 1) // slab
    mine = owner == lax.broadcasted_iota(jnp.int32, (SMALL, LANES), 0)
    line = jnp.sum(jnp.where(mine, repeated, 0.0), axis=0, keepdims=True)
    lane = lax.broadcasted_iota(jnp.int32, (1, LANES), 1)
    lines.append(jnp.where(lane == LANES - 1, hel_ref[...].astype(F32), line))
    if len(lines) < SMALL:
        lines.append(jnp.zeros((SMALL - len(lines), LANES), F32))
    tile = jnp.concatenate(lines, axis=0).astype(BF16)
    for v in range(nvib):
        ready[v, height:, :] = tile

    for i in range(chunks):
        load(i).wait()
        if i + AHEAD < chunks:
            load(i + AHEAD).start()
        moved = jnp.dot(pick, wide[i].astype(BF16), preferred_element_type=F32)
        moved = moved.astype(BF16).reshape(nvib, slab, WIDE)
        for t in range(WIDE // LANES):
            row = i * tall + t * slab
            ready[:, row : row + slab, :] = moved[:, :, t * LANES : (t + 1) * LANES]
        save(i).start()
    for i in range(chunks):
        save(i).wait()


def unpack(dims, msg_ref, out_ref, amp_ref, wide, sems):
    slab, nvib, nang, pieces = dims
    rows = slab * nvib
    tall = STEP // LANES * slab
    steps = nang // STEP

    def save(step):
        cols = pl.ds(step * STEP, STEP)
        return pltpu.make_async_copy(wide.at[:, cols], out_ref.at[:, cols], sems.at[step])

    pick = moved_rows(rows, slab)
    for step in range(steps):
        parts = [
            msg_ref[:, row : row + slab, :].reshape(rows, LANES)
            for row in range(step * tall, (step + 1) * tall, slab)
        ]
        wide[:, step * STEP : (step + 1) * STEP] = jnp.dot(
            pick, jnp.concatenate(parts, axis=1), preferred_element_type=F32
        )
        save(step).start()
    base = nang // LANES * slab
    lines = jnp.sum(msg_ref[:, base : base + SMALL, :].astype(F32), axis=0)
    lines = [lines[i : i + 1] + lines[pieces + i : pieces + i + 1] for i in range(pieces)]
    amp_ref[...] = jnp.concatenate(lines, axis=1)[:, : amp_ref.shape[1]]
    for step in range(steps):
        save(step).wait()


def rows_in(ref, first, count, slab, nang, base):
    return jnp.concatenate(
        [
            jnp.concatenate(
                [ref[m, base + i * slab : base + (i + 1) * slab, :] for i in range(nang // LANES)],
                axis=1,
            )
            for m in [first + i for i in range(count)]
        ],
        axis=0,
    )


def small_in(ref, m, base, nang):
    page = ref[m, base : base + SMALL, :].astype(F32)
    lines = [page[i : i + 1, :] for i in range(nang // LANES)]
    value = page[len(lines) : len(lines) + 1, LANES - 1 :]
    return jnp.concatenate(lines, axis=1), jnp.broadcast_to(-2.0 * value * value, (1, LANES))


def link(mirror, side, near, far):
    if mirror:
        return jnp.where(lax.axis_index("g") == 0, near, far)
    return far if side == 0 else near


def place(mirror, own, i):
    if mirror:
        return jnp.where(lax.axis_index("g") == 0, own - 1 - i, i)
    return i


def unfold(dims, msg_ref, src, pot, radii, khat, coup):
    own, nslab, slab, nang, nquad, mirror = dims
    share = nquad // own
    top = share // LANES * slab
    base = top + nang // LANES * slab
    lane = lax.broadcasted_iota(jnp.int32, (slab, LANES), 1)
    row = lax.broadcasted_iota(jnp.int32, (slab, LANES), 0)
    for k in range(own):
        for m in range(nslab):
            for t in range(share // LANES):
                cols = pl.ds(k * share + t * LANES, LANES)
                tile = msg_ref[k * nslab + m, t * slab : (t + 1) * slab, :]
                pot[m * slab : (m + 1) * slab, cols] = tile.astype(F32)
    for i in range(own):
        first = place(mirror, own, i) * nslab
        src[i] = rows_in(msg_ref, first, nslab, slab, nang, top)
        coup[i], khat[i] = small_in(msg_ref, first, base, nang)
    for m in range(nslab):
        page = msg_ref[m, base : base + SMALL, :].astype(F32)
        line = page[nang // LANES : nang // LANES + 1, :]
        for i in range(2):
            hit = (lane == row + 2 * i * slab) | (lane == row + (2 * i + 1) * slab)
            value = jnp.sum(jnp.where(hit, line, 0.0), axis=1, keepdims=True)
            radii[i, m * slab : (m + 1) * slab, :] = jnp.broadcast_to(value, (slab, LANES))


def wider(tile, size):
    return jnp.concatenate([tile] * (size // LANES), axis=1)


def inner(dims, *refs):
    own, nslab, slab, nang, nquad, mirror = dims
    nrad = nslab * slab
    basis, kin_ref, pot, radii, khat, coup, chain, part, first_b, new_ref, rows, scaled = refs
    count = own - 1
    for i in range(count):
        rows[i] = part[i + 1].astype(BF16)

    @pl.loop(0, nquad // STEP)
    def _(qi):
        cols = pl.ds(pl.multiple_of(qi * STEP, STEP), STEP)
        grid = jnp.dot(
            rows[...].reshape(count * nrad, nang), basis[:, cols], preferred_element_type=F32
        )
        prod = grid.reshape(count, nrad, STEP) * pot[:, cols][None]
        scaled[:, cols] = prod.astype(BF16).reshape(count * nrad, STEP)

    factor = wider(radii[0], STEP)
    damp = wider(radii[1], STEP)

    @pl.loop(0, nang // STEP)
    def _(ji):
        cols = pl.ds(pl.multiple_of(ji * STEP, STEP), STEP)
        ang = lax.dot_general(
            scaled[...], basis[cols, :], NT, preferred_element_type=F32
        ).reshape(count, nrad, STEP)
        for i in range(count):
            total = ang[i] + jnp.dot(
                kin_ref[...], rows[i, :, cols], preferred_element_type=F32
            )
            total += wider(khat[i + 1], STEP) * factor * part[i + 1, :, cols]
            if i + 1 < count:
                total += chain[i + 1, :, cols] * rows[i + 1, :, cols].astype(F32)
            if i > 0:
                total += chain[i, :, cols] * rows[i - 1, :, cols].astype(F32)
            before = first_b[i + 1, :, cols].astype(F32)
            new_ref[i, :, cols] = damp * (2.0 * total - damp * before)


def advance(dims, sides, n, *refs):
    own, nslab, slab, nang, nquad, mirror = dims
    nrad = nslab * slab
    refs = list(refs)
    take = lambda count: [refs.pop(0) for _ in range(count)]
    edge_of = [0, own - 1]
    if n == 1:
        msg_ref, basis_hbm, kin_ref = take(3)
        new_ref, src, basis, pot, radii, khat, coup, chain = take(8)
        rows, scaled, sems = take(3)
        for qi in range(nquad // STEP):
            cols = pl.ds(qi * STEP, STEP)
            pltpu.make_async_copy(basis_hbm.at[:, cols], basis.at[:, cols], sems.at[qi]).start()
        unfold(dims, msg_ref, src, pot, radii, khat, coup)
        rows[...] = src[...]
        for i in range(own - 1):
            chain[i] = link(mirror, 0, coup[i + 1], coup[i])
    else:
        raw = take(sides)
        basis, kin_ref, pot, radii, khat, coup, chain = take(7)
        scale = wider(radii[1] if n == 2 else 2.0 * radii[1], nang)
        base = nang // LANES * slab
        if n == 2:
            part, first_b = take(2)
            inner_ref = take(1)[0] if mirror else None
            full, block, new_ref, part_h, halo_b, halo_c, halo_k = take(7)
            rows, scaled, joint = take(3)
        else:
            part, first_b, first_f, halo_part, halo1_b, halo1_c, halo1_k, level1_b = take(8)
            new_ref, part_h, part_hh, halo_c = take(4)
            full, halo_b, halo_k, rows, scaled, joint = take(6)
        split = mirror and n == 2
        level = block if split else rows
        shift = 1 if split else own
        for i in range(own):
            value = part[i]
            full[i] = value
            level[i] = value.astype(BF16)
        for s in range(sides):
            halo_b[s] = rows_in(raw[s], 0, nslab, slab, nang, 0)
            halo_c[s], halo_k[s] = small_in(raw[s], 0, base, nang)
            at = edge_of[s]
            if n == 2:
                joint[s, 0] = link(mirror, s, coup[at], halo_c[s])
                seen = halo_b[s]
                rows[shift + s] = seen
            else:
                joint[s, 0] = link(mirror, s, coup[at], halo1_c[s])
                joint[s, 1] = link(mirror, s, halo1_c[s], halo_c[s])
                value = halo_part[s] + wider(radii[1], nang) * (
                    joint[s, 1] * halo_b[s].astype(F32)
                )
                seen = value.astype(BF16)
                rows[own + s] = seen
                rows[own + sides + s] = halo_b[s]
            value = full[at] + scale * (joint[s, 0] * seen.astype(F32))
            full[at] = value
            level[at] = value.astype(BF16)
        if split:
            rows[0] = block[0]
        elif n == 2:
            block[...] = rows[:own]
    if n == 1:
        split, level, shift = False, rows, own
    count = shift + sides * (n - 1)

    @pl.loop(0, nquad // STEP)
    def _(qi):
        cols = pl.ds(pl.multiple_of(qi * STEP, STEP), STEP)
        if n == 1:
            pltpu.make_async_copy(basis_hbm.at[:, cols], basis.at[:, cols], sems.at[qi]).wait()
        grid = jnp.dot(
            rows[...].reshape(count * nrad, nang), basis[:, cols], preferred_element_type=F32
        )
        prod = grid.reshape(count, nrad, STEP) * pot[:, cols][None]
        scaled[:, cols] = prod.astype(BF16).reshape(count * nrad, STEP)

    factor = wider(radii[0], STEP)
    damp = wider(radii[1], STEP)

    @pl.loop(0, nang // STEP)
    def _(ji):
        cols = pl.ds(pl.multiple_of(ji * STEP, STEP), STEP)
        ang = lax.dot_general(
            scaled[...], basis[cols, :], NT, preferred_element_type=F32
        ).reshape(count, nrad, STEP)

        def local(i, hat, value):
            kin = jnp.dot(kin_ref[...], rows[i, :, cols], preferred_element_type=F32)
            return ang[i] + kin + wider(hat, STEP) * factor * value

        for i in range(own):
            if split and i > 0:
                value = inner_ref[i - 1, :, cols]
                if i == 1:
                    value += 2.0 * damp * (chain[0, :, cols] * level[0, :, cols].astype(F32))
                new_ref[i, :, cols] = value
                continue
            value = rows[i, :, cols].astype(F32) if n == 1 else full[i, :, cols]
            total = local(i, khat[i], value)
            if i + 1 < own:
                total += chain[i, :, cols] * level[i + 1, :, cols].astype(F32)
            if i > 0:
                total += chain[i - 1, :, cols] * level[i - 1, :, cols].astype(F32)
            if n == 1:
                new_ref[i, :, cols] = damp * total
            else:
                before = first_b if n == 2 else first_f
                new_ref[i, :, cols] = damp * (
                    2.0 * total - damp * before[i, :, cols].astype(F32)
                )
        for s in range(sides if n > 1 else 0):
            at = edge_of[s]
            i = shift + s
            hat = halo_k[s] if n == 2 else halo1_k[s]
            total = local(i, hat, rows[i, :, cols].astype(F32))
            edge_b = first_b if n == 2 else level1_b
            total += joint[s, 0, :, cols] * edge_b[at, :, cols].astype(F32)
            if n == 2:
                part_h[s, :, cols] = damp * total
                continue
            before = halo1_b[s, :, cols].astype(F32)
            part_h[s, :, cols] = damp * (2.0 * total - damp * before)
            i = own + sides + s
            total = local(i, halo_k[s], rows[i, :, cols].astype(F32))
            total += joint[s, 1, :, cols] * before
            part_hh[s, :, cols] = damp * total


def close(dims, sides, nchan, *refs):
    own, nslab, slab, nang, nquad, mirror = dims
    nrad = nslab * slab
    raw, refs = refs[:sides], refs[sides:]
    part, part_h, part_hh, halo1_c, halo2_c, coup, radii = refs[:7]
    rad_ref, vib_ref, proj_ref, out_ref, final = refs[7:]
    base = nang // LANES * slab
    damp = wider(radii[1], nang)
    for i in range(own):
        final[i] = part[i].astype(BF16)
    for s in range(sides):
        at = 0 if s == 0 else own - 1
        far = rows_in(raw[s], 0, nslab, slab, nang, 0).astype(F32)
        far_c, _ = small_in(raw[s], 0, base, nang)
        value = part_hh[s] + damp * (link(mirror, s, halo2_c[s], far_c) * far)
        value = value.astype(BF16).astype(F32)
        value = part_h[s] + 2.0 * damp * (link(mirror, s, halo1_c[s], halo2_c[s]) * value)
        value = value.astype(BF16).astype(F32)
        term = 2.0 * damp * (link(mirror, s, coup[at], halo1_c[s]) * value)
        fixed = (part[at] if s == 0 or own > 1 else fixed) + term
        final[at] = fixed.astype(BF16)

    chan = nchan // nslab
    pieces = -(-chan // LANES)
    vib = lax.axis_index("hl") * nslab + lax.axis_index("rad")
    rows_at = lax.broadcasted_iota(jnp.int32, (nrad, chan), 0)
    for m in range(nslab):
        cols = slice(m * chan, (m + 1) * chan)
        table = lax.dot_general(
            final[...].reshape(own * nrad, nang),
            proj_ref[cols, :],
            NT,
            preferred_element_type=F32,
        ).reshape(own, nrad, chan)
        hit = (rows_at == rad_ref[:, cols]) & (vib_ref[:, cols] == vib)
        for i in range(own):
            amp = jnp.sum(jnp.where(hit, table[i], 0.0), axis=0, keepdims=True)
            if pieces * LANES > chan:
                amp = jnp.concatenate([amp, jnp.zeros((1, pieces * LANES - chan), F32)], axis=1)
            high = amp.astype(BF16).astype(F32)
            tile = [
                half[:, p * LANES : (p + 1) * LANES]
                for half in (high, amp - high)
                for p in range(pieces)
            ]
            if len(tile) < SMALL:
                tile.append(jnp.zeros((SMALL - len(tile), LANES), F32))
            to = place(mirror, own, i) * nslab + m
            out_ref[to, base : base + SMALL, :] = jnp.concatenate(tile, axis=0).astype(BF16)
            for t in range(nang // LANES):
                out_ref[to, t * slab : (t + 1) * slab, :] = final[
                    i, m * slab : (m + 1) * slab, t * LANES : (t + 1) * LANES
                ]


def per_device(
    psi_start,
    potential,
    basis,
    kinetic,
    radial_factor,
    damping,
    coupling,
    helicity,
    chan_rad,
    chan_vib,
    projector,
):
    _, slab, nvib, nang = psi_start.shape
    nquad = basis.shape[1]
    nchan = projector.shape[0]
    groups = lax.axis_size("g")
    own = lax.axis_size("hl")
    nslab = lax.axis_size("rad")
    blocks = groups * own
    group = lax.axis_index("g")
    nrad = nslab * slab
    share = nquad // own
    chunks = (nang + share) // WIDE
    height = (nang + share) // LANES * slab + SMALL
    shape = jax.ShapeDtypeStruct

    send = pl.pallas_call(
        functools.partial(pack, (slab, nvib, nang, share, blocks)),
        out_shape=shape((nvib, height, LANES), BF16),
        in_specs=[HBM] * 3 + [VMEM] + [HBM] * 2,
        out_specs=HBM,
        scratch_shapes=[
            pltpu.VMEM((chunks, slab * nvib, WIDE), F32),
            pltpu.VMEM((nvib, height, LANES), BF16),
            pltpu.VMEM((1, nang), BF16),
            pltpu.VMEM((1, slab), F32),
            pltpu.VMEM((1, slab), F32),
            pltpu.SemaphoreType.DMA((chunks,)),
            pltpu.SemaphoreType.DMA((chunks,)),
            pltpu.SemaphoreType.DMA((3,)),
        ],
        compiler_params=PARAMS,
        name="pack",
    )(
        in_hbm(psi_start.reshape(slab * nvib, nang)),
        in_hbm(potential.reshape(slab * nvib, nquad)),
        in_hbm(coupling),
        helicity[None],
        in_hbm(radial_factor[None]),
        in_hbm(damping[None]),
    )
    message = lax.all_to_all(send, ("hl", "rad"), 0, 0, tiled=True)

    mirror = groups == 2 and own >= ITERS
    sides = 1 if mirror else 2
    rows = message[:, share // LANES * slab :]
    halos = []
    for j in range(ITERS):
        if mirror:
            first = jnp.where(group == 0, own - 1 - j, j) * nslab
            part = lax.dynamic_slice_in_dim(rows, first, nslab, 0)
            halos.append([lax.ppermute(part, "g", [(0, 1), (1, 0)])])
            continue
        away, at = j // own + 1, j % own
        upper = rows[at * nslab : (at + 1) * nslab]
        lower = rows[(own - 1 - at) * nslab : (own - at) * nslab]
        up = [(i, i + away) for i in range(groups - away)]
        halos.append(
            [
                lax.ppermute(lower, "g", up),
                lax.ppermute(upper, "g", [(i, j) for j, i in up]),
            ]
        )

    full_type = shape((own, nrad, nang), F32)
    block_type = shape((own, nrad, nang), BF16)
    side_type = shape((sides, nrad, nang), F32)
    halo_type = shape((sides, nrad, nang), BF16)
    coup_type = shape((sides, 1, nang), F32)
    hat_type = shape((sides, 1, LANES), F32)
    dims = (own, nslab, slab, nang, nquad, mirror)

    def run(n, operands, specs, outs, scratch):
        count = (1 if mirror and n == 2 else own) + sides * (n - 1)
        return pl.pallas_call(
            functools.partial(advance, dims, sides, n),
            out_shape=outs,
            in_specs=specs,
            out_specs=[VMEM] * len(outs),
            scratch_shapes=scratch[:-1]
            + [
                pltpu.VMEM((count, nrad, nang), BF16),
                pltpu.VMEM((count * nrad, nquad), BF16),
                scratch[-1],
            ],
            compiler_params=PARAMS,
            cost_estimate=pl.CostEstimate(
                flops=4 * count * nrad * nang * nquad,
                bytes_accessed=8 * 1024 * 1024,
                transcendentals=0,
            ),
            name=f"advance{n}",
        )(*operands)

    new, first_b, basis, pot, radii, khat, coup, chain = run(
        1,
        [message, in_hbm(basis), kinetic],
        [VMEM, HBM, VMEM],
        [
            full_type,
            block_type,
            shape(basis.shape, BF16),
            shape((nrad, nquad), F32),
            shape((2, nrad, LANES), F32),
            shape((own, 1, LANES), F32),
            shape((own, 1, nang), F32),
            shape((max(own - 1, 1), 1, nang), F32),
        ],
        [pltpu.SemaphoreType.DMA((nquad // STEP,))],
    )
    common = [basis, kinetic, pot, radii, khat, coup, chain]
    joint = pltpu.VMEM((sides, 2, 1, nang), F32)
    operands = halos[0] + common + [new, first_b]
    if mirror:
        operands.append(
            pl.pallas_call(
                functools.partial(inner, dims),
                out_shape=shape((own - 1, nrad, nang), F32),
                in_specs=[VMEM] * 9,
                out_specs=VMEM,
                scratch_shapes=[
                    pltpu.VMEM((own - 1, nrad, nang), BF16),
                    pltpu.VMEM(((own - 1) * nrad, nquad), BF16),
                ],
                compiler_params=PARAMS,
                cost_estimate=pl.CostEstimate(
                    flops=4 * own * nrad * nang * nquad,
                    bytes_accessed=8 * 1024 * 1024,
                    transcendentals=0,
                ),
                name="inner",
            )(*common, new, first_b)
        )
    first_f, level1_b, new, halo_part, halo1_b, halo1_c, halo1_k = run(
        2,
        operands,
        [VMEM] * len(operands),
        [full_type, block_type, full_type, side_type, halo_type, coup_type, hat_type],
        [joint],
    )
    operands = (
        halos[1]
        + common
        + [new, first_b, first_f, halo_part, halo1_b, halo1_c, halo1_k, level1_b]
    )
    new, halo_part, far_part, halo2_c = run(
        3,
        operands,
        [VMEM] * len(operands),
        [full_type, side_type, side_type, coup_type],
        [
            pltpu.VMEM((own, nrad, nang), F32),
            pltpu.VMEM((sides, nrad, nang), BF16),
            pltpu.VMEM((sides, 1, LANES), F32),
            joint,
        ],
    )
    operands = halos[2] + [new, halo_part, far_part, halo1_c, halo2_c, coup, radii]
    operands += [chan_rad[None], chan_vib[None], projector]
    back = pl.pallas_call(
        functools.partial(close, dims, sides, nchan),
        out_shape=shape((own * nslab, nang // LANES * slab + SMALL, LANES), BF16),
        in_specs=[VMEM] * len(operands),
        out_specs=VMEM,
        scratch_shapes=[pltpu.VMEM((own, nrad, nang), BF16)],
        compiler_params=PARAMS,
        name="close",
    )(*operands)

    home = lax.all_to_all(back, ("hl", "rad"), 0, 0, tiled=True)
    chan = nchan // nslab
    psi_final, amplitude = pl.pallas_call(
        functools.partial(unpack, (slab, nvib, nang, -(-chan // LANES))),
        out_shape=[shape((slab * nvib, nang), F32), shape((1, chan), F32)],
        in_specs=[VMEM],
        out_specs=[HBM, VMEM],
        scratch_shapes=[
            pltpu.VMEM((slab * nvib, nang), F32),
            pltpu.SemaphoreType.DMA((nang // STEP,)),
        ],
        compiler_params=PARAMS,
        name="unpack",
    )(home)
    return (psi_final.reshape(1, slab, nvib, nang), amplitude)


def solution(mesh):
    nhel, nrad = mesh.shape["hel"], mesh.shape["rad"]

    def run(*args):
        nvib = args[0].shape[2]
        groups = nhel * nrad // nvib
        fine = Mesh(mesh.devices.reshape(groups, nhel // groups, nrad), ("g", "hl", "rad"))
        hel = ("g", "hl")
        placed = (
            P(hel, "rad", None, None),
            P("rad", None, None),
            P(),
            P(),
            P("rad"),
            P("rad"),
            P(hel, None),
            P(hel),
            P(),
            P(),
            P(),
        )
        return jax.shard_map(
            per_device,
            mesh=fine,
            in_specs=placed,
            out_specs=(P(hel, "rad", None, None), P(hel, "rad")),
            check_vma=False,
        )(*args)

    return run
```

```python
import functools

import jax
import jax.numpy as jnp
from jax import lax
from jax.experimental import pallas as pl
from jax.experimental.pallas import tpu as pltpu
from jax.sharding import Mesh
from jax.sharding import PartitionSpec as P

ITERS = 3
LANES = 128
STEP = 256
WIDE = 384
SMALL = 8
NT = (((1,), (1,)), ((), ()))
F32 = jnp.float32
BF16 = jnp.bfloat16
VMEM = pl.BlockSpec(memory_space=pltpu.VMEM)
HBM = pl.BlockSpec(memory_space=pltpu.HBM)
PARAMS = pltpu.CompilerParams(vmem_limit_bytes=24 * 1024 * 1024)


def in_hbm(array):
    return pltpu.with_memory_space_constraint(array, pltpu.HBM)


def moved_rows(rows, major):
    minor = rows // major
    at = lax.broadcasted_iota(jnp.int32, (1, rows), 1)
    dest = lax.rem(at, minor) * major + at // minor
    return (lax.broadcasted_iota(jnp.int32, (rows, rows), 0) == dest).astype(BF16)


def pack(
    dims, psi_ref, pot_ref, coup_ref, hel_ref, rf_ref, dp_ref, out_ref,
    wide, ready, coup, rf, dp, in_sems, out_sems, sems,
):
    slab, nvib, nang, share, blocks = dims
    near = lax.axis_size("hl")
    here = lax.axis_index("hl")
    is_last = lax.axis_index("g") * near + here == blocks - 1
    tall = WIDE // LANES * slab
    chunks = (nang + share) // WIDE
    height = (nang + share) // LANES * slab

    def load(i):
        if i * WIDE < share:
            first = pl.multiple_of(here * share + i * WIDE, LANES)
            source = pot_ref.at[:, pl.ds(first, WIDE)]
        else:
            source = psi_ref.at[:, pl.ds(i * WIDE - share, WIDE)]
        return pltpu.make_async_copy(source, wide.at[i], in_sems.at[i])

    def save(i):
        size = tall + (SMALL if i == chunks - 1 else 0)
        lines = pl.ds(i * tall, size)
        return pltpu.make_async_copy(
            ready.at[:, lines, :], out_ref.at[:, lines, :], out_sems.at[i]
        )

    small = [
        pltpu.make_async_copy(source, target, sems.at[i])
        for i, (source, target) in enumerate(
            [(coup_ref, coup), (rf_ref, rf), (dp_ref, dp)]
        )
    ]
    for i in range(chunks):
        load(i).start()
    for copy in small:
        copy.start()
    pick = moved_rows(slab * nvib, nvib)

    for copy in small:
        copy.wait()
    ce = jnp.where(is_last, 0.0, coup[...].astype(F32))
    lines = [ce[:, i * LANES : (i + 1) * LANES] for i in range(nang // LANES)]
    parts = []
    for value in (rf[...], dp[...]):
        high = value.astype(BF16).astype(F32)
        parts += [high, value - high]
    spread = (
        lax.rem(lax.broadcasted_iota(jnp.int32, (slab, LANES), 1), slab)
        == lax.broadcasted_iota(jnp.int32, (slab, LANES), 0)
    ).astype(BF16)
    filler = [jnp.zeros((SMALL - len(parts), slab), F32)]
    repeated = jnp.dot(
        jnp.concatenate(parts + filler, axis=0).astype(BF16), spread, preferred_element_type=F32
    )
    owner = lax.broadcasted_iota(jnp.int32, (SMALL, LANES), 1) // slab
    mine = owner == lax.broadcasted_iota(jnp.int32, (SMALL, LANES), 0)
    line = jnp.sum(jnp.where(mine, repeated, 0.0), axis=0, keepdims=True)
    lane = lax.broadcasted_iota(jnp.int32, (1, LANES), 1)
    lines.append(jnp.where(lane == LANES - 1, hel_ref[...].astype(F32), line))
    if len(lines) < SMALL:
        lines.append(jnp.zeros((SMALL - len(lines), LANES), F32))
    tile = jnp.concatenate(lines, axis=0).astype(BF16)
    for v in range(nvib):
        ready[v, height:, :] = tile

    for i in range(chunks):
        load(i).wait()
        moved = jnp.dot(pick, wide[i].astype(BF16), preferred_element_type=F32)
        moved = moved.astype(BF16).reshape(nvib, slab, WIDE)
        for t in range(WIDE // LANES):
            row = i * tall + t * slab
            ready[:, row : row + slab, :] = moved[:, :, t * LANES : (t + 1) * LANES]
        save(i).start()
    for i in range(chunks):
        save(i).wait()


def unpack(dims, msg_ref, out_ref, amp_ref, wide, sems):
    slab, nvib, nang, pieces = dims
    rows = slab * nvib
    tall = STEP // LANES * slab
    steps = nang // STEP

    def save(step):
        cols = pl.ds(step * STEP, STEP)
        return pltpu.make_async_copy(wide.at[:, cols], out_ref.at[:, cols], sems.at[step])

    pick = moved_rows(rows, slab)
    for step in range(steps):
        parts = [
            msg_ref[:, row : row + slab, :].reshape(rows, LANES)
            for row in range(step * tall, (step + 1) * tall, slab)
        ]
        wide[:, step * STEP : (step + 1) * STEP] = jnp.dot(
            pick, jnp.concatenate(parts, axis=1), preferred_element_type=F32
        )
        save(step).start()
    base = nang // LANES * slab
    lines = jnp.sum(msg_ref[:, base : base + SMALL, :].astype(F32), axis=0)
    lines = [lines[i : i + 1] + lines[pieces + i : pieces + i + 1] for i in range(pieces)]
    amp_ref[...] = jnp.concatenate(lines, axis=1)[:, : amp_ref.shape[1]]
    for step in range(steps):
        save(step).wait()


def rows_in(ref, first, count, slab, nang, base):
    return jnp.concatenate(
        [
            jnp.concatenate(
                [ref[m, base + i * slab : base + (i + 1) * slab, :] for i in range(nang // LANES)],
                axis=1,
            )
            for m in [first + i for i in range(count)]
        ],
        axis=0,
    )


def small_in(ref, m, base, nang):
    page = ref[m, base : base + SMALL, :].astype(F32)
    lines = [page[i : i + 1, :] for i in range(nang // LANES)]
    value = page[len(lines) : len(lines) + 1, LANES - 1 :]
    return jnp.concatenate(lines, axis=1), jnp.broadcast_to(-2.0 * value * value, (1, LANES))


def link(mirror, side, near, far):
    if mirror:
        return jnp.where(lax.axis_index("g") == 0, near, far)
    return far if side == 0 else near


def place(mirror, own, i):
    if mirror:
        return jnp.where(lax.axis_index("g") == 0, own - 1 - i, i)
    return i


def unfold(dims, msg_ref, src, pot, radii, khat, coup):
    own, nslab, slab, nang, nquad, mirror = dims
    share = nquad // own
    top = share // LANES * slab
    base = top + nang // LANES * slab
    lane = lax.broadcasted_iota(jnp.int32, (slab, LANES), 1)
    row = lax.broadcasted_iota(jnp.int32, (slab, LANES), 0)
    for k in range(own):
        for m in range(nslab):
            for t in range(share // LANES):
                cols = pl.ds(k * share + t * LANES, LANES)
                tile = msg_ref[k * nslab + m, t * slab : (t + 1) * slab, :]
                pot[m * slab : (m + 1) * slab, cols] = tile.astype(F32)
    for i in range(own):
        first = place(mirror, own, i) * nslab
        src[i] = rows_in(msg_ref, first, nslab, slab, nang, top)
        coup[i], khat[i] = small_in(msg_ref, first, base, nang)
    for m in range(nslab):
        page = msg_ref[m, base : base + SMALL, :].astype(F32)
        line = page[nang // LANES : nang // LANES + 1, :]
        for i in range(2):
            hit = (lane == row + 2 * i * slab) | (lane == row + (2 * i + 1) * slab)
            value = jnp.sum(jnp.where(hit, line, 0.0), axis=1, keepdims=True)
            radii[i, m * slab : (m + 1) * slab, :] = jnp.broadcast_to(value, (slab, LANES))


def wider(tile, size):
    return jnp.concatenate([tile] * (size // LANES), axis=1)


def inner(dims, *refs):
    own, nslab, slab, nang, nquad, mirror = dims
    nrad = nslab * slab
    basis, kin_ref, pot, radii, khat, coup, chain, part, first_b, new_ref, rows, scaled = refs
    count = own - 1
    for i in range(count):
        rows[i] = part[i + 1].astype(BF16)

    @pl.loop(0, nquad // STEP)
    def _(qi):
        cols = pl.ds(pl.multiple_of(qi * STEP, STEP), STEP)
        grid = jnp.dot(
            rows[...].reshape(count * nrad, nang), basis[:, cols], preferred_element_type=F32
        )
        prod = grid.reshape(count, nrad, STEP) * pot[:, cols][None]
        scaled[:, cols] = prod.astype(BF16).reshape(count * nrad, STEP)

    factor = wider(radii[0], STEP)
    damp = wider(radii[1], STEP)

    @pl.loop(0, nang // STEP)
    def _(ji):
        cols = pl.ds(pl.multiple_of(ji * STEP, STEP), STEP)
        ang = lax.dot_general(
            scaled[...], basis[cols, :], NT, preferred_element_type=F32
        ).reshape(count, nrad, STEP)
        for i in range(count):
            total = ang[i] + jnp.dot(
                kin_ref[...], rows[i, :, cols], preferred_element_type=F32
            )
            total += wider(khat[i + 1], STEP) * factor * part[i + 1, :, cols]
            if i + 1 < count:
                total += chain[i + 1, :, cols] * rows[i + 1, :, cols].astype(F32)
            if i > 0:
                total += chain[i, :, cols] * rows[i - 1, :, cols].astype(F32)
            before = first_b[i + 1, :, cols].astype(F32)
            new_ref[i, :, cols] = damp * (2.0 * total - damp * before)


def advance(dims, sides, n, *refs):
    own, nslab, slab, nang, nquad, mirror = dims
    nrad = nslab * slab
    refs = list(refs)
    take = lambda count: [refs.pop(0) for _ in range(count)]
    edge_of = [0, own - 1]
    if n == 1:
        msg_ref, basis, kin_ref = take(3)
        new_ref, src, pot, radii, khat, coup, chain = take(7)
        rows, scaled = take(2)
        unfold(dims, msg_ref, src, pot, radii, khat, coup)
        rows[...] = src[...]
        for i in range(own - 1):
            chain[i] = link(mirror, 0, coup[i + 1], coup[i])
    else:
        raw = take(sides)
        basis, kin_ref, pot, radii, khat, coup, chain = take(7)
        scale = wider(radii[1] if n == 2 else 2.0 * radii[1], nang)
        base = nang // LANES * slab
        if n == 2:
            part, first_b = take(2)
            inner_ref = take(1)[0] if mirror else None
            full, block, new_ref, part_h, halo_b, halo_c, halo_k = take(7)
            rows, scaled, joint = take(3)
        else:
            part, first_b, first_f, halo_part, halo1_b, halo1_c, halo1_k, level1_b = take(8)
            new_ref, part_h, part_hh, halo_c = take(4)
            full, halo_b, halo_k, rows, scaled, joint = take(6)
        split = mirror and n == 2
        level = block if split else rows
        shift = 1 if split else own
        for i in range(own):
            value = part[i]
            full[i] = value
            level[i] = value.astype(BF16)
        for s in range(sides):
            halo_b[s] = rows_in(raw[s], 0, nslab, slab, nang, 0)
            halo_c[s], halo_k[s] = small_in(raw[s], 0, base, nang)
            at = edge_of[s]
            if n == 2:
                joint[s, 0] = link(mirror, s, coup[at], halo_c[s])
                seen = halo_b[s]
                rows[shift + s] = seen
            else:
                joint[s, 0] = link(mirror, s, coup[at], halo1_c[s])
                joint[s, 1] = link(mirror, s, halo1_c[s], halo_c[s])
                value = halo_part[s] + wider(radii[1], nang) * (
                    joint[s, 1] * halo_b[s].astype(F32)
                )
                seen = value.astype(BF16)
                rows[own + s] = seen
                rows[own + sides + s] = halo_b[s]
            value = full[at] + scale * (joint[s, 0] * seen.astype(F32))
            full[at] = value
            level[at] = value.astype(BF16)
        if split:
            rows[0] = block[0]
        elif n == 2:
            block[...] = rows[:own]
    if n == 1:
        split, level, shift = False, rows, own
    count = shift + sides * (n - 1)

    @pl.loop(0, nquad // STEP)
    def _(qi):
        cols = pl.ds(pl.multiple_of(qi * STEP, STEP), STEP)
        grid = jnp.dot(
            rows[...].reshape(count * nrad, nang), basis[:, cols], preferred_element_type=F32
        )
        prod = grid.reshape(count, nrad, STEP) * pot[:, cols][None]
        scaled[:, cols] = prod.astype(BF16).reshape(count * nrad, STEP)

    factor = wider(radii[0], STEP)
    damp = wider(radii[1], STEP)

    @pl.loop(0, nang // STEP)
    def _(ji):
        cols = pl.ds(pl.multiple_of(ji * STEP, STEP), STEP)
        ang = lax.dot_general(
            scaled[...], basis[cols, :], NT, preferred_element_type=F32
        ).reshape(count, nrad, STEP)

        def local(i, hat, value):
            kin = jnp.dot(kin_ref[...], rows[i, :, cols], preferred_element_type=F32)
            return ang[i] + kin + wider(hat, STEP) * factor * value

        for i in range(own):
            if split and i > 0:
                value = inner_ref[i - 1, :, cols]
                if i == 1:
                    value += 2.0 * damp * (chain[0, :, cols] * level[0, :, cols].astype(F32))
                new_ref[i, :, cols] = value
                continue
            value = rows[i, :, cols].astype(F32) if n == 1 else full[i, :, cols]
            total = local(i, khat[i], value)
            if i + 1 < own:
                total += chain[i, :, cols] * level[i + 1, :, cols].astype(F32)
            if i > 0:
                total += chain[i - 1, :, cols] * level[i - 1, :, cols].astype(F32)
            if n == 1:
                new_ref[i, :, cols] = damp * total
            else:
                before = first_b if n == 2 else first_f
                new_ref[i, :, cols] = damp * (
                    2.0 * total - damp * before[i, :, cols].astype(F32)
                )
        for s in range(sides if n > 1 else 0):
            at = edge_of[s]
            i = shift + s
            hat = halo_k[s] if n == 2 else halo1_k[s]
            total = local(i, hat, rows[i, :, cols].astype(F32))
            edge_b = first_b if n == 2 else level1_b
            total += joint[s, 0, :, cols] * edge_b[at, :, cols].astype(F32)
            if n == 2:
                part_h[s, :, cols] = damp * total
                continue
            before = halo1_b[s, :, cols].astype(F32)
            part_h[s, :, cols] = damp * (2.0 * total - damp * before)
            i = own + sides + s
            total = local(i, halo_k[s], rows[i, :, cols].astype(F32))
            total += joint[s, 1, :, cols] * before
            part_hh[s, :, cols] = damp * total


def close(dims, sides, nchan, *refs):
    own, nslab, slab, nang, nquad, mirror = dims
    nrad = nslab * slab
    raw, refs = refs[:sides], refs[sides:]
    part, part_h, part_hh, halo1_c, halo2_c, coup, radii = refs[:7]
    rad_ref, vib_ref, proj_ref, out_ref, final = refs[7:]
    base = nang // LANES * slab
    damp = wider(radii[1], nang)
    for i in range(own):
        final[i] = part[i].astype(BF16)
    for s in range(sides):
        at = 0 if s == 0 else own - 1
        far = rows_in(raw[s], 0, nslab, slab, nang, 0).astype(F32)
        far_c, _ = small_in(raw[s], 0, base, nang)
        value = part_hh[s] + damp * (link(mirror, s, halo2_c[s], far_c) * far)
        value = value.astype(BF16).astype(F32)
        value = part_h[s] + 2.0 * damp * (link(mirror, s, halo1_c[s], halo2_c[s]) * value)
        value = value.astype(BF16).astype(F32)
        term = 2.0 * damp * (link(mirror, s, coup[at], halo1_c[s]) * value)
        fixed = (part[at] if s == 0 or own > 1 else fixed) + term
        final[at] = fixed.astype(BF16)

    chan = nchan // nslab
    pieces = -(-chan // LANES)
    vib = lax.axis_index("hl") * nslab + lax.axis_index("rad")
    rows_at = lax.broadcasted_iota(jnp.int32, (nrad, chan), 0)
    for m in range(nslab):
        cols = slice(m * chan, (m + 1) * chan)
        table = lax.dot_general(
            final[...].reshape(own * nrad, nang),
            proj_ref[cols, :],
            NT,
            preferred_element_type=F32,
        ).reshape(own, nrad, chan)
        hit = (rows_at == rad_ref[:, cols]) & (vib_ref[:, cols] == vib)
        for i in range(own):
            amp = jnp.sum(jnp.where(hit, table[i], 0.0), axis=0, keepdims=True)
            if pieces * LANES > chan:
                amp = jnp.concatenate([amp, jnp.zeros((1, pieces * LANES - chan), F32)], axis=1)
            high = amp.astype(BF16).astype(F32)
            tile = [
                half[:, p * LANES : (p + 1) * LANES]
                for half in (high, amp - high)
                for p in range(pieces)
            ]
            if len(tile) < SMALL:
                tile.append(jnp.zeros((SMALL - len(tile), LANES), F32))
            to = place(mirror, own, i) * nslab + m
            out_ref[to, base : base + SMALL, :] = jnp.concatenate(tile, axis=0).astype(BF16)
            for t in range(nang // LANES):
                out_ref[to, t * slab : (t + 1) * slab, :] = final[
                    i, m * slab : (m + 1) * slab, t * LANES : (t + 1) * LANES
                ]


def per_device(
    psi_start,
    potential,
    basis,
    kinetic,
    radial_factor,
    damping,
    coupling,
    helicity,
    chan_rad,
    chan_vib,
    projector,
):
    _, slab, nvib, nang = psi_start.shape
    nquad = basis.shape[1]
    nchan = projector.shape[0]
    groups = lax.axis_size("g")
    own = lax.axis_size("hl")
    nslab = lax.axis_size("rad")
    blocks = groups * own
    group = lax.axis_index("g")
    nrad = nslab * slab
    share = nquad // own
    chunks = (nang + share) // WIDE
    height = (nang + share) // LANES * slab + SMALL
    shape = jax.ShapeDtypeStruct

    send = pl.pallas_call(
        functools.partial(pack, (slab, nvib, nang, share, blocks)),
        out_shape=shape((nvib, height, LANES), BF16),
        in_specs=[HBM] * 3 + [VMEM] + [HBM] * 2,
        out_specs=HBM,
        scratch_shapes=[
            pltpu.VMEM((chunks, slab * nvib, WIDE), F32),
            pltpu.VMEM((nvib, height, LANES), BF16),
            pltpu.VMEM((1, nang), BF16),
            pltpu.VMEM((1, slab), F32),
            pltpu.VMEM((1, slab), F32),
            pltpu.SemaphoreType.DMA((chunks,)),
            pltpu.SemaphoreType.DMA((chunks,)),
            pltpu.SemaphoreType.DMA((3,)),
        ],
        compiler_params=PARAMS,
        name="pack",
    )(
        in_hbm(psi_start.reshape(slab * nvib, nang)),
        in_hbm(potential.reshape(slab * nvib, nquad)),
        in_hbm(coupling),
        helicity[None],
        in_hbm(radial_factor[None]),
        in_hbm(damping[None]),
    )
    message = lax.all_to_all(send, ("hl", "rad"), 0, 0, tiled=True)

    mirror = groups == 2 and own >= ITERS
    sides = 1 if mirror else 2
    rows = message[:, share // LANES * slab :]
    halos = []
    for j in range(ITERS):
        if mirror:
            first = jnp.where(group == 0, own - 1 - j, j) * nslab
            part = lax.dynamic_slice_in_dim(rows, first, nslab, 0)
            halos.append([lax.ppermute(part, "g", [(0, 1), (1, 0)])])
            continue
        away, at = j // own + 1, j % own
        upper = rows[at * nslab : (at + 1) * nslab]
        lower = rows[(own - 1 - at) * nslab : (own - at) * nslab]
        up = [(i, i + away) for i in range(groups - away)]
        halos.append(
            [
                lax.ppermute(lower, "g", up),
                lax.ppermute(upper, "g", [(i, j) for j, i in up]),
            ]
        )

    full_type = shape((own, nrad, nang), F32)
    block_type = shape((own, nrad, nang), BF16)
    side_type = shape((sides, nrad, nang), F32)
    halo_type = shape((sides, nrad, nang), BF16)
    coup_type = shape((sides, 1, nang), F32)
    hat_type = shape((sides, 1, LANES), F32)
    dims = (own, nslab, slab, nang, nquad, mirror)

    def run(n, operands, specs, outs, scratch):
        count = (1 if mirror and n == 2 else own) + sides * (n - 1)
        return pl.pallas_call(
            functools.partial(advance, dims, sides, n),
            out_shape=outs,
            in_specs=specs,
            out_specs=[VMEM] * len(outs),
            scratch_shapes=scratch[:-1]
            + [
                pltpu.VMEM((count, nrad, nang), BF16),
                pltpu.VMEM((count * nrad, nquad), BF16),
            ]
            + scratch[-1:],
            compiler_params=PARAMS,
            cost_estimate=pl.CostEstimate(
                flops=4 * count * nrad * nang * nquad,
                bytes_accessed=8 * 1024 * 1024,
                transcendentals=0,
            ),
            name=f"advance{n}",
        )(*operands)

    new, first_b, pot, radii, khat, coup, chain = run(
        1,
        [message, basis, kinetic],
        [VMEM] * 3,
        [
            full_type,
            block_type,
            shape((nrad, nquad), F32),
            shape((2, nrad, LANES), F32),
            shape((own, 1, LANES), F32),
            shape((own, 1, nang), F32),
            shape((max(own - 1, 1), 1, nang), F32),
        ],
        [],
    )
    common = [basis, kinetic, pot, radii, khat, coup, chain]
    joint = pltpu.VMEM((sides, 2, 1, nang), F32)
    operands = halos[0] + common + [new, first_b]
    if mirror:
        operands.append(
            pl.pallas_call(
                functools.partial(inner, dims),
                out_shape=shape((own - 1, nrad, nang), F32),
                in_specs=[VMEM] * 9,
                out_specs=VMEM,
                scratch_shapes=[
                    pltpu.VMEM((own - 1, nrad, nang), BF16),
                    pltpu.VMEM(((own - 1) * nrad, nquad), BF16),
                ],
                compiler_params=PARAMS,
                cost_estimate=pl.CostEstimate(
                    flops=4 * own * nrad * nang * nquad,
                    bytes_accessed=8 * 1024 * 1024,
                    transcendentals=0,
                ),
                name="inner",
            )(*common, new, first_b)
        )
    first_f, level1_b, new, halo_part, halo1_b, halo1_c, halo1_k = run(
        2,
        operands,
        [VMEM] * len(operands),
        [full_type, block_type, full_type, side_type, halo_type, coup_type, hat_type],
        [joint],
    )
    operands = (
        halos[1]
        + common
        + [new, first_b, first_f, halo_part, halo1_b, halo1_c, halo1_k, level1_b]
    )
    new, halo_part, far_part, halo2_c = run(
        3,
        operands,
        [VMEM] * len(operands),
        [full_type, side_type, side_type, coup_type],
        [
            pltpu.VMEM((own, nrad, nang), F32),
            pltpu.VMEM((sides, nrad, nang), BF16),
            pltpu.VMEM((sides, 1, LANES), F32),
            joint,
        ],
    )
    operands = halos[2] + [new, halo_part, far_part, halo1_c, halo2_c, coup, radii]
    operands += [chan_rad[None], chan_vib[None], projector]
    back = pl.pallas_call(
        functools.partial(close, dims, sides, nchan),
        out_shape=shape((own * nslab, nang // LANES * slab + SMALL, LANES), BF16),
        in_specs=[VMEM] * len(operands),
        out_specs=VMEM,
        scratch_shapes=[pltpu.VMEM((own, nrad, nang), BF16)],
        compiler_params=PARAMS,
        name="close",
    )(*operands)

    home = lax.all_to_all(back, ("hl", "rad"), 0, 0, tiled=True)
    chan = nchan // nslab
    psi_final, amplitude = pl.pallas_call(
        functools.partial(unpack, (slab, nvib, nang, -(-chan // LANES))),
        out_shape=[shape((slab * nvib, nang), F32), shape((1, chan), F32)],
        in_specs=[VMEM],
        out_specs=[HBM, VMEM],
        scratch_shapes=[
            pltpu.VMEM((slab * nvib, nang), F32),
            pltpu.SemaphoreType.DMA((nang // STEP,)),
        ],
        compiler_params=PARAMS,
        name="unpack",
    )(home)
    return (psi_final.reshape(1, slab, nvib, nang), amplitude)


def solution(mesh):
    nhel, nrad = mesh.shape["hel"], mesh.shape["rad"]

    def run(*args):
        nvib = args[0].shape[2]
        groups = nhel * nrad // nvib
        fine = Mesh(mesh.devices.reshape(groups, nhel // groups, nrad), ("g", "hl", "rad"))
        hel = ("g", "hl")
        placed = (
            P(hel, "rad", None, None),
            P("rad", None, None),
            P(),
            P(),
            P("rad"),
            P("rad"),
            P(hel, None),
            P(hel),
            P(),
            P(),
            P(),
        )
        return jax.shard_map(
            per_device,
            mesh=fine,
            in_specs=placed,
            out_specs=(P(hel, "rad", None, None), P(hel, "rad")),
            check_vma=False,
        )(*args)

    return run
```

```python
import functools

import jax
import jax.numpy as jnp
from jax import lax
from jax.experimental import pallas as pl
from jax.experimental.pallas import tpu as pltpu
from jax.sharding import Mesh
from jax.sharding import PartitionSpec as P

ITERS = 3
LANES = 128
STEP = 256
WIDE = 384
SMALL = 8
NT = (((1,), (1,)), ((), ()))
F32 = jnp.float32
BF16 = jnp.bfloat16
VMEM = pl.BlockSpec(memory_space=pltpu.VMEM)
HBM = pl.BlockSpec(memory_space=pltpu.HBM)
PARAMS = pltpu.CompilerParams(vmem_limit_bytes=24 * 1024 * 1024)


def in_hbm(array):
    return pltpu.with_memory_space_constraint(array, pltpu.HBM)


def moved_rows(rows, major):
    minor = rows // major
    at = lax.broadcasted_iota(jnp.int32, (1, rows), 1)
    dest = lax.rem(at, minor) * major + at // minor
    return (lax.broadcasted_iota(jnp.int32, (rows, rows), 0) == dest).astype(BF16)


def pack(
    dims, psi_ref, pot_ref, coup_ref, hel_ref, rf_ref, dp_ref, out_ref,
    wide, ready, coup, rf, dp, in_sems, out_sems, sems,
):
    slab, nvib, nang, share, blocks = dims
    near = lax.axis_size("hl")
    here = lax.axis_index("hl")
    is_last = lax.axis_index("g") * near + here == blocks - 1
    tall = WIDE // LANES * slab
    chunks = (nang + share) // WIDE
    height = (nang + share) // LANES * slab

    def load(i):
        if i * WIDE < share:
            first = pl.multiple_of(here * share + i * WIDE, LANES)
            source = pot_ref.at[:, pl.ds(first, WIDE)]
        else:
            source = psi_ref.at[:, pl.ds(i * WIDE - share, WIDE)]
        return pltpu.make_async_copy(source, wide.at[i], in_sems.at[i])

    def save(i):
        size = tall + (SMALL if i == chunks - 1 else 0)
        lines = pl.ds(i * tall, size)
        return pltpu.make_async_copy(
            ready.at[:, lines, :], out_ref.at[:, lines, :], out_sems.at[i]
        )

    small = [
        pltpu.make_async_copy(source, target, sems.at[i])
        for i, (source, target) in enumerate(
            [(coup_ref, coup), (rf_ref, rf), (dp_ref, dp)]
        )
    ]
    for i in range(chunks):
        load(i).start()
    for copy in small:
        copy.start()
    pick = moved_rows(slab * nvib, nvib)

    for copy in small:
        copy.wait()
    ce = jnp.where(is_last, 0.0, coup[...].astype(F32))
    lines = [ce[:, i * LANES : (i + 1) * LANES] for i in range(nang // LANES)]
    parts = []
    for value in (rf[...], dp[...]):
        high = value.astype(BF16).astype(F32)
        parts += [high, value - high]
    spread = (
        lax.rem(lax.broadcasted_iota(jnp.int32, (slab, LANES), 1), slab)
        == lax.broadcasted_iota(jnp.int32, (slab, LANES), 0)
    ).astype(BF16)
    filler = [jnp.zeros((SMALL - len(parts), slab), F32)]
    repeated = jnp.dot(
        jnp.concatenate(parts + filler, axis=0).astype(BF16), spread, preferred_element_type=F32
    )
    owner = lax.broadcasted_iota(jnp.int32, (SMALL, LANES), 1) // slab
    mine = owner == lax.broadcasted_iota(jnp.int32, (SMALL, LANES), 0)
    line = jnp.sum(jnp.where(mine, repeated, 0.0), axis=0, keepdims=True)
    lane = lax.broadcasted_iota(jnp.int32, (1, LANES), 1)
    lines.append(jnp.where(lane == LANES - 1, hel_ref[...].astype(F32), line))
    if len(lines) < SMALL:
        lines.append(jnp.zeros((SMALL - len(lines), LANES), F32))
    tile = jnp.concatenate(lines, axis=0).astype(BF16)
    for v in range(nvib):
        ready[v, height:, :] = tile

    for i in range(chunks):
        load(i).wait()
        moved = jnp.dot(pick, wide[i].astype(BF16), preferred_element_type=F32)
        moved = moved.astype(BF16).reshape(nvib, slab, WIDE)
        for t in range(WIDE // LANES):
            row = i * tall + t * slab
            ready[:, row : row + slab, :] = moved[:, :, t * LANES : (t + 1) * LANES]
        save(i).start()
    for i in range(chunks):
        save(i).wait()


def unpack(dims, msg_ref, out_ref, amp_ref, wide, sems):
    slab, nvib, nang, pieces = dims
    rows = slab * nvib
    tall = STEP // LANES * slab
    steps = nang // STEP

    def save(step):
        cols = pl.ds(step * STEP, STEP)
        return pltpu.make_async_copy(wide.at[:, cols], out_ref.at[:, cols], sems.at[step])

    pick = moved_rows(rows, slab)
    for step in range(steps):
        parts = [
            msg_ref[:, row : row + slab, :].reshape(rows, LANES)
            for row in range(step * tall, (step + 1) * tall, slab)
        ]
        wide[:, step * STEP : (step + 1) * STEP] = jnp.dot(
            pick, jnp.concatenate(parts, axis=1), preferred_element_type=F32
        )
        save(step).start()
    base = nang // LANES * slab
    lines = jnp.sum(msg_ref[:, base : base + SMALL, :].astype(F32), axis=0)
    lines = [lines[i : i + 1] + lines[pieces + i : pieces + i + 1] for i in range(pieces)]
    amp_ref[...] = jnp.concatenate(lines, axis=1)[:, : amp_ref.shape[1]]
    for step in range(steps):
        save(step).wait()


def rows_in(ref, first, count, slab, nang, base):
    return jnp.concatenate(
        [
            jnp.concatenate(
                [ref[m, base + i * slab : base + (i + 1) * slab, :] for i in range(nang // LANES)],
                axis=1,
            )
            for m in [first + i for i in range(count)]
        ],
        axis=0,
    )


def small_in(ref, m, base, nang):
    page = ref[m, base : base + SMALL, :].astype(F32)
    lines = [page[i : i + 1, :] for i in range(nang // LANES)]
    value = page[len(lines) : len(lines) + 1, LANES - 1 :]
    return jnp.concatenate(lines, axis=1), jnp.broadcast_to(-2.0 * value * value, (1, LANES))


def link(mirror, side, near, far):
    if mirror:
        return jnp.where(lax.axis_index("g") == 0, near, far)
    return far if side == 0 else near


def place(mirror, own, i):
    if mirror:
        return jnp.where(lax.axis_index("g") == 0, own - 1 - i, i)
    return i


def unfold(dims, msg_ref, src, pot, radii, khat, coup):
    own, nslab, slab, nang, nquad, mirror = dims
    share = nquad // own
    top = share // LANES * slab
    base = top + nang // LANES * slab
    lane = lax.broadcasted_iota(jnp.int32, (slab, LANES), 1)
    row = lax.broadcasted_iota(jnp.int32, (slab, LANES), 0)
    for k in range(own):
        for m in range(nslab):
            for t in range(share // LANES):
                cols = pl.ds(k * share + t * LANES, LANES)
                tile = msg_ref[k * nslab + m, t * slab : (t + 1) * slab, :]
                pot[m * slab : (m + 1) * slab, cols] = tile.astype(F32)
    for i in range(own):
        first = place(mirror, own, i) * nslab
        src[i] = rows_in(msg_ref, first, nslab, slab, nang, top)
        coup[i], khat[i] = small_in(msg_ref, first, base, nang)
    for m in range(nslab):
        page = msg_ref[m, base : base + SMALL, :].astype(F32)
        line = page[nang // LANES : nang // LANES + 1, :]
        for i in range(2):
            hit = (lane == row + 2 * i * slab) | (lane == row + (2 * i + 1) * slab)
            value = jnp.sum(jnp.where(hit, line, 0.0), axis=1, keepdims=True)
            radii[i, m * slab : (m + 1) * slab, :] = jnp.broadcast_to(value, (slab, LANES))


def wider(tile, size):
    return jnp.concatenate([tile] * (size // LANES), axis=1)


def inner(dims, *refs):
    own, nslab, slab, nang, nquad, mirror = dims
    nrad = nslab * slab
    basis, kin_ref, pot, radii, khat, coup, chain, part, first_b, msg_ref = refs[:10]
    new_ref, send_ref, rows, scaled = refs[10:]
    top = nquad // own // LANES * slab
    first = place(mirror, own, ITERS - 1) * nslab
    for m in range(nslab):
        send_ref[m] = msg_ref[first + m, top:, :]
    count = own - 1
    for i in range(count):
        rows[i] = part[i + 1].astype(BF16)

    @pl.loop(0, nquad // STEP)
    def _(qi):
        cols = pl.ds(pl.multiple_of(qi * STEP, STEP), STEP)
        grid = jnp.dot(
            rows[...].reshape(count * nrad, nang), basis[:, cols], preferred_element_type=F32
        )
        prod = grid.reshape(count, nrad, STEP) * pot[:, cols][None]
        scaled[:, cols] = prod.astype(BF16).reshape(count * nrad, STEP)

    factor = wider(radii[0], STEP)
    damp = wider(radii[1], STEP)

    @pl.loop(0, nang // STEP)
    def _(ji):
        cols = pl.ds(pl.multiple_of(ji * STEP, STEP), STEP)
        ang = lax.dot_general(
            scaled[...], basis[cols, :], NT, preferred_element_type=F32
        ).reshape(count, nrad, STEP)
        for i in range(count):
            total = ang[i] + jnp.dot(
                kin_ref[...], rows[i, :, cols], preferred_element_type=F32
            )
            total += wider(khat[i + 1], STEP) * factor * part[i + 1, :, cols]
            if i + 1 < count:
                total += chain[i + 1, :, cols] * rows[i + 1, :, cols].astype(F32)
            if i > 0:
                total += chain[i, :, cols] * rows[i - 1, :, cols].astype(F32)
            before = first_b[i + 1, :, cols].astype(F32)
            new_ref[i, :, cols] = damp * (2.0 * total - damp * before)


def advance(dims, sides, n, *refs):
    own, nslab, slab, nang, nquad, mirror = dims
    nrad = nslab * slab
    refs = list(refs)
    take = lambda count: [refs.pop(0) for _ in range(count)]
    edge_of = [0, own - 1]
    if n == 1:
        msg_ref, basis, kin_ref = take(3)
        new_ref, src, pot, radii, khat, coup, chain = take(7)
        rows, scaled = take(2)
        unfold(dims, msg_ref, src, pot, radii, khat, coup)
        rows[...] = src[...]
        for i in range(own - 1):
            chain[i] = link(mirror, 0, coup[i + 1], coup[i])
    else:
        raw = take(sides)
        basis, kin_ref, pot, radii, khat, coup, chain = take(7)
        scale = wider(radii[1] if n == 2 else 2.0 * radii[1], nang)
        base = nang // LANES * slab
        if n == 2:
            part, first_b = take(2)
            inner_ref = take(1)[0] if mirror else None
            full, block, new_ref, part_h, halo_b, halo_c, halo_k = take(7)
            rows, scaled, joint = take(3)
        else:
            part, first_b, first_f, halo_part, halo1_b, halo1_c, halo1_k, level1_b = take(8)
            new_ref, part_h, part_hh, halo_c = take(4)
            full, halo_b, halo_k, rows, scaled, joint = take(6)
        split = mirror and n == 2
        level = block if split else rows
        shift = 1 if split else own
        for i in range(own):
            value = part[i]
            full[i] = value
            level[i] = value.astype(BF16)
        for s in range(sides):
            halo_b[s] = rows_in(raw[s], 0, nslab, slab, nang, 0)
            halo_c[s], halo_k[s] = small_in(raw[s], 0, base, nang)
            at = edge_of[s]
            if n == 2:
                joint[s, 0] = link(mirror, s, coup[at], halo_c[s])
                seen = halo_b[s]
                rows[shift + s] = seen
            else:
                joint[s, 0] = link(mirror, s, coup[at], halo1_c[s])
                joint[s, 1] = link(mirror, s, halo1_c[s], halo_c[s])
                value = halo_part[s] + wider(radii[1], nang) * (
                    joint[s, 1] * halo_b[s].astype(F32)
                )
                seen = value.astype(BF16)
                rows[own + s] = seen
                rows[own + sides + s] = halo_b[s]
            value = full[at] + scale * (joint[s, 0] * seen.astype(F32))
            full[at] = value
            level[at] = value.astype(BF16)
        if split:
            rows[0] = block[0]
        elif n == 2:
            block[...] = rows[:own]
    if n == 1:
        split, level, shift = False, rows, own
    count = shift + sides * (n - 1)

    @pl.loop(0, nquad // STEP)
    def _(qi):
        cols = pl.ds(pl.multiple_of(qi * STEP, STEP), STEP)
        grid = jnp.dot(
            rows[...].reshape(count * nrad, nang), basis[:, cols], preferred_element_type=F32
        )
        prod = grid.reshape(count, nrad, STEP) * pot[:, cols][None]
        scaled[:, cols] = prod.astype(BF16).reshape(count * nrad, STEP)

    factor = wider(radii[0], STEP)
    damp = wider(radii[1], STEP)

    @pl.loop(0, nang // STEP)
    def _(ji):
        cols = pl.ds(pl.multiple_of(ji * STEP, STEP), STEP)
        ang = lax.dot_general(
            scaled[...], basis[cols, :], NT, preferred_element_type=F32
        ).reshape(count, nrad, STEP)

        def local(i, hat, value):
            kin = jnp.dot(kin_ref[...], rows[i, :, cols], preferred_element_type=F32)
            return ang[i] + kin + wider(hat, STEP) * factor * value

        for i in range(own):
            if split and i > 0:
                value = inner_ref[i - 1, :, cols]
                if i == 1:
                    value += 2.0 * damp * (chain[0, :, cols] * level[0, :, cols].astype(F32))
                new_ref[i, :, cols] = value
                continue
            value = rows[i, :, cols].astype(F32) if n == 1 else full[i, :, cols]
            total = local(i, khat[i], value)
            if i + 1 < own:
                total += chain[i, :, cols] * level[i + 1, :, cols].astype(F32)
            if i > 0:
                total += chain[i - 1, :, cols] * level[i - 1, :, cols].astype(F32)
            if n == 1:
                new_ref[i, :, cols] = damp * total
            else:
                before = first_b if n == 2 else first_f
                new_ref[i, :, cols] = damp * (
                    2.0 * total - damp * before[i, :, cols].astype(F32)
                )
        for s in range(sides if n > 1 else 0):
            at = edge_of[s]
            i = shift + s
            hat = halo_k[s] if n == 2 else halo1_k[s]
            total = local(i, hat, rows[i, :, cols].astype(F32))
            edge_b = first_b if n == 2 else level1_b
            total += joint[s, 0, :, cols] * edge_b[at, :, cols].astype(F32)
            if n == 2:
                part_h[s, :, cols] = damp * total
                continue
            before = halo1_b[s, :, cols].astype(F32)
            part_h[s, :, cols] = damp * (2.0 * total - damp * before)
            i = own + sides + s
            total = local(i, halo_k[s], rows[i, :, cols].astype(F32))
            total += joint[s, 1, :, cols] * before
            part_hh[s, :, cols] = damp * total


def close(dims, sides, nchan, *refs):
    own, nslab, slab, nang, nquad, mirror = dims
    nrad = nslab * slab
    raw, refs = refs[:sides], refs[sides:]
    part, part_h, part_hh, halo1_c, halo2_c, coup, radii = refs[:7]
    rad_ref, vib_ref, proj_ref, out_ref, final = refs[7:]
    base = nang // LANES * slab
    damp = wider(radii[1], nang)
    for i in range(own):
        final[i] = part[i].astype(BF16)
    for s in range(sides):
        at = 0 if s == 0 else own - 1
        far = rows_in(raw[s], 0, nslab, slab, nang, 0).astype(F32)
        far_c, _ = small_in(raw[s], 0, base, nang)
        value = part_hh[s] + damp * (link(mirror, s, halo2_c[s], far_c) * far)
        value = value.astype(BF16).astype(F32)
        value = part_h[s] + 2.0 * damp * (link(mirror, s, halo1_c[s], halo2_c[s]) * value)
        value = value.astype(BF16).astype(F32)
        term = 2.0 * damp * (link(mirror, s, coup[at], halo1_c[s]) * value)
        fixed = (part[at] if s == 0 or own > 1 else fixed) + term
        final[at] = fixed.astype(BF16)

    chan = nchan // nslab
    pieces = -(-chan // LANES)
    vib = lax.axis_index("hl") * nslab + lax.axis_index("rad")
    rows_at = lax.broadcasted_iota(jnp.int32, (nrad, chan), 0)
    for m in range(nslab):
        cols = slice(m * chan, (m + 1) * chan)
        table = lax.dot_general(
            final[...].reshape(own * nrad, nang),
            proj_ref[cols, :],
            NT,
            preferred_element_type=F32,
        ).reshape(own, nrad, chan)
        hit = (rows_at == rad_ref[:, cols]) & (vib_ref[:, cols] == vib)
        for i in range(own):
            amp = jnp.sum(jnp.where(hit, table[i], 0.0), axis=0, keepdims=True)
            if pieces * LANES > chan:
                amp = jnp.concatenate([amp, jnp.zeros((1, pieces * LANES - chan), F32)], axis=1)
            high = amp.astype(BF16).astype(F32)
            tile = [
                half[:, p * LANES : (p + 1) * LANES]
                for half in (high, amp - high)
                for p in range(pieces)
            ]
            if len(tile) < SMALL:
                tile.append(jnp.zeros((SMALL - len(tile), LANES), F32))
            to = place(mirror, own, i) * nslab + m
            out_ref[to, base : base + SMALL, :] = jnp.concatenate(tile, axis=0).astype(BF16)
            for t in range(nang // LANES):
                out_ref[to, t * slab : (t + 1) * slab, :] = final[
                    i, m * slab : (m + 1) * slab, t * LANES : (t + 1) * LANES
                ]


def per_device(
    psi_start,
    potential,
    basis,
    kinetic,
    radial_factor,
    damping,
    coupling,
    helicity,
    chan_rad,
    chan_vib,
    projector,
):
    _, slab, nvib, nang = psi_start.shape
    nquad = basis.shape[1]
    nchan = projector.shape[0]
    groups = lax.axis_size("g")
    own = lax.axis_size("hl")
    nslab = lax.axis_size("rad")
    blocks = groups * own
    group = lax.axis_index("g")
    nrad = nslab * slab
    share = nquad // own
    chunks = (nang + share) // WIDE
    height = (nang + share) // LANES * slab + SMALL
    shape = jax.ShapeDtypeStruct

    send = pl.pallas_call(
        functools.partial(pack, (slab, nvib, nang, share, blocks)),
        out_shape=pltpu.HBM((nvib, height, LANES), BF16),
        in_specs=[HBM] * 3 + [VMEM] + [HBM] * 2,
        out_specs=HBM,
        scratch_shapes=[
            pltpu.VMEM((chunks, slab * nvib, WIDE), F32),
            pltpu.VMEM((nvib, height, LANES), BF16),
            pltpu.VMEM((1, nang), BF16),
            pltpu.VMEM((1, slab), F32),
            pltpu.VMEM((1, slab), F32),
            pltpu.SemaphoreType.DMA((chunks,)),
            pltpu.SemaphoreType.DMA((chunks,)),
            pltpu.SemaphoreType.DMA((3,)),
        ],
        compiler_params=PARAMS,
        name="pack",
    )(
        in_hbm(psi_start.reshape(slab * nvib, nang)),
        in_hbm(potential.reshape(slab * nvib, nquad)),
        in_hbm(coupling),
        helicity[None],
        in_hbm(radial_factor[None]),
        in_hbm(damping[None]),
    )
    message = lax.all_to_all(send, ("hl", "rad"), 0, 0, tiled=True)

    mirror = groups == 2 and own >= ITERS
    sides = 1 if mirror else 2
    rows = message[:, share // LANES * slab :]
    halos = []
    swapped = [(0, 1), (1, 0)]
    for j in range(ITERS - 1 if mirror else ITERS):
        if mirror:
            first = jnp.where(group == 0, own - 1 - j, j) * nslab
            part = lax.dynamic_slice_in_dim(rows, first, nslab, 0)
            halos.append([lax.ppermute(part, "g", swapped)])
            continue
        away, at = j // own + 1, j % own
        upper = rows[at * nslab : (at + 1) * nslab]
        lower = rows[(own - 1 - at) * nslab : (own - at) * nslab]
        up = [(i, i + away) for i in range(groups - away)]
        halos.append(
            [
                lax.ppermute(lower, "g", up),
                lax.ppermute(upper, "g", [(i, j) for j, i in up]),
            ]
        )

    full_type = shape((own, nrad, nang), F32)
    block_type = shape((own, nrad, nang), BF16)
    side_type = shape((sides, nrad, nang), F32)
    halo_type = shape((sides, nrad, nang), BF16)
    coup_type = shape((sides, 1, nang), F32)
    hat_type = shape((sides, 1, LANES), F32)
    dims = (own, nslab, slab, nang, nquad, mirror)

    def run(n, operands, specs, outs, scratch):
        count = (1 if mirror and n == 2 else own) + sides * (n - 1)
        return pl.pallas_call(
            functools.partial(advance, dims, sides, n),
            out_shape=outs,
            in_specs=specs,
            out_specs=[VMEM] * len(outs),
            scratch_shapes=scratch[:-1]
            + [
                pltpu.VMEM((count, nrad, nang), BF16),
                pltpu.VMEM((count * nrad, nquad), BF16),
            ]
            + scratch[-1:],
            compiler_params=PARAMS,
            cost_estimate=pl.CostEstimate(
                flops=4 * count * nrad * nang * nquad,
                bytes_accessed=8 * 1024 * 1024,
                transcendentals=0,
            ),
            name=f"advance{n}",
        )(*operands)

    new, first_b, pot, radii, khat, coup, chain = run(
        1,
        [message, basis, kinetic],
        [VMEM] * 3,
        [
            full_type,
            block_type,
            shape((nrad, nquad), F32),
            shape((2, nrad, LANES), F32),
            shape((own, 1, LANES), F32),
            shape((own, 1, nang), F32),
            shape((max(own - 1, 1), 1, nang), F32),
        ],
        [],
    )
    common = [basis, kinetic, pot, radii, khat, coup, chain]
    joint = pltpu.VMEM((sides, 2, 1, nang), F32)
    operands = halos[0] + common + [new, first_b]
    if mirror:
        ready, part = pl.pallas_call(
            functools.partial(inner, dims),
            out_shape=[
                shape((own - 1, nrad, nang), F32),
                shape((nslab, height - share // LANES * slab, LANES), BF16),
            ],
            in_specs=[VMEM] * 10,
            out_specs=[VMEM] * 2,
            scratch_shapes=[
                pltpu.VMEM((own - 1, nrad, nang), BF16),
                pltpu.VMEM(((own - 1) * nrad, nquad), BF16),
            ],
            compiler_params=PARAMS,
            cost_estimate=pl.CostEstimate(
                flops=4 * own * nrad * nang * nquad,
                bytes_accessed=8 * 1024 * 1024,
                transcendentals=0,
            ),
            name="inner",
        )(*common, new, first_b, message)
        operands.append(ready)
        halos.append([lax.ppermute(part, "g", swapped)])
    first_f, level1_b, new, halo_part, halo1_b, halo1_c, halo1_k = run(
        2,
        operands,
        [VMEM] * len(operands),
        [full_type, block_type, full_type, side_type, halo_type, coup_type, hat_type],
        [joint],
    )
    operands = (
        halos[1]
        + common
        + [new, first_b, first_f, halo_part, halo1_b, halo1_c, halo1_k, level1_b]
    )
    new, halo_part, far_part, halo2_c = run(
        3,
        operands,
        [VMEM] * len(operands),
        [full_type, side_type, side_type, coup_type],
        [
            pltpu.VMEM((own, nrad, nang), F32),
            pltpu.VMEM((sides, nrad, nang), BF16),
            pltpu.VMEM((sides, 1, LANES), F32),
            joint,
        ],
    )
    operands = halos[2] + [new, halo_part, far_part, halo1_c, halo2_c, coup, radii]
    operands += [chan_rad[None], chan_vib[None], projector]
    back = pl.pallas_call(
        functools.partial(close, dims, sides, nchan),
        out_shape=shape((own * nslab, nang // LANES * slab + SMALL, LANES), BF16),
        in_specs=[VMEM] * len(operands),
        out_specs=VMEM,
        scratch_shapes=[pltpu.VMEM((own, nrad, nang), BF16)],
        compiler_params=PARAMS,
        name="close",
    )(*operands)

    home = lax.all_to_all(back, ("hl", "rad"), 0, 0, tiled=True)
    chan = nchan // nslab
    psi_final, amplitude = pl.pallas_call(
        functools.partial(unpack, (slab, nvib, nang, -(-chan // LANES))),
        out_shape=[shape((slab * nvib, nang), F32), shape((1, chan), F32)],
        in_specs=[VMEM],
        out_specs=[HBM, VMEM],
        scratch_shapes=[
            pltpu.VMEM((slab * nvib, nang), F32),
            pltpu.SemaphoreType.DMA((nang // STEP,)),
        ],
        compiler_params=PARAMS,
        name="unpack",
    )(home)
    return (psi_final.reshape(1, slab, nvib, nang), amplitude)


def solution(mesh):
    nhel, nrad = mesh.shape["hel"], mesh.shape["rad"]

    def run(*args):
        nvib = args[0].shape[2]
        groups = nhel * nrad // nvib
        fine = Mesh(mesh.devices.reshape(groups, nhel // groups, nrad), ("g", "hl", "rad"))
        hel = ("g", "hl")
        placed = (
            P(hel, "rad", None, None),
            P("rad", None, None),
            P(),
            P(),
            P("rad"),
            P("rad"),
            P(hel, None),
            P(hel),
            P(),
            P(),
            P(),
        )
        return jax.shard_map(
            per_device,
            mesh=fine,
            in_specs=placed,
            out_specs=(P(hel, "rad", None, None), P(hel, "rad")),
            check_vma=False,
        )(*args)

    return run
```

```python
import functools

import jax
import jax.numpy as jnp
from jax import lax
from jax.experimental import pallas as pl
from jax.experimental.pallas import tpu as pltpu
from jax.sharding import Mesh
from jax.sharding import PartitionSpec as P

ITERS = 3
LANES = 128
STEP = 256
WIDE = 384
QSTEP = 512
JSTEP = 384
SMALL = 8
NT = (((1,), (1,)), ((), ()))
F32 = jnp.float32
BF16 = jnp.bfloat16
VMEM = pl.BlockSpec(memory_space=pltpu.VMEM)
HBM = pl.BlockSpec(memory_space=pltpu.HBM)
PARAMS = pltpu.CompilerParams(vmem_limit_bytes=24 * 1024 * 1024)


def in_hbm(array):
    return pltpu.with_memory_space_constraint(array, pltpu.HBM)


def moved_rows(rows, major):
    minor = rows // major
    at = lax.broadcasted_iota(jnp.int32, (1, rows), 1)
    dest = lax.rem(at, minor) * major + at // minor
    return (lax.broadcasted_iota(jnp.int32, (rows, rows), 0) == dest).astype(BF16)


def pack(
    dims, psi_ref, pot_ref, coup_ref, hel_ref, rf_ref, dp_ref, out_ref,
    wide, ready, coup, rf, dp, in_sems, out_sems, sems,
):
    slab, nvib, nang, share, blocks = dims
    near = lax.axis_size("hl")
    here = lax.axis_index("hl")
    is_last = lax.axis_index("g") * near + here == blocks - 1
    tall = WIDE // LANES * slab
    chunks = (nang + share) // WIDE
    height = (nang + share) // LANES * slab

    def load(i):
        if i * WIDE < share:
            first = pl.multiple_of(here * share + i * WIDE, LANES)
            source = pot_ref.at[:, pl.ds(first, WIDE)]
        else:
            source = psi_ref.at[:, pl.ds(i * WIDE - share, WIDE)]
        return pltpu.make_async_copy(source, wide.at[i], in_sems.at[i])

    def save(i):
        size = tall + (SMALL if i == chunks - 1 else 0)
        lines = pl.ds(i * tall, size)
        return pltpu.make_async_copy(
            ready.at[:, lines, :], out_ref.at[:, lines, :], out_sems.at[i]
        )

    small = [
        pltpu.make_async_copy(source, target, sems.at[i])
        for i, (source, target) in enumerate(
            [(coup_ref, coup), (rf_ref, rf), (dp_ref, dp)]
        )
    ]
    for i in range(chunks):
        load(i).start()
    for copy in small:
        copy.start()
    pick = moved_rows(slab * nvib, nvib)

    for copy in small:
        copy.wait()
    ce = jnp.where(is_last, 0.0, coup[...].astype(F32))
    lines = [ce[:, i * LANES : (i + 1) * LANES] for i in range(nang // LANES)]
    parts = []
    for value in (rf[...], dp[...]):
        high = value.astype(BF16).astype(F32)
        parts += [high, value - high]
    spread = (
        lax.rem(lax.broadcasted_iota(jnp.int32, (slab, LANES), 1), slab)
        == lax.broadcasted_iota(jnp.int32, (slab, LANES), 0)
    ).astype(BF16)
    filler = [jnp.zeros((SMALL - len(parts), slab), F32)]
    repeated = jnp.dot(
        jnp.concatenate(parts + filler, axis=0).astype(BF16), spread, preferred_element_type=F32
    )
    owner = lax.broadcasted_iota(jnp.int32, (SMALL, LANES), 1) // slab
    mine = owner == lax.broadcasted_iota(jnp.int32, (SMALL, LANES), 0)
    line = jnp.sum(jnp.where(mine, repeated, 0.0), axis=0, keepdims=True)
    lane = lax.broadcasted_iota(jnp.int32, (1, LANES), 1)
    lines.append(jnp.where(lane == LANES - 1, hel_ref[...].astype(F32), line))
    if len(lines) < SMALL:
        lines.append(jnp.zeros((SMALL - len(lines), LANES), F32))
    tile = jnp.concatenate(lines, axis=0).astype(BF16)
    for v in range(nvib):
        ready[v, height:, :] = tile

    for i in range(chunks):
        load(i).wait()
        moved = jnp.dot(pick, wide[i].astype(BF16), preferred_element_type=F32)
        moved = moved.astype(BF16).reshape(nvib, slab, WIDE)
        for t in range(WIDE // LANES):
            row = i * tall + t * slab
            ready[:, row : row + slab, :] = moved[:, :, t * LANES : (t + 1) * LANES]
        save(i).start()
    for i in range(chunks):
        save(i).wait()


def unpack(dims, msg_ref, out_ref, amp_ref, wide, sems):
    slab, nvib, nang, pieces = dims
    rows = slab * nvib
    tall = STEP // LANES * slab
    steps = nang // STEP

    def save(step):
        cols = pl.ds(step * STEP, STEP)
        return pltpu.make_async_copy(wide.at[:, cols], out_ref.at[:, cols], sems.at[step])

    pick = moved_rows(rows, slab)
    for step in range(steps):
        parts = [
            msg_ref[:, row : row + slab, :].reshape(rows, LANES)
            for row in range(step * tall, (step + 1) * tall, slab)
        ]
        wide[:, step * STEP : (step + 1) * STEP] = jnp.dot(
            pick, jnp.concatenate(parts, axis=1), preferred_element_type=F32
        )
        save(step).start()
    base = nang // LANES * slab
    lines = jnp.sum(msg_ref[:, base : base + SMALL, :].astype(F32), axis=0)
    lines = [lines[i : i + 1] + lines[pieces + i : pieces + i + 1] for i in range(pieces)]
    amp_ref[...] = jnp.concatenate(lines, axis=1)[:, : amp_ref.shape[1]]
    for step in range(steps):
        save(step).wait()


def rows_in(ref, first, count, slab, nang, base):
    return jnp.concatenate(
        [
            jnp.concatenate(
                [ref[m, base + i * slab : base + (i + 1) * slab, :] for i in range(nang // LANES)],
                axis=1,
            )
            for m in [first + i for i in range(count)]
        ],
        axis=0,
    )


def small_in(ref, m, base, nang):
    page = ref[m, base : base + SMALL, :].astype(F32)
    lines = [page[i : i + 1, :] for i in range(nang // LANES)]
    value = page[len(lines) : len(lines) + 1, LANES - 1 :]
    return jnp.concatenate(lines, axis=1), jnp.broadcast_to(-2.0 * value * value, (1, LANES))


def link(mirror, side, near, far):
    if mirror:
        return jnp.where(lax.axis_index("g") == 0, near, far)
    return far if side == 0 else near


def place(mirror, own, i):
    if mirror:
        return jnp.where(lax.axis_index("g") == 0, own - 1 - i, i)
    return i


def unfold(dims, msg_ref, src, pot, radii, khat, coup):
    own, nslab, slab, nang, nquad, mirror = dims
    share = nquad // own
    top = share // LANES * slab
    base = top + nang // LANES * slab
    lane = lax.broadcasted_iota(jnp.int32, (slab, LANES), 1)
    row = lax.broadcasted_iota(jnp.int32, (slab, LANES), 0)
    for k in range(own):
        for m in range(nslab):
            for t in range(share // LANES):
                cols = pl.ds(k * share + t * LANES, LANES)
                tile = msg_ref[k * nslab + m, t * slab : (t + 1) * slab, :]
                pot[m * slab : (m + 1) * slab, cols] = tile.astype(F32)
    for i in range(own):
        first = place(mirror, own, i) * nslab
        src[i] = rows_in(msg_ref, first, nslab, slab, nang, top)
        coup[i], khat[i] = small_in(msg_ref, first, base, nang)
    for m in range(nslab):
        page = msg_ref[m, base : base + SMALL, :].astype(F32)
        line = page[nang // LANES : nang // LANES + 1, :]
        for i in range(2):
            hit = (lane == row + 2 * i * slab) | (lane == row + (2 * i + 1) * slab)
            value = jnp.sum(jnp.where(hit, line, 0.0), axis=1, keepdims=True)
            radii[i, m * slab : (m + 1) * slab, :] = jnp.broadcast_to(value, (slab, LANES))


def wider(tile, size):
    return jnp.concatenate([tile] * (size // LANES), axis=1)


def inner(dims, *refs):
    own, nslab, slab, nang, nquad, mirror = dims
    nrad = nslab * slab
    basis, kin_ref, pot, radii, khat, coup, chain, part, first_b, msg_ref = refs[:10]
    new_ref, send_ref, rows, scaled = refs[10:]
    top = nquad // own // LANES * slab
    first = place(mirror, own, ITERS - 1) * nslab
    for m in range(nslab):
        send_ref[m] = msg_ref[first + m, top:, :]
    count = own - 1
    for i in range(count):
        rows[i] = part[i + 1].astype(BF16)

    @pl.loop(0, nquad // QSTEP)
    def _(qi):
        cols = pl.ds(pl.multiple_of(qi * QSTEP, QSTEP), QSTEP)
        grid = jnp.dot(
            rows[...].reshape(count * nrad, nang), basis[:, cols], preferred_element_type=F32
        )
        prod = grid.reshape(count, nrad, QSTEP) * pot[:, cols][None]
        scaled[:, cols] = prod.astype(BF16).reshape(count * nrad, QSTEP)

    factor = wider(radii[0], JSTEP)
    damp = wider(radii[1], JSTEP)

    @pl.loop(0, nang // JSTEP)
    def _(ji):
        cols = pl.ds(pl.multiple_of(ji * JSTEP, JSTEP), JSTEP)
        ang = lax.dot_general(
            scaled[...], basis[cols, :], NT, preferred_element_type=F32
        ).reshape(count, nrad, JSTEP)
        for i in range(count):
            total = ang[i] + jnp.dot(
                kin_ref[...], rows[i, :, cols], preferred_element_type=F32
            )
            total += wider(khat[i + 1], JSTEP) * factor * part[i + 1, :, cols]
            if i + 1 < count:
                total += chain[i + 1, :, cols] * rows[i + 1, :, cols].astype(F32)
            if i > 0:
                total += chain[i, :, cols] * rows[i - 1, :, cols].astype(F32)
            before = first_b[i + 1, :, cols].astype(F32)
            new_ref[i, :, cols] = damp * (2.0 * total - damp * before)


def advance(dims, sides, n, *refs):
    own, nslab, slab, nang, nquad, mirror = dims
    nrad = nslab * slab
    refs = list(refs)
    take = lambda count: [refs.pop(0) for _ in range(count)]
    edge_of = [0, own - 1]
    if n == 1:
        msg_ref, basis, kin_ref = take(3)
        new_ref, src, pot, radii, khat, coup, chain = take(7)
        rows, scaled = take(2)
        unfold(dims, msg_ref, src, pot, radii, khat, coup)
        rows[...] = src[...]
        for i in range(own - 1):
            chain[i] = link(mirror, 0, coup[i + 1], coup[i])
    else:
        raw = take(sides)
        basis, kin_ref, pot, radii, khat, coup, chain = take(7)
        scale = wider(radii[1] if n == 2 else 2.0 * radii[1], nang)
        base = nang // LANES * slab
        if n == 2:
            part, first_b = take(2)
            inner_ref = take(1)[0] if mirror else None
            full, block, new_ref, part_h, halo_b, halo_c, halo_k = take(7)
            rows, scaled, joint = take(3)
        else:
            part, first_b, first_f, halo_part, halo1_b, halo1_c, halo1_k, level1_b = take(8)
            new_ref, part_h, part_hh, halo_c = take(4)
            full, halo_b, halo_k, rows, scaled, joint = take(6)
        split = mirror and n == 2
        level = block if split else rows
        shift = 1 if split else own
        for i in range(own):
            value = part[i]
            full[i] = value
            level[i] = value.astype(BF16)
        for s in range(sides):
            halo_b[s] = rows_in(raw[s], 0, nslab, slab, nang, 0)
            halo_c[s], halo_k[s] = small_in(raw[s], 0, base, nang)
            at = edge_of[s]
            if n == 2:
                joint[s, 0] = link(mirror, s, coup[at], halo_c[s])
                seen = halo_b[s]
                rows[shift + s] = seen
            else:
                joint[s, 0] = link(mirror, s, coup[at], halo1_c[s])
                joint[s, 1] = link(mirror, s, halo1_c[s], halo_c[s])
                value = halo_part[s] + wider(radii[1], nang) * (
                    joint[s, 1] * halo_b[s].astype(F32)
                )
                seen = value.astype(BF16)
                rows[own + s] = seen
                rows[own + sides + s] = halo_b[s]
            value = full[at] + scale * (joint[s, 0] * seen.astype(F32))
            full[at] = value
            level[at] = value.astype(BF16)
        if split:
            rows[0] = block[0]
        elif n == 2:
            block[...] = rows[:own]
    if n == 1:
        split, level, shift = False, rows, own
    count = shift + sides * (n - 1)

    @pl.loop(0, nquad // QSTEP)
    def _(qi):
        cols = pl.ds(pl.multiple_of(qi * QSTEP, QSTEP), QSTEP)
        grid = jnp.dot(
            rows[...].reshape(count * nrad, nang), basis[:, cols], preferred_element_type=F32
        )
        prod = grid.reshape(count, nrad, QSTEP) * pot[:, cols][None]
        scaled[:, cols] = prod.astype(BF16).reshape(count * nrad, QSTEP)

    factor = wider(radii[0], JSTEP)
    damp = wider(radii[1], JSTEP)

    @pl.loop(0, nang // JSTEP)
    def _(ji):
        cols = pl.ds(pl.multiple_of(ji * JSTEP, JSTEP), JSTEP)
        ang = lax.dot_general(
            scaled[...], basis[cols, :], NT, preferred_element_type=F32
        ).reshape(count, nrad, JSTEP)

        def local(i, hat, value):
            kin = jnp.dot(kin_ref[...], rows[i, :, cols], preferred_element_type=F32)
            return ang[i] + kin + wider(hat, JSTEP) * factor * value

        for i in range(own):
            if split and i > 0:
                value = inner_ref[i - 1, :, cols]
                if i == 1:
                    value += 2.0 * damp * (chain[0, :, cols] * level[0, :, cols].astype(F32))
                new_ref[i, :, cols] = value
                continue
            value = rows[i, :, cols].astype(F32) if n == 1 else full[i, :, cols]
            total = local(i, khat[i], value)
            if i + 1 < own:
                total += chain[i, :, cols] * level[i + 1, :, cols].astype(F32)
            if i > 0:
                total += chain[i - 1, :, cols] * level[i - 1, :, cols].astype(F32)
            if n == 1:
                new_ref[i, :, cols] = damp * total
            else:
                before = first_b if n == 2 else first_f
                new_ref[i, :, cols] = damp * (
                    2.0 * total - damp * before[i, :, cols].astype(F32)
                )
        for s in range(sides if n > 1 else 0):
            at = edge_of[s]
            i = shift + s
            hat = halo_k[s] if n == 2 else halo1_k[s]
            total = local(i, hat, rows[i, :, cols].astype(F32))
            edge_b = first_b if n == 2 else level1_b
            total += joint[s, 0, :, cols] * edge_b[at, :, cols].astype(F32)
            if n == 2:
                part_h[s, :, cols] = damp * total
                continue
            before = halo1_b[s, :, cols].astype(F32)
            part_h[s, :, cols] = damp * (2.0 * total - damp * before)
            i = own + sides + s
            total = local(i, halo_k[s], rows[i, :, cols].astype(F32))
            total += joint[s, 1, :, cols] * before
            part_hh[s, :, cols] = damp * total


def close(dims, sides, nchan, *refs):
    own, nslab, slab, nang, nquad, mirror = dims
    nrad = nslab * slab
    raw, refs = refs[:sides], refs[sides:]
    part, part_h, part_hh, halo1_c, halo2_c, coup, radii = refs[:7]
    rad_ref, vib_ref, proj_ref, out_ref, final = refs[7:]
    base = nang // LANES * slab
    damp = wider(radii[1], nang)
    for i in range(own):
        final[i] = part[i].astype(BF16)
    for s in range(sides):
        at = 0 if s == 0 else own - 1
        far = rows_in(raw[s], 0, nslab, slab, nang, 0).astype(F32)
        far_c, _ = small_in(raw[s], 0, base, nang)
        value = part_hh[s] + damp * (link(mirror, s, halo2_c[s], far_c) * far)
        value = value.astype(BF16).astype(F32)
        value = part_h[s] + 2.0 * damp * (link(mirror, s, halo1_c[s], halo2_c[s]) * value)
        value = value.astype(BF16).astype(F32)
        term = 2.0 * damp * (link(mirror, s, coup[at], halo1_c[s]) * value)
        fixed = (part[at] if s == 0 or own > 1 else fixed) + term
        final[at] = fixed.astype(BF16)

    chan = nchan // nslab
    pieces = -(-chan // LANES)
    vib = lax.axis_index("hl") * nslab + lax.axis_index("rad")
    rows_at = lax.broadcasted_iota(jnp.int32, (nrad, chan), 0)
    for m in range(nslab):
        cols = slice(m * chan, (m + 1) * chan)
        table = lax.dot_general(
            final[...].reshape(own * nrad, nang),
            proj_ref[cols, :],
            NT,
            preferred_element_type=F32,
        ).reshape(own, nrad, chan)
        hit = (rows_at == rad_ref[:, cols]) & (vib_ref[:, cols] == vib)
        for i in range(own):
            amp = jnp.sum(jnp.where(hit, table[i], 0.0), axis=0, keepdims=True)
            if pieces * LANES > chan:
                amp = jnp.concatenate([amp, jnp.zeros((1, pieces * LANES - chan), F32)], axis=1)
            high = amp.astype(BF16).astype(F32)
            tile = [
                half[:, p * LANES : (p + 1) * LANES]
                for half in (high, amp - high)
                for p in range(pieces)
            ]
            if len(tile) < SMALL:
                tile.append(jnp.zeros((SMALL - len(tile), LANES), F32))
            to = place(mirror, own, i) * nslab + m
            out_ref[to, base : base + SMALL, :] = jnp.concatenate(tile, axis=0).astype(BF16)
            for t in range(nang // LANES):
                out_ref[to, t * slab : (t + 1) * slab, :] = final[
                    i, m * slab : (m + 1) * slab, t * LANES : (t + 1) * LANES
                ]


def per_device(
    psi_start,
    potential,
    basis,
    kinetic,
    radial_factor,
    damping,
    coupling,
    helicity,
    chan_rad,
    chan_vib,
    projector,
):
    _, slab, nvib, nang = psi_start.shape
    nquad = basis.shape[1]
    nchan = projector.shape[0]
    groups = lax.axis_size("g")
    own = lax.axis_size("hl")
    nslab = lax.axis_size("rad")
    blocks = groups * own
    group = lax.axis_index("g")
    nrad = nslab * slab
    share = nquad // own
    chunks = (nang + share) // WIDE
    height = (nang + share) // LANES * slab + SMALL
    shape = jax.ShapeDtypeStruct

    send = pl.pallas_call(
        functools.partial(pack, (slab, nvib, nang, share, blocks)),
        out_shape=pltpu.HBM((nvib, height, LANES), BF16),
        in_specs=[HBM] * 3 + [VMEM] + [HBM] * 2,
        out_specs=HBM,
        scratch_shapes=[
            pltpu.VMEM((chunks, slab * nvib, WIDE), F32),
            pltpu.VMEM((nvib, height, LANES), BF16),
            pltpu.VMEM((1, nang), BF16),
            pltpu.VMEM((1, slab), F32),
            pltpu.VMEM((1, slab), F32),
            pltpu.SemaphoreType.DMA((chunks,)),
            pltpu.SemaphoreType.DMA((chunks,)),
            pltpu.SemaphoreType.DMA((3,)),
        ],
        compiler_params=PARAMS,
        name="pack",
    )(
        in_hbm(psi_start.reshape(slab * nvib, nang)),
        in_hbm(potential.reshape(slab * nvib, nquad)),
        in_hbm(coupling),
        helicity[None],
        in_hbm(radial_factor[None]),
        in_hbm(damping[None]),
    )
    message = lax.all_to_all(send, ("hl", "rad"), 0, 0, tiled=True)

    mirror = groups == 2 and own >= ITERS
    sides = 1 if mirror else 2
    rows = message[:, share // LANES * slab :]
    halos = []
    swapped = [(0, 1), (1, 0)]
    for j in range(ITERS - 1 if mirror else ITERS):
        if mirror:
            first = jnp.where(group == 0, own - 1 - j, j) * nslab
            part = lax.dynamic_slice_in_dim(rows, first, nslab, 0)
            halos.append([lax.ppermute(part, "g", swapped)])
            continue
        away, at = j // own + 1, j % own
        upper = rows[at * nslab : (at + 1) * nslab]
        lower = rows[(own - 1 - at) * nslab : (own - at) * nslab]
        up = [(i, i + away) for i in range(groups - away)]
        halos.append(
            [
                lax.ppermute(lower, "g", up),
                lax.ppermute(upper, "g", [(i, j) for j, i in up]),
            ]
        )

    full_type = shape((own, nrad, nang), F32)
    block_type = shape((own, nrad, nang), BF16)
    side_type = shape((sides, nrad, nang), F32)
    halo_type = shape((sides, nrad, nang), BF16)
    coup_type = shape((sides, 1, nang), F32)
    hat_type = shape((sides, 1, LANES), F32)
    dims = (own, nslab, slab, nang, nquad, mirror)

    def run(n, operands, specs, outs, scratch):
        count = (1 if mirror and n == 2 else own) + sides * (n - 1)
        return pl.pallas_call(
            functools.partial(advance, dims, sides, n),
            out_shape=outs,
            in_specs=specs,
            out_specs=[VMEM] * len(outs),
            scratch_shapes=scratch[:-1]
            + [
                pltpu.VMEM((count, nrad, nang), BF16),
                pltpu.VMEM((count * nrad, nquad), BF16),
            ]
            + scratch[-1:],
            compiler_params=PARAMS,
            cost_estimate=pl.CostEstimate(
                flops=4 * count * nrad * nang * nquad,
                bytes_accessed=8 * 1024 * 1024,
                transcendentals=0,
            ),
            name=f"advance{n}",
        )(*operands)

    new, first_b, pot, radii, khat, coup, chain = run(
        1,
        [message, basis, kinetic],
        [VMEM] * 3,
        [
            full_type,
            block_type,
            shape((nrad, nquad), F32),
            shape((2, nrad, LANES), F32),
            shape((own, 1, LANES), F32),
            shape((own, 1, nang), F32),
            shape((max(own - 1, 1), 1, nang), F32),
        ],
        [],
    )
    common = [basis, kinetic, pot, radii, khat, coup, chain]
    joint = pltpu.VMEM((sides, 2, 1, nang), F32)
    operands = halos[0] + common + [new, first_b]
    if mirror:
        ready, part = pl.pallas_call(
            functools.partial(inner, dims),
            out_shape=[
                shape((own - 1, nrad, nang), F32),
                shape((nslab, height - share // LANES * slab, LANES), BF16),
            ],
            in_specs=[VMEM] * 10,
            out_specs=[VMEM] * 2,
            scratch_shapes=[
                pltpu.VMEM((own - 1, nrad, nang), BF16),
                pltpu.VMEM(((own - 1) * nrad, nquad), BF16),
            ],
            compiler_params=PARAMS,
            cost_estimate=pl.CostEstimate(
                flops=4 * own * nrad * nang * nquad,
                bytes_accessed=8 * 1024 * 1024,
                transcendentals=0,
            ),
            name="inner",
        )(*common, new, first_b, message)
        operands.append(ready)
        halos.append([lax.ppermute(part, "g", swapped)])
    first_f, level1_b, new, halo_part, halo1_b, halo1_c, halo1_k = run(
        2,
        operands,
        [VMEM] * len(operands),
        [full_type, block_type, full_type, side_type, halo_type, coup_type, hat_type],
        [joint],
    )
    operands = (
        halos[1]
        + common
        + [new, first_b, first_f, halo_part, halo1_b, halo1_c, halo1_k, level1_b]
    )
    new, halo_part, far_part, halo2_c = run(
        3,
        operands,
        [VMEM] * len(operands),
        [full_type, side_type, side_type, coup_type],
        [
            pltpu.VMEM((own, nrad, nang), F32),
            pltpu.VMEM((sides, nrad, nang), BF16),
            pltpu.VMEM((sides, 1, LANES), F32),
            joint,
        ],
    )
    operands = halos[2] + [new, halo_part, far_part, halo1_c, halo2_c, coup, radii]
    operands += [chan_rad[None], chan_vib[None], projector]
    back = pl.pallas_call(
        functools.partial(close, dims, sides, nchan),
        out_shape=shape((own * nslab, nang // LANES * slab + SMALL, LANES), BF16),
        in_specs=[VMEM] * len(operands),
        out_specs=VMEM,
        scratch_shapes=[pltpu.VMEM((own, nrad, nang), BF16)],
        compiler_params=PARAMS,
        name="close",
    )(*operands)

    home = lax.all_to_all(back, ("hl", "rad"), 0, 0, tiled=True)
    chan = nchan // nslab
    psi_final, amplitude = pl.pallas_call(
        functools.partial(unpack, (slab, nvib, nang, -(-chan // LANES))),
        out_shape=[shape((slab * nvib, nang), F32), shape((1, chan), F32)],
        in_specs=[VMEM],
        out_specs=[HBM, VMEM],
        scratch_shapes=[
            pltpu.VMEM((slab * nvib, nang), F32),
            pltpu.SemaphoreType.DMA((nang // STEP,)),
        ],
        compiler_params=PARAMS,
        name="unpack",
    )(home)
    return (psi_final.reshape(1, slab, nvib, nang), amplitude)


def solution(mesh):
    nhel, nrad = mesh.shape["hel"], mesh.shape["rad"]

    def run(*args):
        nvib = args[0].shape[2]
        groups = nhel * nrad // nvib
        fine = Mesh(mesh.devices.reshape(groups, nhel // groups, nrad), ("g", "hl", "rad"))
        hel = ("g", "hl")
        placed = (
            P(hel, "rad", None, None),
            P("rad", None, None),
            P(),
            P(),
            P("rad"),
            P("rad"),
            P(hel, None),
            P(hel),
            P(),
            P(),
            P(),
        )
        return jax.shard_map(
            per_device,
            mesh=fine,
            in_specs=placed,
            out_specs=(P(hel, "rad", None, None), P(hel, "rad")),
            check_vma=False,
        )(*args)

    return run
```

```python
import functools

import jax
import jax.numpy as jnp
from jax import lax
from jax.experimental import pallas as pl
from jax.experimental.pallas import tpu as pltpu
from jax.sharding import Mesh
from jax.sharding import PartitionSpec as P

ITERS = 3
LANES = 128
STEP = 256
WIDE = 384
QSTEP = 512
JSTEP = 384
SMALL = 8
NT = (((1,), (1,)), ((), ()))
F32 = jnp.float32
BF16 = jnp.bfloat16
VMEM = pl.BlockSpec(memory_space=pltpu.VMEM)
HBM = pl.BlockSpec(memory_space=pltpu.HBM)
PARAMS = pltpu.CompilerParams(vmem_limit_bytes=24 * 1024 * 1024)


def in_hbm(array):
    return pltpu.with_memory_space_constraint(array, pltpu.HBM)


def moved_rows(rows, major):
    minor = rows // major
    at = lax.broadcasted_iota(jnp.int32, (1, rows), 1)
    dest = lax.rem(at, minor) * major + at // minor
    return (lax.broadcasted_iota(jnp.int32, (rows, rows), 0) == dest).astype(BF16)


def pack(
    dims, psi_ref, pot_ref, coup_ref, hel_ref, rf_ref, dp_ref, out_ref,
    wide, ready, coup, rf, dp, in_sems, out_sems, sems,
):
    slab, nvib, nang, share, blocks = dims
    near = lax.axis_size("hl")
    here = lax.axis_index("hl")
    is_last = lax.axis_index("g") * near + here == blocks - 1
    tall = WIDE // LANES * slab
    chunks = (nang + share) // WIDE
    height = (nang + share) // LANES * slab

    def load(i):
        if i * WIDE < share:
            first = pl.multiple_of(here * share + i * WIDE, LANES)
            source = pot_ref.at[:, pl.ds(first, WIDE)]
        else:
            source = psi_ref.at[:, pl.ds(i * WIDE - share, WIDE)]
        return pltpu.make_async_copy(source, wide.at[i], in_sems.at[i])

    def save(i):
        size = tall + (SMALL if i == chunks - 1 else 0)
        lines = pl.ds(i * tall, size)
        return pltpu.make_async_copy(
            ready.at[:, lines, :], out_ref.at[:, lines, :], out_sems.at[i]
        )

    small = [
        pltpu.make_async_copy(source, target, sems.at[i])
        for i, (source, target) in enumerate(
            [(coup_ref, coup), (rf_ref, rf), (dp_ref, dp)]
        )
    ]
    for i in range(chunks):
        load(i).start()
    for copy in small:
        copy.start()
    pick = moved_rows(slab * nvib, nvib)

    for copy in small:
        copy.wait()
    ce = jnp.where(is_last, 0.0, coup[...].astype(F32))
    lines = [ce[:, i * LANES : (i + 1) * LANES] for i in range(nang // LANES)]
    parts = []
    for value in (rf[...], dp[...]):
        high = value.astype(BF16).astype(F32)
        parts += [high, value - high]
    spread = (
        lax.rem(lax.broadcasted_iota(jnp.int32, (slab, LANES), 1), slab)
        == lax.broadcasted_iota(jnp.int32, (slab, LANES), 0)
    ).astype(BF16)
    filler = [jnp.zeros((SMALL - len(parts), slab), F32)]
    repeated = jnp.dot(
        jnp.concatenate(parts + filler, axis=0).astype(BF16), spread, preferred_element_type=F32
    )
    owner = lax.broadcasted_iota(jnp.int32, (SMALL, LANES), 1) // slab
    mine = owner == lax.broadcasted_iota(jnp.int32, (SMALL, LANES), 0)
    line = jnp.sum(jnp.where(mine, repeated, 0.0), axis=0, keepdims=True)
    lane = lax.broadcasted_iota(jnp.int32, (1, LANES), 1)
    lines.append(jnp.where(lane == LANES - 1, hel_ref[...].astype(F32), line))
    if len(lines) < SMALL:
        lines.append(jnp.zeros((SMALL - len(lines), LANES), F32))
    tile = jnp.concatenate(lines, axis=0).astype(BF16)
    for v in range(nvib):
        ready[v, height:, :] = tile

    for i in range(chunks):
        load(i).wait()
        moved = jnp.dot(pick, wide[i].astype(BF16), preferred_element_type=F32)
        moved = moved.astype(BF16).reshape(nvib, slab, WIDE)
        for t in range(WIDE // LANES):
            row = i * tall + t * slab
            ready[:, row : row + slab, :] = moved[:, :, t * LANES : (t + 1) * LANES]
        save(i).start()
    for i in range(chunks):
        save(i).wait()


def unpack(dims, msg_ref, out_ref, amp_ref, wide, sems):
    slab, nvib, nang, pieces = dims
    rows = slab * nvib
    tall = STEP // LANES * slab
    steps = nang // STEP

    def save(step):
        cols = pl.ds(step * STEP, STEP)
        return pltpu.make_async_copy(wide.at[:, cols], out_ref.at[:, cols], sems.at[step])

    pick = moved_rows(rows, slab)
    for step in range(steps):
        parts = [
            msg_ref[:, row : row + slab, :].reshape(rows, LANES)
            for row in range(step * tall, (step + 1) * tall, slab)
        ]
        wide[:, step * STEP : (step + 1) * STEP] = jnp.dot(
            pick, jnp.concatenate(parts, axis=1), preferred_element_type=F32
        )
        save(step).start()
    base = nang // LANES * slab
    lines = jnp.sum(msg_ref[:, base : base + SMALL, :].astype(F32), axis=0)
    lines = [lines[i : i + 1] + lines[pieces + i : pieces + i + 1] for i in range(pieces)]
    amp_ref[...] = jnp.concatenate(lines, axis=1)[:, : amp_ref.shape[1]]
    for step in range(steps):
        save(step).wait()


def rows_in(ref, first, count, slab, nang, base):
    return jnp.concatenate(
        [
            jnp.concatenate(
                [ref[m, base + i * slab : base + (i + 1) * slab, :] for i in range(nang // LANES)],
                axis=1,
            )
            for m in [first + i for i in range(count)]
        ],
        axis=0,
    )


def small_in(ref, m, base, nang):
    page = ref[m, base : base + SMALL, :].astype(F32)
    lines = [page[i : i + 1, :] for i in range(nang // LANES)]
    value = page[len(lines) : len(lines) + 1, LANES - 1 :]
    return jnp.concatenate(lines, axis=1), jnp.broadcast_to(-2.0 * value * value, (1, LANES))


def link(mirror, side, near, far):
    if mirror:
        return jnp.where(lax.axis_index("g") == 0, near, far)
    return far if side == 0 else near


def place(mirror, own, i):
    if mirror:
        return jnp.where(lax.axis_index("g") == 0, own - 1 - i, i)
    return i


def unfold(dims, msg_ref, src, pot, radii, khat, coup):
    own, nslab, slab, nang, nquad, mirror = dims
    share = nquad // own
    top = share // LANES * slab
    base = top + nang // LANES * slab
    lane = lax.broadcasted_iota(jnp.int32, (slab, LANES), 1)
    row = lax.broadcasted_iota(jnp.int32, (slab, LANES), 0)
    for k in range(own):
        for m in range(nslab):
            for t in range(share // LANES):
                cols = pl.ds(k * share + t * LANES, LANES)
                tile = msg_ref[k * nslab + m, t * slab : (t + 1) * slab, :]
                pot[m * slab : (m + 1) * slab, cols] = tile.astype(F32)
    for i in range(own):
        first = place(mirror, own, i) * nslab
        src[i] = rows_in(msg_ref, first, nslab, slab, nang, top)
        coup[i], khat[i] = small_in(msg_ref, first, base, nang)
    for m in range(nslab):
        page = msg_ref[m, base : base + SMALL, :].astype(F32)
        line = page[nang // LANES : nang // LANES + 1, :]
        for i in range(2):
            hit = (lane == row + 2 * i * slab) | (lane == row + (2 * i + 1) * slab)
            value = jnp.sum(jnp.where(hit, line, 0.0), axis=1, keepdims=True)
            radii[i, m * slab : (m + 1) * slab, :] = jnp.broadcast_to(value, (slab, LANES))


def wider(tile, size):
    return jnp.concatenate([tile] * (size // LANES), axis=1)


def inner(dims, *refs):
    own, nslab, slab, nang, nquad, mirror = dims
    nrad = nslab * slab
    basis, kin_ref, pot, radii, khat, coup, chain, part, first_b, msg_ref = refs[:10]
    new_ref, send_ref, rows, scaled = refs[10:]
    top = nquad // own // LANES * slab
    first = place(mirror, own, ITERS - 1) * nslab
    for m in range(nslab):
        send_ref[m] = msg_ref[first + m, top:, :]
    count = own - 1
    for i in range(count):
        rows[i] = part[i + 1].astype(BF16)

    @pl.loop(0, nquad // QSTEP)
    def _(qi):
        cols = pl.ds(pl.multiple_of(qi * QSTEP, QSTEP), QSTEP)
        grid = jnp.dot(
            rows[...].reshape(count * nrad, nang), basis[:, cols], preferred_element_type=F32
        )
        prod = grid.reshape(count, nrad, QSTEP) * pot[:, cols][None]
        scaled[:, cols] = prod.astype(BF16).reshape(count * nrad, QSTEP)

    factor = wider(radii[0], JSTEP)
    damp = wider(radii[1], JSTEP)

    @pl.loop(0, nang // JSTEP)
    def _(ji):
        cols = pl.ds(pl.multiple_of(ji * JSTEP, JSTEP), JSTEP)
        ang = lax.dot_general(
            scaled[...], basis[cols, :], NT, preferred_element_type=F32
        ).reshape(count, nrad, JSTEP)
        for i in range(count):
            total = ang[i] + jnp.dot(
                kin_ref[...], rows[i, :, cols], preferred_element_type=F32
            )
            total += wider(khat[i + 1], JSTEP) * factor * part[i + 1, :, cols]
            if i + 1 < count:
                total += chain[i + 1, :, cols] * rows[i + 1, :, cols].astype(F32)
            if i > 0:
                total += chain[i, :, cols] * rows[i - 1, :, cols].astype(F32)
            before = first_b[i + 1, :, cols].astype(F32)
            new_ref[i, :, cols] = damp * (2.0 * total - damp * before)


def advance(dims, sides, n, *refs):
    own, nslab, slab, nang, nquad, mirror = dims
    nrad = nslab * slab
    refs = list(refs)
    take = lambda count: [refs.pop(0) for _ in range(count)]
    edge_of = [0, own - 1]
    if n == 1:
        msg_ref, basis, kin_ref = take(3)
        new_ref, src, pot, radii, khat, coup, chain = take(7)
        if mirror:
            send_ref = take(1)[0]
            first = place(mirror, own, 1) * nslab
            for m in range(nslab):
                send_ref[m] = msg_ref[first + m, nquad // own // LANES * slab :, :]
        rows, scaled = take(2)
        unfold(dims, msg_ref, src, pot, radii, khat, coup)
        rows[...] = src[...]
        for i in range(own - 1):
            chain[i] = link(mirror, 0, coup[i + 1], coup[i])
    else:
        raw = take(sides)
        basis, kin_ref, pot, radii, khat, coup, chain = take(7)
        scale = wider(radii[1] if n == 2 else 2.0 * radii[1], nang)
        base = nang // LANES * slab
        if n == 2:
            part, first_b = take(2)
            inner_ref = take(1)[0] if mirror else None
            full, block, new_ref, part_h, halo_b, halo_c, halo_k = take(7)
            rows, scaled, joint = take(3)
        else:
            part, first_b, first_f, halo_part, halo1_b, halo1_c, halo1_k, level1_b = take(8)
            new_ref, part_h, part_hh, halo_c = take(4)
            full, halo_b, halo_k, rows, scaled, joint = take(6)
        split = mirror and n == 2
        level = block if split else rows
        shift = 1 if split else own
        for i in range(own):
            value = part[i]
            full[i] = value
            level[i] = value.astype(BF16)
        for s in range(sides):
            halo_b[s] = rows_in(raw[s], 0, nslab, slab, nang, 0)
            halo_c[s], halo_k[s] = small_in(raw[s], 0, base, nang)
            at = edge_of[s]
            if n == 2:
                joint[s, 0] = link(mirror, s, coup[at], halo_c[s])
                seen = halo_b[s]
                rows[shift + s] = seen
            else:
                joint[s, 0] = link(mirror, s, coup[at], halo1_c[s])
                joint[s, 1] = link(mirror, s, halo1_c[s], halo_c[s])
                value = halo_part[s] + wider(radii[1], nang) * (
                    joint[s, 1] * halo_b[s].astype(F32)
                )
                seen = value.astype(BF16)
                rows[own + s] = seen
                rows[own + sides + s] = halo_b[s]
            value = full[at] + scale * (joint[s, 0] * seen.astype(F32))
            full[at] = value
            level[at] = value.astype(BF16)
        if split:
            rows[0] = block[0]
        elif n == 2:
            block[...] = rows[:own]
    if n == 1:
        split, level, shift = False, rows, own
    count = shift + sides * (n - 1)

    @pl.loop(0, nquad // QSTEP)
    def _(qi):
        cols = pl.ds(pl.multiple_of(qi * QSTEP, QSTEP), QSTEP)
        grid = jnp.dot(
            rows[...].reshape(count * nrad, nang), basis[:, cols], preferred_element_type=F32
        )
        prod = grid.reshape(count, nrad, QSTEP) * pot[:, cols][None]
        scaled[:, cols] = prod.astype(BF16).reshape(count * nrad, QSTEP)

    factor = wider(radii[0], JSTEP)
    damp = wider(radii[1], JSTEP)

    @pl.loop(0, nang // JSTEP)
    def _(ji):
        cols = pl.ds(pl.multiple_of(ji * JSTEP, JSTEP), JSTEP)
        ang = lax.dot_general(
            scaled[...], basis[cols, :], NT, preferred_element_type=F32
        ).reshape(count, nrad, JSTEP)

        def local(i, hat, value):
            kin = jnp.dot(kin_ref[...], rows[i, :, cols], preferred_element_type=F32)
            return ang[i] + kin + wider(hat, JSTEP) * factor * value

        for i in range(own):
            if split and i > 0:
                value = inner_ref[i - 1, :, cols]
                if i == 1:
                    value += 2.0 * damp * (chain[0, :, cols] * level[0, :, cols].astype(F32))
                new_ref[i, :, cols] = value
                continue
            value = rows[i, :, cols].astype(F32) if n == 1 else full[i, :, cols]
            total = local(i, khat[i], value)
            if i + 1 < own:
                total += chain[i, :, cols] * level[i + 1, :, cols].astype(F32)
            if i > 0:
                total += chain[i - 1, :, cols] * level[i - 1, :, cols].astype(F32)
            if n == 1:
                new_ref[i, :, cols] = damp * total
            else:
                before = first_b if n == 2 else first_f
                new_ref[i, :, cols] = damp * (
                    2.0 * total - damp * before[i, :, cols].astype(F32)
                )
        for s in range(sides if n > 1 else 0):
            at = edge_of[s]
            i = shift + s
            hat = halo_k[s] if n == 2 else halo1_k[s]
            total = local(i, hat, rows[i, :, cols].astype(F32))
            edge_b = first_b if n == 2 else level1_b
            total += joint[s, 0, :, cols] * edge_b[at, :, cols].astype(F32)
            if n == 2:
                part_h[s, :, cols] = damp * total
                continue
            before = halo1_b[s, :, cols].astype(F32)
            part_h[s, :, cols] = damp * (2.0 * total - damp * before)
            i = own + sides + s
            total = local(i, halo_k[s], rows[i, :, cols].astype(F32))
            total += joint[s, 1, :, cols] * before
            part_hh[s, :, cols] = damp * total


def close(dims, sides, nchan, *refs):
    own, nslab, slab, nang, nquad, mirror = dims
    nrad = nslab * slab
    raw, refs = refs[:sides], refs[sides:]
    part, part_h, part_hh, halo1_c, halo2_c, coup, radii = refs[:7]
    rad_ref, vib_ref, proj_ref, out_ref, final = refs[7:]
    base = nang // LANES * slab
    damp = wider(radii[1], nang)
    for i in range(own):
        final[i] = part[i].astype(BF16)
    for s in range(sides):
        at = 0 if s == 0 else own - 1
        far = rows_in(raw[s], 0, nslab, slab, nang, 0).astype(F32)
        far_c, _ = small_in(raw[s], 0, base, nang)
        value = part_hh[s] + damp * (link(mirror, s, halo2_c[s], far_c) * far)
        value = value.astype(BF16).astype(F32)
        value = part_h[s] + 2.0 * damp * (link(mirror, s, halo1_c[s], halo2_c[s]) * value)
        value = value.astype(BF16).astype(F32)
        term = 2.0 * damp * (link(mirror, s, coup[at], halo1_c[s]) * value)
        fixed = (part[at] if s == 0 or own > 1 else fixed) + term
        final[at] = fixed.astype(BF16)

    chan = nchan // nslab
    pieces = -(-chan // LANES)
    vib = lax.axis_index("hl") * nslab + lax.axis_index("rad")
    rows_at = lax.broadcasted_iota(jnp.int32, (nrad, chan), 0)
    for m in range(nslab):
        cols = slice(m * chan, (m + 1) * chan)
        table = lax.dot_general(
            final[...].reshape(own * nrad, nang),
            proj_ref[cols, :],
            NT,
            preferred_element_type=F32,
        ).reshape(own, nrad, chan)
        hit = (rows_at == rad_ref[:, cols]) & (vib_ref[:, cols] == vib)
        for i in range(own):
            amp = jnp.sum(jnp.where(hit, table[i], 0.0), axis=0, keepdims=True)
            if pieces * LANES > chan:
                amp = jnp.concatenate([amp, jnp.zeros((1, pieces * LANES - chan), F32)], axis=1)
            high = amp.astype(BF16).astype(F32)
            tile = [
                half[:, p * LANES : (p + 1) * LANES]
                for half in (high, amp - high)
                for p in range(pieces)
            ]
            if len(tile) < SMALL:
                tile.append(jnp.zeros((SMALL - len(tile), LANES), F32))
            to = place(mirror, own, i) * nslab + m
            out_ref[to, base : base + SMALL, :] = jnp.concatenate(tile, axis=0).astype(BF16)
            for t in range(nang // LANES):
                out_ref[to, t * slab : (t + 1) * slab, :] = final[
                    i, m * slab : (m + 1) * slab, t * LANES : (t + 1) * LANES
                ]


def per_device(
    psi_start,
    potential,
    basis,
    kinetic,
    radial_factor,
    damping,
    coupling,
    helicity,
    chan_rad,
    chan_vib,
    projector,
):
    _, slab, nvib, nang = psi_start.shape
    nquad = basis.shape[1]
    nchan = projector.shape[0]
    groups = lax.axis_size("g")
    own = lax.axis_size("hl")
    nslab = lax.axis_size("rad")
    blocks = groups * own
    group = lax.axis_index("g")
    nrad = nslab * slab
    share = nquad // own
    chunks = (nang + share) // WIDE
    height = (nang + share) // LANES * slab + SMALL
    shape = jax.ShapeDtypeStruct

    send = pl.pallas_call(
        functools.partial(pack, (slab, nvib, nang, share, blocks)),
        out_shape=pltpu.HBM((nvib, height, LANES), BF16),
        in_specs=[HBM] * 3 + [VMEM] + [HBM] * 2,
        out_specs=HBM,
        scratch_shapes=[
            pltpu.VMEM((chunks, slab * nvib, WIDE), F32),
            pltpu.VMEM((nvib, height, LANES), BF16),
            pltpu.VMEM((1, nang), BF16),
            pltpu.VMEM((1, slab), F32),
            pltpu.VMEM((1, slab), F32),
            pltpu.SemaphoreType.DMA((chunks,)),
            pltpu.SemaphoreType.DMA((chunks,)),
            pltpu.SemaphoreType.DMA((3,)),
        ],
        compiler_params=PARAMS,
        name="pack",
    )(
        in_hbm(psi_start.reshape(slab * nvib, nang)),
        in_hbm(potential.reshape(slab * nvib, nquad)),
        in_hbm(coupling),
        helicity[None],
        in_hbm(radial_factor[None]),
        in_hbm(damping[None]),
    )
    message = lax.all_to_all(send, ("hl", "rad"), 0, 0, tiled=True)

    mirror = groups == 2 and own >= ITERS
    sides = 1 if mirror else 2
    rows = message[:, share // LANES * slab :]
    halos = []
    swapped = [(0, 1), (1, 0)]
    for j in range(1 if mirror else ITERS):
        if mirror:
            first = jnp.where(group == 0, own - 1 - j, j) * nslab
            part = lax.dynamic_slice_in_dim(rows, first, nslab, 0)
            halos.append([lax.ppermute(part, "g", swapped)])
            continue
        away, at = j // own + 1, j % own
        upper = rows[at * nslab : (at + 1) * nslab]
        lower = rows[(own - 1 - at) * nslab : (own - at) * nslab]
        up = [(i, i + away) for i in range(groups - away)]
        halos.append(
            [
                lax.ppermute(lower, "g", up),
                lax.ppermute(upper, "g", [(i, j) for j, i in up]),
            ]
        )

    full_type = shape((own, nrad, nang), F32)
    block_type = shape((own, nrad, nang), BF16)
    side_type = shape((sides, nrad, nang), F32)
    halo_type = shape((sides, nrad, nang), BF16)
    coup_type = shape((sides, 1, nang), F32)
    hat_type = shape((sides, 1, LANES), F32)
    dims = (own, nslab, slab, nang, nquad, mirror)

    def run(n, operands, specs, outs, scratch):
        count = (1 if mirror and n == 2 else own) + sides * (n - 1)
        return pl.pallas_call(
            functools.partial(advance, dims, sides, n),
            out_shape=outs,
            in_specs=specs,
            out_specs=[VMEM] * len(outs),
            scratch_shapes=scratch[:-1]
            + [
                pltpu.VMEM((count, nrad, nang), BF16),
                pltpu.VMEM((count * nrad, nquad), BF16),
            ]
            + scratch[-1:],
            compiler_params=PARAMS,
            cost_estimate=pl.CostEstimate(
                flops=4 * count * nrad * nang * nquad,
                bytes_accessed=8 * 1024 * 1024,
                transcendentals=0,
            ),
            name=f"advance{n}",
        )(*operands)

    new, first_b, pot, radii, khat, coup, chain, *sent = run(
        1,
        [message, basis, kinetic],
        [VMEM] * 3,
        [
            full_type,
            block_type,
            shape((nrad, nquad), F32),
            shape((2, nrad, LANES), F32),
            shape((own, 1, LANES), F32),
            shape((own, 1, nang), F32),
            shape((max(own - 1, 1), 1, nang), F32),
        ]
        + [shape((nslab, height - share // LANES * slab, LANES), BF16)] * mirror,
        [],
    )
    if mirror:
        halos.append([lax.ppermute(sent[0], "g", swapped)])
    common = [basis, kinetic, pot, radii, khat, coup, chain]
    joint = pltpu.VMEM((sides, 2, 1, nang), F32)
    operands = halos[0] + common + [new, first_b]
    if mirror:
        ready, part = pl.pallas_call(
            functools.partial(inner, dims),
            out_shape=[
                shape((own - 1, nrad, nang), F32),
                shape((nslab, height - share // LANES * slab, LANES), BF16),
            ],
            in_specs=[VMEM] * 10,
            out_specs=[VMEM] * 2,
            scratch_shapes=[
                pltpu.VMEM((own - 1, nrad, nang), BF16),
                pltpu.VMEM(((own - 1) * nrad, nquad), BF16),
            ],
            compiler_params=PARAMS,
            cost_estimate=pl.CostEstimate(
                flops=4 * own * nrad * nang * nquad,
                bytes_accessed=8 * 1024 * 1024,
                transcendentals=0,
            ),
            name="inner",
        )(*common, new, first_b, message)
        operands.append(ready)
        halos.append([lax.ppermute(part, "g", swapped)])
    first_f, level1_b, new, halo_part, halo1_b, halo1_c, halo1_k = run(
        2,
        operands,
        [VMEM] * len(operands),
        [full_type, block_type, full_type, side_type, halo_type, coup_type, hat_type],
        [joint],
    )
    operands = (
        halos[1]
        + common
        + [new, first_b, first_f, halo_part, halo1_b, halo1_c, halo1_k, level1_b]
    )
    new, halo_part, far_part, halo2_c = run(
        3,
        operands,
        [VMEM] * len(operands),
        [full_type, side_type, side_type, coup_type],
        [
            pltpu.VMEM((own, nrad, nang), F32),
            pltpu.VMEM((sides, nrad, nang), BF16),
            pltpu.VMEM((sides, 1, LANES), F32),
            joint,
        ],
    )
    operands = halos[2] + [new, halo_part, far_part, halo1_c, halo2_c, coup, radii]
    operands += [chan_rad[None], chan_vib[None], projector]
    back = pl.pallas_call(
        functools.partial(close, dims, sides, nchan),
        out_shape=shape((own * nslab, nang // LANES * slab + SMALL, LANES), BF16),
        in_specs=[VMEM] * len(operands),
        out_specs=VMEM,
        scratch_shapes=[pltpu.VMEM((own, nrad, nang), BF16)],
        compiler_params=PARAMS,
        name="close",
    )(*operands)

    home = lax.all_to_all(back, ("hl", "rad"), 0, 0, tiled=True)
    chan = nchan // nslab
    psi_final, amplitude = pl.pallas_call(
        functools.partial(unpack, (slab, nvib, nang, -(-chan // LANES))),
        out_shape=[shape((slab * nvib, nang), F32), shape((1, chan), F32)],
        in_specs=[VMEM],
        out_specs=[HBM, VMEM],
        scratch_shapes=[
            pltpu.VMEM((slab * nvib, nang), F32),
            pltpu.SemaphoreType.DMA((nang // STEP,)),
        ],
        compiler_params=PARAMS,
        name="unpack",
    )(home)
    return (psi_final.reshape(1, slab, nvib, nang), amplitude)


def solution(mesh):
    nhel, nrad = mesh.shape["hel"], mesh.shape["rad"]

    def run(*args):
        nvib = args[0].shape[2]
        groups = nhel * nrad // nvib
        fine = Mesh(mesh.devices.reshape(groups, nhel // groups, nrad), ("g", "hl", "rad"))
        hel = ("g", "hl")
        placed = (
            P(hel, "rad", None, None),
            P("rad", None, None),
            P(),
            P(),
            P("rad"),
            P("rad"),
            P(hel, None),
            P(hel),
            P(),
            P(),
            P(),
        )
        return jax.shard_map(
            per_device,
            mesh=fine,
            in_specs=placed,
            out_specs=(P(hel, "rad", None, None), P(hel, "rad")),
            check_vma=False,
        )(*args)

    return run
```
